1024 devices in a mesh: dp: 32 (over z_hi, x, core), tensor: 32 (over z_lo, y).
Axes of the slice: x: 8, y: 8, z: 8 (z_hi: 2, z_lo: 4; z = z_hi * 4 + z_lo), core: 2. Of those that a mesh axis runs over, the one named last changes fastest.
Arguments:
- grad_out: bfloat16 [8192, 4096], P(('dp', 'tensor')), may hold values from -2.5 to 2.5
- gate_pre: bfloat16 [8192, 14848], P('dp', 'tensor'), may hold values from -8 to 8
- up_pre: bfloat16 [8192, 14848], P('dp', 'tensor'), may hold values from -6 to 6
- down_weight: bfloat16 [4096, 14848], P(None, 'tensor'), may hold values from -1.5 to 1.5
Outputs:
- grad_weight: float32 [4096, 14848], P('dp', 'tensor')
- grad_gate: bfloat16 [8192, 14848], P('dp', 'tensor')
- grad_up: bfloat16 [8192, 14848], P('dp', 'tensor')
The draws below stay inside these ranges and needn't reach their ends.
All inputs are finite; a program needn't handle non-finite values.
Results may differ from the reference program's by a relative error of at most 0.015.
Values may be sent and summed in bfloat16 or wider, within the bound.
No kernel may reach another device: no remote copies, remote signals or barrier semaphores. Data moves between devices by JAX's collectives and lax.ppermute only.
A program may use at most 32 MiB of HBM per device.

```python
import jax
import jax.numpy as jnp
from jax import lax

D_W = 4096
FF_W = 14848
TOKG = 256
TOKENS = 8192
N_DP = 32


def raised(array, key, source, target, blocks, factor):
    def block_of(dim):
        return (jnp.arange(array.shape[dim]) // (array.shape[dim] // blocks)).reshape((-1,) + (1,) * (array.ndim - 1 - dim))

    near = jax.random.permutation(key, blocks)[block_of(target)]
    far = (block_of(target) + blocks // 2) % blocks
    return jnp.where((block_of(source) == near) | (block_of(source) == far), factor * array, array)


def shard_levels(own_key, shape, cuts, low, high):
    def one(dim, parts):
        draws = jax.random.uniform(jax.random.fold_in(jax.random.fold_in(own_key, 6), dim), (parts,), jnp.float32, low / len(cuts), high / len(cuts))
        return jnp.repeat(jnp.exp(draws), shape[dim] // parts).reshape((-1,) + (1,) * (len(shape) - dim - 1))

    loudness = one(*cuts[0])
    for cut in cuts[1:]:
        loudness = loudness * one(*cut)
    return loudness


def normal_values(rng, shape, scale, bound, split=(), held_as=jnp.bfloat16):
    array = jax.random.normal(rng, shape, jnp.float32) * scale
    if len(split) > 0:
        array = shard_levels(rng, shape, split, -0.22, 0.18) * array
    return jnp.clip(array, min=-bound, max=bound).astype(held_as)


def gaussian_with(stream_key, dims, width, most, shards, heavy, kind=jnp.bfloat16):
    values = width * jax.random.normal(stream_key, dims, jnp.float32)
    if shards:
        values = values * shard_levels(stream_key, dims, shards, -0.22, 0.18)
    return jnp.clip(raised(values, jax.random.fold_in(stream_key, 3), *heavy), -most, most).astype(kind)


def setup_inputs(seed: int = 0) -> dict:
    seeds = jax.random.split(jax.random.key(seed), 5)
    grad_out = gaussian_with(seeds[0], (TOKENS, D_W), (4 * TOKENS ** -0.5), 2.5, ((0, 1024),), (0, 1, 1024, 6.0))
    gate_pre = normal_values(seeds[1], (TOKENS, FF_W), 2.0, 8.0, ((0, 32), (1, 32)))
    up_pre = normal_values(seeds[2], (TOKENS, FF_W), 1.0, 6.0, ((0, 32), (1, 32)))
    down_weight = normal_values(seeds[3], (D_W, FF_W), (max(D_W // 256, 1)) ** -0.5, 1.5, ((1, 32),))
    return dict(grad_out=grad_out, gate_pre=gate_pre, up_pre=up_pre, down_weight=down_weight)


def reference(grad_out, gate_pre, up_pre, down_weight):
    gate = gate_pre.astype(jnp.float32)
    upper = up_pre.astype(jnp.float32)
    sig = jax.nn.sigmoid(gate)
    act = gate * sig
    hidden = (act * upper).astype(jnp.bfloat16)
    grad_hidden = jnp.dot(grad_out, down_weight, preferred_element_type=jnp.float32)
    grad_up = (grad_hidden * act).astype(jnp.bfloat16)
    grad_gate = (grad_hidden * upper * sig * (1.0 + gate * (1.0 - sig))).astype(jnp.bfloat16)
    grouped_out = grad_out.reshape(N_DP, TOKG, D_W)
    grouped_hidden = hidden.reshape(N_DP, TOKG, FF_W)

    def add_group(total, pair):
        part = jnp.dot(pair[0].T, pair[1], preferred_element_type=jnp.float32)
        rounded = lax.optimization_barrier(part.astype(jnp.bfloat16))
        return total + rounded.astype(jnp.float32), None

    grad_weight, unused = lax.scan(add_group, jnp.zeros((D_W, FF_W), jnp.float32), (grouped_out, grouped_hidden))
    return grad_weight, grad_gate, grad_up
```

```python
import jax
import jax.numpy as jnp
from jax import lax
from jax.sharding import Mesh, PartitionSpec as P

AXES = ("zh", "x", "c", "zl", "y")
STEPS = (64.0, 32.0, 16.0, 8.0, 4.0, 2.0)


def exponents(most):
    k = jnp.zeros_like(most)
    for bit in STEPS:
        fits = most * (2.0**bit) <= 32768.0
        most = jnp.where(fits, most * (2.0**bit), most)
        k = jnp.where(fits, k + bit, k)
    return k


def power(k, sign):
    scale = jnp.ones_like(k)
    for bit in STEPS:
        has = k >= bit
        scale = jnp.where(has, scale * (2.0 ** (sign * bit)), scale)
        k = jnp.where(has, k - bit, k)
    return scale


def coded(rows):
    n = rows.shape[0]
    wide = rows.astype(jnp.float32)
    most = jnp.max(jnp.abs(wide).reshape(n * 8, 4, 128), axis=(0, 2))
    k = jnp.repeat(exponents(most), 128)[None, None, :]
    return (wide * power(k, 1)).astype(jnp.float16), jnp.broadcast_to(k, (1, 8, 512)).astype(jnp.float16)


def body(grad_out, gate_pre, up_pre, down_weight):
    f_w = grad_out.shape[1]
    gate = gate_pre.T.astype(jnp.float32)
    upper = up_pre.T.astype(jnp.float32)
    sig = jax.nn.sigmoid(gate)
    act = gate * sig
    hidden = (act * upper).astype(jnp.bfloat16)
    h, t = hidden.shape

    split = grad_out.reshape(8, 2, 8, 256).transpose(2, 0, 1, 3).reshape(8, 8, 512)
    mine = lax.all_to_all(split, "x", 0, 0)
    own = grad_out.reshape(8, 8, 512).transpose(1, 0, 2)
    both = jnp.concatenate([own, mine], 0)
    near = lax.all_gather(both, "zl", axis=1)
    hiddens = lax.all_to_all(jnp.broadcast_to(hidden[None], (8, h, t)), "x", 0, 0)

    near = near.reshape(64, 8, 512)
    a, ka = coded(near[:32])
    b, kb = coded(near[32:])
    message = jnp.concatenate([a, b, ka, kb], 0)
    got = lax.all_gather(message, "y", axis=1, tiled=True).astype(jnp.float32)
    whole = (got[:32] * power(got[64], -1)).astype(jnp.bfloat16)
    feats = (got[32:64] * power(got[65], -1)).astype(jnp.bfloat16)
    whole = whole.reshape(8, t, 512)
    feats = feats.reshape(8, t, 512)

    part = lax.dot_general(hiddens, feats, (((0, 2), (0, 1)), ((), ())), preferred_element_type=jnp.float32)
    part = part.astype(jnp.bfloat16).reshape(h, 2, 2, 128).transpose(2, 1, 0, 3)
    part = lax.all_to_all(part, "c", 0, 0).astype(jnp.float32).sum(0).astype(jnp.bfloat16)
    part = lax.all_to_all(part, "zh", 0, 0).astype(jnp.float32).sum(0)

    weight = down_weight.T.reshape(h, 8, 512)
    grad_hidden = lax.dot_general(weight, whole, (((1, 2), (0, 2)), ((), ())), preferred_element_type=jnp.float32)
    grad_up = (grad_hidden * act).astype(jnp.bfloat16)
    grad_gate = (grad_hidden * upper * sig * (1.0 + gate * (1.0 - sig))).astype(jnp.bfloat16)
    return part.T, grad_gate.T, grad_up.T


def solution(mesh):
    dims = (2, 8, 2, 4, 8)
    fine = Mesh(mesh.devices.reshape(dims), AXES)
    dp, tensor = ("zh", "x", "c"), ("zl", "y")
    in_specs = (P(dp + tensor, None), P(dp, tensor), P(dp, tensor), P(None, tensor))
    out_specs = (P(dp, tensor), P(dp, tensor), P(dp, tensor))
    return jax.shard_map(body, mesh=fine, in_specs=in_specs, out_specs=out_specs, check_vma=False)
```

```python
import jax
import jax.numpy as jnp
from jax import lax
from jax.sharding import Mesh, PartitionSpec as P

AXES = ("zh", "x", "c", "zl", "y")
STEPS = (64.0, 32.0, 16.0, 8.0, 4.0, 2.0)


def exponents(most):
    k = jnp.zeros_like(most)
    for bit in STEPS:
        fits = most * (2.0**bit) <= 32768.0
        most = jnp.where(fits, most * (2.0**bit), most)
        k = jnp.where(fits, k + bit, k)
    return k


def power(k, sign):
    scale = jnp.ones_like(k)
    for bit in STEPS:
        has = k >= bit
        scale = jnp.where(has, scale * (2.0 ** (sign * bit)), scale)
        k = jnp.where(has, k - bit, k)
    return scale


def coded(rows):
    n = rows.shape[0]
    wide = rows.astype(jnp.float32)
    most = jnp.max(jnp.abs(wide).reshape(n * 8, 4, 128), axis=(0, 2))
    k = jnp.repeat(exponents(most), 128)[None, None, :]
    return (wide * power(k, 1)).astype(jnp.float16), jnp.broadcast_to(k, (1, 8, 512)).astype(jnp.float16)


def body(grad_out, gate_pre, up_pre, down_weight):
    f_w = grad_out.shape[1]
    gate = gate_pre.T.astype(jnp.float32)
    upper = up_pre.T.astype(jnp.float32)
    sig = jax.nn.sigmoid(gate)
    act = gate * sig
    hidden = (act * upper).astype(jnp.bfloat16)
    h, t = hidden.shape

    split = grad_out.reshape(8, 2, 8, 256).transpose(2, 0, 1, 3).reshape(8, 8, 512)
    mine = lax.all_to_all(jnp.broadcast_to(split[:, None], (8, 4, 8, 512)).reshape(32, 8, 512), ("x", "zl"), 0, 0)
    own = grad_out.reshape(8, 8, 512).transpose(1, 0, 2)
    near = lax.all_gather(own, "zl", axis=1)
    hiddens = lax.all_to_all(jnp.broadcast_to(hidden[None], (8, h, t)), "x", 0, 0)

    a, ka = coded(near.reshape(32, 8, 512))
    b, kb = coded(mine)
    message = jnp.concatenate([a, b, ka, kb], 0)
    got = lax.all_gather(message, "y", axis=1, tiled=True).astype(jnp.float32)
    whole = (got[:32] * power(got[64], -1)).astype(jnp.bfloat16)
    feats = (got[32:64] * power(got[65], -1)).astype(jnp.bfloat16)
    whole = whole.reshape(8, t, 512)
    feats = feats.reshape(8, t, 512)

    part = lax.dot_general(hiddens, feats, (((0, 2), (0, 1)), ((), ())), preferred_element_type=jnp.float32)
    part = part.astype(jnp.bfloat16).reshape(h, 2, 2, 128).transpose(2, 1, 0, 3)
    part = lax.all_to_all(part, "c", 0, 0).astype(jnp.float32).sum(0).astype(jnp.bfloat16)
    part = lax.all_to_all(part, "zh", 0, 0).astype(jnp.float32).sum(0)

    weight = down_weight.T.reshape(h, 8, 512)
    grad_hidden = lax.dot_general(weight, whole, (((1, 2), (0, 2)), ((), ())), preferred_element_type=jnp.float32)
    grad_up = (grad_hidden * act).astype(jnp.bfloat16)
    grad_gate = (grad_hidden * upper * sig * (1.0 + gate * (1.0 - sig))).astype(jnp.bfloat16)
    return part.T, grad_gate.T, grad_up.T


def solution(mesh):
    dims = (2, 8, 2, 4, 8)
    fine = Mesh(mesh.devices.reshape(dims), AXES)
    dp, tensor = ("zh", "x", "c"), ("zl", "y")
    in_specs = (P(dp + tensor, None), P(dp, tensor), P(dp, tensor), P(None, tensor))
    out_specs = (P(dp, tensor), P(dp, tensor), P(dp, tensor))
    return jax.shard_map(body, mesh=fine, in_specs=in_specs, out_specs=out_specs, check_vma=False)
```

```python
import jax
import jax.numpy as jnp
from jax import lax
from jax.experimental import pallas as pl
from jax.experimental.pallas import tpu as pltpu
from jax.sharding import Mesh, PartitionSpec as P

AXES = ("zh", "x", "c", "zl", "y")
STEPS = (64.0, 32.0, 16.0, 8.0, 4.0, 2.0)


def exponents(most):
    k = jnp.zeros_like(most)
    for bit in STEPS:
        fits = most * (2.0**bit) <= 32768.0
        most = jnp.where(fits, most * (2.0**bit), most)
        k = jnp.where(fits, k + bit, k)
    return k


def power(k, sign):
    scale = jnp.ones_like(k)
    for bit in STEPS:
        has = k >= bit
        scale = jnp.where(has, scale * (2.0 ** (sign * bit)), scale)
        k = jnp.where(has, k - bit, k)
    return scale


def coded(rows):
    n = rows.shape[0]
    wide = rows.astype(jnp.float32)
    most = jnp.max(jnp.abs(wide).reshape(n * 8, 4, 128), axis=(0, 2))
    k = jnp.repeat(exponents(most), 128)[None, None, :]
    return (wide * power(k, 1)).astype(jnp.float16), jnp.broadcast_to(k, (1, 8, 512)).astype(jnp.float16)


def hidden_kernel(gate_ref, up_ref, out_ref, done, sem):
    gate = gate_ref[...].astype(jnp.float32)
    sig = jax.nn.sigmoid(gate)
    done[...] = ((gate * sig) * up_ref[...].astype(jnp.float32)).astype(jnp.bfloat16)
    copies = [pltpu.make_async_copy(done, out_ref.at[i], sem.at[i]) for i in range(8)]
    for copy in copies:
        copy.start()
    for copy in copies:
        copy.wait()


def hidden_copies(gate, up):
    h, t = gate.shape
    return pl.pallas_call(
        hidden_kernel,
        out_shape=jax.ShapeDtypeStruct((8, h, t), jnp.bfloat16),
        in_specs=[pl.BlockSpec(memory_space=pltpu.VMEM)] * 2,
        out_specs=pl.BlockSpec(memory_space=pl.ANY),
        scratch_shapes=[pltpu.VMEM((h, t), jnp.bfloat16), pltpu.SemaphoreType.DMA((8,))],
        cost_estimate=pl.CostEstimate(flops=2_000_000, bytes_accessed=10 * h * t * 2, transcendentals=h * t),
        name="hidden_copies",
    )(gate, up)


def split_kernel(g_ref, out_ref):
    for x in range(8):
        for z in range(2):
            piece = g_ref[:, 2048 * z + 256 * x : 2048 * z + 256 * (x + 1)]
            for zl in range(4):
                out_ref[4 * x + zl, :, 256 * z : 256 * (z + 1)] = piece


def split_rows(g):
    return pl.pallas_call(
        split_kernel,
        out_shape=jax.ShapeDtypeStruct((32, 8, 512), jnp.bfloat16),
        in_specs=[pl.BlockSpec(memory_space=pltpu.VMEM)],
        out_specs=pl.BlockSpec(memory_space=pltpu.VMEM),
        name="split_rows",
    )(g)


def turned(x, axis, by):
    size = lax.axis_size(axis)
    return lax.ppermute(x, axis, [(i, (i + by) % size) for i in range(size)])


def body(grad_out, gate_pre, up_pre, down_weight):
    gate_t, up_t = gate_pre.T, up_pre.T
    h, t = gate_t.shape
    zh, c, zl = lax.axis_index("zh"), lax.axis_index("c"), lax.axis_index("zl")

    mine = lax.all_to_all(split_rows(grad_out), ("x", "zl"), 0, 0)
    turns = jnp.stack([grad_out] + [turned(grad_out, "zl", s) for s in (1, 2, 3)])
    hiddens = lax.all_to_all(hidden_copies(gate_t, up_t), "x", 0, 0)

    near = turns.reshape(4, 8, 8, 512).transpose(2, 0, 1, 3)
    near = jnp.take(near, (zl - jnp.arange(4)) % 4, axis=1)
    a, ka = coded(near.reshape(32, 8, 512))
    b, kb = coded(mine)
    message = jnp.concatenate([a, b, ka, kb], 0)
    got = lax.all_gather(message, "y", axis=1, tiled=True)

    def half(z):
        rows = lax.dynamic_slice_in_dim(got, z * 256, 256, 2)
        feats = (rows[32:64].astype(jnp.float32) * power(rows[65].astype(jnp.float32), -1)).astype(jnp.bfloat16).reshape(8, t, 256)
        part = lax.dot_general(hiddens, feats, (((0, 2), (0, 1)), ((), ())), preferred_element_type=jnp.float32)
        ours = lax.dynamic_slice_in_dim(part, c * 128, 128, 1)
        theirs = lax.dynamic_slice_in_dim(part, (1 - c) * 128, 128, 1).astype(jnp.bfloat16)
        return ours + turned(theirs, "c", 1).astype(jnp.float32)

    away = turned(half(1 - zh).astype(jnp.bfloat16), "zh", 1)
    here = half(zh)

    whole = (got[:32].astype(jnp.float32) * power(got[64].astype(jnp.float32), -1)).astype(jnp.bfloat16).reshape(8, t, 512)
    weight = down_weight.T.reshape(h, 8, 512)
    grad_hidden = lax.dot_general(weight, whole, (((1, 2), (0, 2)), ((), ())), preferred_element_type=jnp.float32)
    gate = gate_t.astype(jnp.float32)
    upper = up_t.astype(jnp.float32)
    sig = jax.nn.sigmoid(gate)
    act = gate * sig
    grad_up = (grad_hidden * act).astype(jnp.bfloat16)
    grad_gate = (grad_hidden * upper * sig * (1.0 + gate * (1.0 - sig))).astype(jnp.bfloat16)
    return (here + away.astype(jnp.float32)).T, grad_gate.T, grad_up.T


def solution(mesh):
    dims = (2, 8, 2, 4, 8)
    fine = Mesh(mesh.devices.reshape(dims), AXES)
    dp, tensor = ("zh", "x", "c"), ("zl", "y")
    in_specs = (P(dp + tensor, None), P(dp, tensor), P(dp, tensor), P(None, tensor))
    out_specs = (P(dp, tensor), P(dp, tensor), P(dp, tensor))
    return jax.shard_map(body, mesh=fine, in_specs=in_specs, out_specs=out_specs, check_vma=False)
```

```python
import jax
import jax.numpy as jnp
from jax import lax
from jax.experimental import pallas as pl
from jax.experimental.pallas import tpu as pltpu
from jax.sharding import Mesh, PartitionSpec as P


AXES = ("zh", "x", "c", "zl", "y")
STEPS = (64.0, 32.0, 16.0, 8.0, 4.0, 2.0)


def exponents(most):
    k = jnp.zeros_like(most)
    for bit in STEPS:
        fits = most * (2.0**bit) <= 32768.0
        most = jnp.where(fits, most * (2.0**bit), most)
        k = jnp.where(fits, k + bit, k)
    return k


def power(k, sign):
    scale = jnp.ones_like(k)
    for bit in STEPS:
        has = k >= bit
        scale = jnp.where(has, scale * (2.0 ** (sign * bit)), scale)
        k = jnp.where(has, k - bit, k)
    return scale


def coded(rows):
    n = rows.shape[0]
    wide = rows.astype(jnp.float32)
    most = jnp.max(jnp.abs(wide).reshape(n * 8, 4, 128), axis=(0, 2))
    k = jnp.repeat(exponents(most), 128)[None, None, :]
    return (wide * power(k, 1)).astype(jnp.float16), jnp.broadcast_to(k, (1, 8, 512)).astype(jnp.float16)


def hidden_kernel(gate_ref, up_ref, out_ref, done, sem):
    gate = gate_ref[...].astype(jnp.float32)
    sig = jax.nn.sigmoid(gate)
    done[...] = ((gate * sig) * up_ref[...].astype(jnp.float32)).astype(jnp.bfloat16)
    copies = [pltpu.make_async_copy(done, out_ref.at[i], sem.at[i]) for i in range(8)]
    for copy in copies:
        copy.start()
    for copy in copies:
        copy.wait()


def hidden_copies(gate, up):
    h, t = gate.shape
    return pl.pallas_call(
        hidden_kernel,
        out_shape=jax.ShapeDtypeStruct((8, h, t), jnp.bfloat16),
        in_specs=[pl.BlockSpec(memory_space=pltpu.VMEM)] * 2,
        out_specs=pl.BlockSpec(memory_space=pl.ANY),
        scratch_shapes=[pltpu.VMEM((h, t), jnp.bfloat16), pltpu.SemaphoreType.DMA((8,))],
        cost_estimate=pl.CostEstimate(flops=2_000_000, bytes_accessed=10 * h * t * 2, transcendentals=h * t),
        name="hidden_copies",
    )(gate, up)


def split_kernel(g_ref, out_ref, held, sem):
    zh, c = lax.axis_index("zh"), lax.axis_index("c")
    for x in range(8):
        for i, z in enumerate((1 - zh, zh)):
            for j, core in enumerate((1 - c, c)):
                at = pl.multiple_of(2048 * z + 256 * x + 128 * core, 128)
                piece = g_ref[:, pl.ds(at, 128)]
                for zl in range(4):
                    held[4 * x + zl, :, 256 * i + 128 * j : 256 * i + 128 * (j + 1)] = piece
    copy = pltpu.make_async_copy(held, out_ref, sem)
    copy.start()
    copy.wait()


def split_rows(g):
    return pl.pallas_call(
        split_kernel,
        out_shape=jax.ShapeDtypeStruct((32, 8, 512), jnp.bfloat16),
        in_specs=[pl.BlockSpec(memory_space=pltpu.VMEM)],
        out_specs=pl.BlockSpec(memory_space=pl.ANY),
        scratch_shapes=[pltpu.VMEM((32, 8, 512), jnp.bfloat16), pltpu.SemaphoreType.DMA],
        name="split_rows",
    )(g)


def turned(x, axis, by):
    size = lax.axis_size(axis)
    return lax.ppermute(x, axis, [(i, (i + by) % size) for i in range(size)])


def sections(grad_out, gate_pre, up_pre, down_weight):
    gate_t, up_t = gate_pre.T, up_pre.T
    h, t = gate_t.shape
    zl = lax.axis_index("zl")

    pieces = split_rows(grad_out)
    mine = lax.all_to_all(pieces, ("x", "zl"), 0, 0)
    turns = [grad_out]
    for s in (1, 2, 3):
        turns.append(turned(grad_out, "zl", s))
    copies = hidden_copies(gate_t, up_t)
    hiddens = lax.all_to_all(copies, "x", 0, 0)

    near = jnp.stack(turns).reshape(4, 8, 8, 512).transpose(2, 0, 1, 3)
    near = jnp.take(near, (zl - jnp.arange(4)) % 4, axis=1)
    a, ka = coded(near.reshape(32, 8, 512))
    b, kb = coded(mine)
    message = jnp.concatenate([a, b, ka, kb], 0)
    got = lax.all_gather(message, "y", axis=1, tiled=True)

    def half(got, i):
        rows = got[:, :, 256 * i : 256 * (i + 1)]
        feats = (rows[32:64].astype(jnp.float32) * power(rows[65].astype(jnp.float32), -1)).astype(jnp.bfloat16).reshape(8, t, 256)
        part = lax.dot_general(hiddens, feats, (((0, 2), (0, 1)), ((), ())), preferred_element_type=jnp.float32)
        other = turned(part[:, :128].astype(jnp.bfloat16), "c", 1)
        return part[:, 128:] + other.astype(jnp.float32)

    first = half(got, 0).astype(jnp.bfloat16)
    away = turned(first, "zh", 1)
    got, first = lax.optimization_barrier((got, first))
    here = half(got, 1)

    whole = (got[:32].astype(jnp.float32) * power(got[64].astype(jnp.float32), -1)).astype(jnp.bfloat16).reshape(8, t, 512)
    weight = down_weight.T.reshape(h, 8, 512)
    grad_hidden = lax.dot_general(weight, whole, (((1, 2), (0, 2)), ((), ())), preferred_element_type=jnp.float32)
    gate = gate_t.astype(jnp.float32)
    upper = up_t.astype(jnp.float32)
    sig = jax.nn.sigmoid(gate)
    act = gate * sig
    grad_up = (grad_hidden * act).astype(jnp.bfloat16)
    grad_gate = (grad_hidden * upper * sig * (1.0 + gate * (1.0 - sig))).astype(jnp.bfloat16)
    return (here + away.astype(jnp.float32)).T, grad_gate.T, grad_up.T


def solution(mesh):
    dims = (2, 8, 2, 4, 8)
    fine = Mesh(mesh.devices.reshape(dims), AXES)
    dp, tensor = ("zh", "x", "c"), ("zl", "y")
    in_specs = (P(dp + tensor, None), P(dp, tensor), P(dp, tensor), P(None, tensor))
    out_specs = (P(dp, tensor), P(dp, tensor), P(dp, tensor))
    return jax.shard_map(sections, mesh=fine, in_specs=in_specs, out_specs=out_specs, check_vma=False)
```

```python
import jax
import jax.numpy as jnp
from jax import lax
from jax.experimental import pallas as pl
from jax.experimental.pallas import tpu as pltpu
from jax.sharding import Mesh, PartitionSpec as P


AXES = ("zh", "x", "c", "zl", "y")
STEPS = (64.0, 32.0, 16.0, 8.0, 4.0, 2.0)


def exponents(most):
    k = jnp.zeros_like(most)
    for bit in STEPS:
        fits = most * (2.0**bit) <= 32768.0
        most = jnp.where(fits, most * (2.0**bit), most)
        k = jnp.where(fits, k + bit, k)
    return k


def power(k, sign):
    scale = jnp.ones_like(k)
    for bit in STEPS:
        has = k >= bit
        scale = jnp.where(has, scale * (2.0 ** (sign * bit)), scale)
        k = jnp.where(has, k - bit, k)
    return scale


def scales_of(most):
    k = exponents(jnp.max(jnp.max(most, axis=1, keepdims=True), axis=0, keepdims=True))
    return power(k, 1), k


def own_kernel(a_ref, b_ref, c_ref, d_ref, out_ref, k_ref):
    zl = lax.axis_index("zl")
    turns = (a_ref, b_ref, c_ref, d_ref)
    for b in range(4):
        most = None
        for ref in turns:
            for q in range(8):
                value = jnp.abs(ref[:, 512 * q + 128 * b : 512 * q + 128 * (b + 1)].astype(jnp.float32))
                most = value if most is None else jnp.maximum(most, value)
        scale, k = scales_of(most)
        k_ref[:, 128 * b : 128 * (b + 1)] = jnp.broadcast_to(k, (8, 128)).astype(jnp.bfloat16)
        for s, ref in enumerate(turns):
            place = lax.rem(zl + 4 - s, 4)
            for q in range(8):
                value = ref[:, 512 * q + 128 * b : 512 * q + 128 * (b + 1)].astype(jnp.float32) * scale
                out_ref[4 * q + place, :, 128 * b : 128 * (b + 1)] = value.astype(jnp.bfloat16)


def rows_kernel(rows_ref, out_ref, k_ref):
    for b in range(4):
        cols = slice(128 * b, 128 * (b + 1))
        most = jnp.max(jnp.abs(rows_ref[:, :, cols].astype(jnp.float32)), axis=0)
        scale, k = scales_of(most)
        k_ref[:, cols] = jnp.broadcast_to(k, (8, 128)).astype(jnp.bfloat16)
        out_ref[:, :, cols] = (rows_ref[:, :, cols].astype(jnp.float32) * scale[None]).astype(jnp.bfloat16)


def scaled(kernel, *rows):
    return pl.pallas_call(
        kernel,
        out_shape=(jax.ShapeDtypeStruct((32, 8, 512), jnp.bfloat16), jax.ShapeDtypeStruct((8, 512), jnp.bfloat16)),
        in_specs=[pl.BlockSpec(memory_space=pltpu.VMEM)] * len(rows),
        out_specs=(pl.BlockSpec(memory_space=pltpu.VMEM),) * 2,
        cost_estimate=pl.CostEstimate(flops=1_000_000, bytes_accessed=600_000, transcendentals=0),
        compiler_params=pltpu.CompilerParams(vmem_limit_bytes=4 << 20),
    )(*rows)


def hidden_kernel(gate_ref, up_ref, out_ref, done, sem):
    h = gate_ref.shape[0]
    copies = []
    for n in range(4):
        part = h // 4 // 16 * 16
        at = pl.ds(n * part, part if n < 3 else h - 3 * part)
        gate = gate_ref[at, :].astype(jnp.float32)
        sig = jax.nn.sigmoid(gate)
        done[at, :] = ((gate * sig) * up_ref[at, :].astype(jnp.float32)).astype(jnp.bfloat16)
        for i in range(8):
            copies.append(pltpu.make_async_copy(done.at[at, :], out_ref.at[i, at, :], sem.at[n, i]))
            copies[-1].start()
    for copy in copies:
        copy.wait()


def hidden_copies(gate, up):
    h, t = gate.shape
    return pl.pallas_call(
        hidden_kernel,
        out_shape=jax.ShapeDtypeStruct((8, h, t), jnp.bfloat16),
        in_specs=[pl.BlockSpec(memory_space=pltpu.VMEM)] * 2,
        out_specs=pl.BlockSpec(memory_space=pl.ANY),
        scratch_shapes=[pltpu.VMEM((h, t), jnp.bfloat16), pltpu.SemaphoreType.DMA((4, 8))],
        cost_estimate=pl.CostEstimate(flops=2_000_000, bytes_accessed=10 * h * t * 2, transcendentals=h * t),
        compiler_params=pltpu.CompilerParams(vmem_limit_bytes=2 << 20),
        name="hidden_copies",
    )(gate, up)


def split_kernel(g_ref, out_ref, held, sem):
    zh, c = lax.axis_index("zh"), lax.axis_index("c")
    for x in range(8):
        for i, core in enumerate((1 - c, c)):
            for j, z in enumerate((1 - zh, zh)):
                at = pl.multiple_of(2048 * z + 256 * x + 128 * core, 128)
                piece = g_ref[:, pl.ds(at, 128)]
                for zl in range(4):
                    held[4 * x + zl, :, 256 * i + 128 * j : 256 * i + 128 * (j + 1)] = piece
    copy = pltpu.make_async_copy(held, out_ref, sem)
    copy.start()
    copy.wait()


def split_rows(g):
    return pl.pallas_call(
        split_kernel,
        out_shape=jax.ShapeDtypeStruct((32, 8, 512), jnp.bfloat16),
        in_specs=[pl.BlockSpec(memory_space=pltpu.VMEM)],
        out_specs=pl.BlockSpec(memory_space=pl.ANY),
        scratch_shapes=[pltpu.VMEM((32, 8, 512), jnp.bfloat16), pltpu.SemaphoreType.DMA],
        compiler_params=pltpu.CompilerParams(vmem_limit_bytes=2 << 20),
        name="split_rows",
    )(g)


def turned(x, axis, by):
    size = lax.axis_size(axis)
    return lax.ppermute(x, axis, [(i, (i + by) % size) for i in range(size)])


def sections(grad_out, gate_pre, up_pre, down_weight):
    gate_t, up_t = gate_pre.T, up_pre.T
    h, t = gate_t.shape

    pieces = split_rows(grad_out)
    mine = lax.all_to_all(pieces, ("x", "zl"), 0, 0)
    turns = [grad_out]
    for s in (1, 2, 3):
        turns.append(turned(grad_out, "zl", s))
    copies = hidden_copies(gate_t, up_t)
    hiddens = lax.all_to_all(copies, "x", 0, 0)

    own, own_k = scaled(own_kernel, *turns)
    feats, feats_k = scaled(rows_kernel, mine)
    message = jnp.concatenate([own, feats, own_k[None], feats_k[None]], 0).astype(jnp.float16)
    got = lax.all_gather(message, "y", axis=1, tiled=True)

    scale = power(got[65].astype(jnp.float32), -1)
    feats = (got[32:64].astype(jnp.float32) * scale).astype(jnp.bfloat16).reshape(8, t, 512)
    part = lax.dot_general(hiddens, feats, (((0, 2), (0, 1)), ((), ())), preferred_element_type=jnp.float32)
    swap = lax.all_gather(part[:, :256].astype(jnp.bfloat16), "c", axis=0)
    part = part[:, 256:] + lax.dynamic_index_in_dim(swap, 1 - lax.axis_index("c"), 0, keepdims=False).astype(jnp.float32)
    away = turned(part[:, :128].astype(jnp.bfloat16), "zh", 1)
    here = part[:, 128:]

    scale = power(got[64].astype(jnp.float32), -1)
    whole = (got[:32].astype(jnp.float32) * scale).astype(jnp.bfloat16).reshape(8, t, 512)
    weight = down_weight.T.reshape(h, 8, 512)
    grad_hidden = lax.dot_general(weight, whole, (((1, 2), (0, 2)), ((), ())), preferred_element_type=jnp.float32)
    gate = gate_t.astype(jnp.float32)
    upper = up_t.astype(jnp.float32)
    sig = jax.nn.sigmoid(gate)
    act = gate * sig
    grad_up = (grad_hidden * act).astype(jnp.bfloat16)
    grad_gate = (grad_hidden * upper * sig * (1.0 + gate * (1.0 - sig))).astype(jnp.bfloat16)
    return (here + away.astype(jnp.float32)).T, grad_gate.T, grad_up.T


def solution(mesh):
    dims = (2, 8, 2, 4, 8)
    fine = Mesh(mesh.devices.reshape(dims), AXES)
    dp, tensor = ("zh", "x", "c"), ("zl", "y")
    in_specs = (P(dp + tensor, None), P(dp, tensor), P(dp, tensor), P(None, tensor))
    out_specs = (P(dp, tensor), P(dp, tensor), P(dp, tensor))
    return jax.shard_map(sections, mesh=fine, in_specs=in_specs, out_specs=out_specs, check_vma=False)
```

```python
import jax
import jax.numpy as jnp
from jax import lax
from jax.experimental import pallas as pl
from jax.experimental.pallas import tpu as pltpu
from jax.sharding import Mesh, PartitionSpec as P


AXES = ("zh", "x", "c", "zl", "y")
STEPS = (64.0, 32.0, 16.0, 8.0, 4.0, 2.0)


def exponents(most):
    k = jnp.zeros_like(most)
    for bit in STEPS:
        fits = most * (2.0**bit) <= 32768.0
        most = jnp.where(fits, most * (2.0**bit), most)
        k = jnp.where(fits, k + bit, k)
    return k


def power(k, sign):
    scale = jnp.ones_like(k)
    for bit in STEPS:
        has = k >= bit
        scale = jnp.where(has, scale * (2.0 ** (sign * bit)), scale)
        k = jnp.where(has, k - bit, k)
    return scale


def scales_of(most):
    k = exponents(jnp.max(jnp.max(most, axis=1, keepdims=True), axis=0, keepdims=True))
    return power(k, 1), k


def own_kernel(a_ref, b_ref, c_ref, d_ref, out_ref, k_ref):
    zl = lax.axis_index("zl")
    turns = (a_ref, b_ref, c_ref, d_ref)
    for b in range(4):
        most = None
        for ref in turns:
            for q in range(8):
                value = jnp.abs(ref[:, 512 * q + 128 * b : 512 * q + 128 * (b + 1)].astype(jnp.float32))
                most = value if most is None else jnp.maximum(most, value)
        scale, k = scales_of(most)
        k_ref[:, 128 * b : 128 * (b + 1)] = jnp.broadcast_to(k, (8, 128)).astype(jnp.bfloat16)
        for s, ref in enumerate(turns):
            place = lax.rem(zl + 4 - s, 4)
            for q in range(8):
                value = ref[:, 512 * q + 128 * b : 512 * q + 128 * (b + 1)].astype(jnp.float32) * scale
                out_ref[4 * q + place, :, 128 * b : 128 * (b + 1)] = value.astype(jnp.bfloat16)


def rows_kernel(rows_ref, out_ref, k_ref):
    for b in range(4):
        cols = slice(128 * b, 128 * (b + 1))
        most = jnp.max(jnp.abs(rows_ref[:, :, cols].astype(jnp.float32)), axis=0)
        scale, k = scales_of(most)
        k_ref[:, cols] = jnp.broadcast_to(k, (8, 128)).astype(jnp.bfloat16)
        out_ref[:, :, cols] = (rows_ref[:, :, cols].astype(jnp.float32) * scale[None]).astype(jnp.bfloat16)


def scaled(kernel, *rows):
    return pl.pallas_call(
        kernel,
        out_shape=(jax.ShapeDtypeStruct((32, 8, 512), jnp.bfloat16), jax.ShapeDtypeStruct((8, 512), jnp.bfloat16)),
        in_specs=[pl.BlockSpec(memory_space=pltpu.VMEM)] * len(rows),
        out_specs=(pl.BlockSpec(memory_space=pltpu.VMEM),) * 2,
        cost_estimate=pl.CostEstimate(flops=1_000_000, bytes_accessed=600_000, transcendentals=0),
        compiler_params=pltpu.CompilerParams(vmem_limit_bytes=4 << 20),
    )(*rows)


def hidden_kernel(gate_ref, up_ref, out_ref, gate_in, up_in, done, in_sem, out_sem):
    h = gate_ref.shape[0]
    part = h // 4 // 16 * 16
    bands = [pl.ds(n * part, part if n < 3 else h - 3 * part) for n in range(4)]
    loads = []
    for n, band in enumerate(bands):
        for i, (ref, into) in enumerate(((gate_ref, gate_in), (up_ref, up_in))):
            loads.append(pltpu.make_async_copy(ref.at[band, :], into.at[band, :], in_sem.at[n, i]))
            loads[-1].start()
    copies = []
    for n, band in enumerate(bands):
        loads[2 * n].wait()
        loads[2 * n + 1].wait()
        gate = gate_in[band, :].astype(jnp.float32)
        sig = jax.nn.sigmoid(gate)
        done[band, :] = ((gate * sig) * up_in[band, :].astype(jnp.float32)).astype(jnp.bfloat16)
        for i in range(8):
            copies.append(pltpu.make_async_copy(done.at[band, :], out_ref.at[i, band, :], out_sem.at[n, i]))
            copies[-1].start()
    for copy in copies:
        copy.wait()


def hidden_copies(gate, up):
    h, t = gate.shape
    return pl.pallas_call(
        hidden_kernel,
        out_shape=jax.ShapeDtypeStruct((8, h, t), jnp.bfloat16),
        in_specs=[pl.BlockSpec(memory_space=pltpu.HBM)] * 2,
        out_specs=pl.BlockSpec(memory_space=pl.ANY),
        scratch_shapes=[pltpu.VMEM((h, t), jnp.bfloat16)] * 3 + [pltpu.SemaphoreType.DMA((4, 2)), pltpu.SemaphoreType.DMA((4, 8))],
        cost_estimate=pl.CostEstimate(flops=2_000_000, bytes_accessed=10 * h * t * 2, transcendentals=h * t),
        compiler_params=pltpu.CompilerParams(vmem_limit_bytes=60 * 1024 * 1024),
        name="hidden_copies",
    )(gate, up)


def split_kernel(g_ref, out_ref, held, sem):
    zh, c = lax.axis_index("zh"), lax.axis_index("c")
    for x in range(8):
        for i, core in enumerate((1 - c, c)):
            for j, z in enumerate((1 - zh, zh)):
                at = pl.multiple_of(2048 * z + 256 * x + 128 * core, 128)
                piece = g_ref[:, pl.ds(at, 128)]
                for zl in range(4):
                    held[4 * x + zl, :, 256 * i + 128 * j : 256 * i + 128 * (j + 1)] = piece
    copy = pltpu.make_async_copy(held, out_ref, sem)
    copy.start()
    copy.wait()


def split_rows(g):
    return pl.pallas_call(
        split_kernel,
        out_shape=jax.ShapeDtypeStruct((32, 8, 512), jnp.bfloat16),
        in_specs=[pl.BlockSpec(memory_space=pltpu.VMEM)],
        out_specs=pl.BlockSpec(memory_space=pl.ANY),
        scratch_shapes=[pltpu.VMEM((32, 8, 512), jnp.bfloat16), pltpu.SemaphoreType.DMA],
        compiler_params=pltpu.CompilerParams(vmem_limit_bytes=2 << 20),
        name="split_rows",
    )(g)


def weights_kernel(hidden_ref, feats_ref, theirs_ref, ours_ref, held, sem):
    t = hidden_ref.shape[2]
    loads = [pltpu.make_async_copy(hidden_ref.at[i], held.at[:, t * i : t * (i + 1)], sem.at[i]) for i in range(8)]
    for load in loads:
        load.start()
    for i in range(0, 8, 2):
        loads[i].wait()
        loads[i + 1].wait()
        cols = slice(t * i, t * (i + 2))
        for n, ref in enumerate((theirs_ref, ours_ref)):
            part = jnp.dot(held[:, cols], feats_ref[cols, 256 * n : 256 * (n + 1)], preferred_element_type=jnp.float32)
            ref[...] = part if i == 0 else ref[...] + part


def weight_parts(hiddens, feats):
    _, h, t = hiddens.shape
    return pl.pallas_call(
        weights_kernel,
        out_shape=(jax.ShapeDtypeStruct((h, 256), jnp.float32),) * 2,
        in_specs=[pl.BlockSpec(memory_space=pltpu.HBM), pl.BlockSpec(memory_space=pltpu.VMEM)],
        out_specs=(pl.BlockSpec(memory_space=pltpu.VMEM),) * 2,
        scratch_shapes=[pltpu.VMEM((h, 8 * t), jnp.bfloat16), pltpu.SemaphoreType.DMA((8,))],
        cost_estimate=pl.CostEstimate(flops=2 * 8 * t * h * 512, bytes_accessed=4_000_000, transcendentals=0),
        compiler_params=pltpu.CompilerParams(vmem_limit_bytes=12 << 20),
        name="weight_parts",
    )(hiddens, feats)


def turned(x, axis, by):
    size = lax.axis_size(axis)
    return lax.ppermute(x, axis, [(i, (i + by) % size) for i in range(size)])


def sections(grad_out, gate_pre, up_pre, down_weight):
    gate_t, up_t = gate_pre.T, up_pre.T
    h, t = gate_t.shape

    pieces = split_rows(grad_out)
    mine = lax.all_to_all(pieces, ("x", "zl"), 0, 0)
    turns = [grad_out]
    for s in (1, 2, 3):
        turns.append(turned(grad_out, "zl", s))
    copies = hidden_copies(gate_t, up_t)
    hiddens = lax.all_to_all(copies, "x", 0, 0)

    own, own_k = scaled(own_kernel, *turns)
    feats, feats_k = scaled(rows_kernel, mine)
    message = jnp.concatenate([own, feats, own_k[None], feats_k[None]], 0).astype(jnp.float16)
    got = lax.all_gather(message, "y", axis=1, tiled=True)

    scale = power(got[65].astype(jnp.float32), -1)
    feats = (got[32:64].astype(jnp.float32) * scale).astype(jnp.bfloat16).reshape(8 * t, 512)
    theirs, ours = weight_parts(hiddens, feats)
    swap = lax.all_gather(theirs.astype(jnp.bfloat16), "c", axis=0)
    part = ours + lax.dynamic_index_in_dim(swap, 1 - lax.axis_index("c"), 0, keepdims=False).astype(jnp.float32)
    away = turned(part[:, :128].astype(jnp.bfloat16), "zh", 1)
    here = part[:, 128:]

    scale = power(got[64].astype(jnp.float32), -1)
    whole = (got[:32].astype(jnp.float32) * scale).astype(jnp.bfloat16).reshape(8, t, 512)
    weight = down_weight.T.reshape(h, 8, 512)
    grad_hidden = lax.dot_general(weight, whole, (((1, 2), (0, 2)), ((), ())), preferred_element_type=jnp.float32)
    gate = gate_t.astype(jnp.float32)
    upper = up_t.astype(jnp.float32)
    sig = jax.nn.sigmoid(gate)
    act = gate * sig
    grad_up = (grad_hidden * act).astype(jnp.bfloat16)
    grad_gate = (grad_hidden * upper * sig * (1.0 + gate * (1.0 - sig))).astype(jnp.bfloat16)
    return (here + away.astype(jnp.float32)).T, grad_gate.T, grad_up.T


def solution(mesh):
    dims = (2, 8, 2, 4, 8)
    fine = Mesh(mesh.devices.reshape(dims), AXES)
    dp, tensor = ("zh", "x", "c"), ("zl", "y")
    in_specs = (P(dp + tensor, None), P(dp, tensor), P(dp, tensor), P(None, tensor))
    out_specs = (P(dp, tensor), P(dp, tensor), P(dp, tensor))
    return jax.shard_map(sections, mesh=fine, in_specs=in_specs, out_specs=out_specs, check_vma=False)
```

```python
import jax
import jax.numpy as jnp
from jax import lax
from jax.experimental import pallas as pl
from jax.experimental.pallas import tpu as pltpu
from jax.sharding import Mesh, PartitionSpec as P


AXES = ("zh", "x", "c", "zl", "y")
STEPS = (64.0, 32.0, 16.0, 8.0, 4.0, 2.0)


def exponents(most):
    k = jnp.zeros_like(most)
    for bit in STEPS:
        fits = most * (2.0**bit) <= 32768.0
        most = jnp.where(fits, most * (2.0**bit), most)
        k = jnp.where(fits, k + bit, k)
    return k


def power(k, sign):
    scale = jnp.ones_like(k)
    for bit in STEPS:
        has = k >= bit
        scale = jnp.where(has, scale * (2.0 ** (sign * bit)), scale)
        k = jnp.where(has, k - bit, k)
    return scale


def scales_of(most):
    k = exponents(jnp.max(jnp.max(most, axis=1, keepdims=True), axis=0, keepdims=True))
    return power(k, 1), k


def own_kernel(a_ref, b_ref, c_ref, d_ref, out_ref, k_ref):
    zl = lax.axis_index("zl")
    turns = (a_ref, b_ref, c_ref, d_ref)
    for b in range(4):
        most = None
        for ref in turns:
            for q in range(8):
                value = jnp.abs(ref[:, 512 * q + 128 * b : 512 * q + 128 * (b + 1)].astype(jnp.float32))
                most = value if most is None else jnp.maximum(most, value)
        scale, k = scales_of(most)
        k_ref[:, 128 * b : 128 * (b + 1)] = jnp.broadcast_to(k, (8, 128)).astype(jnp.bfloat16)
        for s, ref in enumerate(turns):
            place = lax.bitwise_xor(zl, s)
            for q in range(8):
                value = ref[:, 512 * q + 128 * b : 512 * q + 128 * (b + 1)].astype(jnp.float32) * scale
                out_ref[4 * q + place, :, 128 * b : 128 * (b + 1)] = value.astype(jnp.bfloat16)


def rows_kernel(rows_ref, out_ref, k_ref):
    for b in range(4):
        cols = slice(128 * b, 128 * (b + 1))
        most = jnp.max(jnp.abs(rows_ref[:, :, cols].astype(jnp.float32)), axis=0)
        scale, k = scales_of(most)
        k_ref[:, cols] = jnp.broadcast_to(k, (8, 128)).astype(jnp.bfloat16)
        out_ref[:, :, cols] = (rows_ref[:, :, cols].astype(jnp.float32) * scale[None]).astype(jnp.bfloat16)


def scaled(kernel, *rows):
    return pl.pallas_call(
        kernel,
        out_shape=(jax.ShapeDtypeStruct((32, 8, 512), jnp.bfloat16), jax.ShapeDtypeStruct((8, 512), jnp.bfloat16)),
        in_specs=[pl.BlockSpec(memory_space=pltpu.VMEM)] * len(rows),
        out_specs=(pl.BlockSpec(memory_space=pltpu.VMEM),) * 2,
        cost_estimate=pl.CostEstimate(flops=1_000_000, bytes_accessed=600_000, transcendentals=0),
        compiler_params=pltpu.CompilerParams(vmem_limit_bytes=4 << 20),
    )(*rows)


def hidden_kernel(gate_ref, up_ref, out_ref, gate_in, up_in, done, in_sem, out_sem):
    h = gate_ref.shape[0]
    part = h // 4 // 16 * 16
    bands = [pl.ds(n * part, part if n < 3 else h - 3 * part) for n in range(4)]
    loads = []
    for n, band in enumerate(bands):
        for i, (ref, into) in enumerate(((gate_ref, gate_in), (up_ref, up_in))):
            loads.append(pltpu.make_async_copy(ref.at[band, :], into.at[band, :], in_sem.at[n, i]))
            loads[-1].start()
    copies = []
    for n, band in enumerate(bands):
        loads[2 * n].wait()
        loads[2 * n + 1].wait()
        gate = gate_in[band, :].astype(jnp.float32)
        sig = jax.nn.sigmoid(gate)
        done[band, :] = ((gate * sig) * up_in[band, :].astype(jnp.float32)).astype(jnp.bfloat16)
        for i in range(8):
            copies.append(pltpu.make_async_copy(done.at[band, :], out_ref.at[i, band, :], out_sem.at[n, i]))
            copies[-1].start()
    for copy in copies:
        copy.wait()


def hidden_copies(gate, up):
    h, t = gate.shape
    return pl.pallas_call(
        hidden_kernel,
        out_shape=jax.ShapeDtypeStruct((8, h, t), jnp.bfloat16),
        in_specs=[pl.BlockSpec(memory_space=pltpu.HBM)] * 2,
        out_specs=pl.BlockSpec(memory_space=pl.ANY),
        scratch_shapes=[pltpu.VMEM((h, t), jnp.bfloat16)] * 3 + [pltpu.SemaphoreType.DMA((4, 2)), pltpu.SemaphoreType.DMA((4, 8))],
        cost_estimate=pl.CostEstimate(flops=2_000_000, bytes_accessed=10 * h * t * 2, transcendentals=h * t),
        compiler_params=pltpu.CompilerParams(vmem_limit_bytes=60 * 1024 * 1024),
        name="hidden_copies",
    )(gate, up)


def split_kernel(g_ref, out_ref, held, sem):
    zh, c = lax.axis_index("zh"), lax.axis_index("c")
    for x in range(8):
        for i, core in enumerate((1 - c, c)):
            for j, z in enumerate((1 - zh, zh)):
                at = pl.multiple_of(2048 * z + 256 * x + 128 * core, 128)
                piece = g_ref[:, pl.ds(at, 128)]
                for zl in range(4):
                    held[4 * x + zl, :, 256 * i + 128 * j : 256 * i + 128 * (j + 1)] = piece
    copy = pltpu.make_async_copy(held, out_ref, sem)
    copy.start()
    copy.wait()


def split_rows(g):
    return pl.pallas_call(
        split_kernel,
        out_shape=jax.ShapeDtypeStruct((32, 8, 512), jnp.bfloat16),
        in_specs=[pl.BlockSpec(memory_space=pltpu.VMEM)],
        out_specs=pl.BlockSpec(memory_space=pl.ANY),
        scratch_shapes=[pltpu.VMEM((32, 8, 512), jnp.bfloat16), pltpu.SemaphoreType.DMA],
        compiler_params=pltpu.CompilerParams(vmem_limit_bytes=2 << 20),
        name="split_rows",
    )(g)


def weights_kernel(hidden_ref, feats_ref, theirs_ref, ours_ref, held, sem):
    t = hidden_ref.shape[2]
    loads = [pltpu.make_async_copy(hidden_ref.at[i], held.at[:, t * i : t * (i + 1)], sem.at[i]) for i in range(8)]
    for load in loads:
        load.start()
    for i in range(0, 8, 2):
        loads[i].wait()
        loads[i + 1].wait()
        cols = slice(t * i, t * (i + 2))
        for n, ref in enumerate((theirs_ref, ours_ref)):
            part = jnp.dot(held[:, cols], feats_ref[cols, 256 * n : 256 * (n + 1)], preferred_element_type=jnp.float32)
            ref[...] = part if i == 0 else ref[...] + part


def weight_parts(hiddens, feats):
    _, h, t = hiddens.shape
    return pl.pallas_call(
        weights_kernel,
        out_shape=(jax.ShapeDtypeStruct((h, 256), jnp.float32),) * 2,
        in_specs=[pl.BlockSpec(memory_space=pltpu.HBM), pl.BlockSpec(memory_space=pltpu.VMEM)],
        out_specs=(pl.BlockSpec(memory_space=pltpu.VMEM),) * 2,
        scratch_shapes=[pltpu.VMEM((h, 8 * t), jnp.bfloat16), pltpu.SemaphoreType.DMA((8,))],
        cost_estimate=pl.CostEstimate(flops=2 * 8 * t * h * 512, bytes_accessed=4_000_000, transcendentals=0),
        compiler_params=pltpu.CompilerParams(vmem_limit_bytes=12 << 20),
        name="weight_parts",
    )(hiddens, feats)


def turned(x, axis, by):
    return lax.ppermute(x, axis, [(i, i ^ by) for i in range(lax.axis_size(axis))])


def inputs_kernel(whole_ref, weight_ref, gate_ref, up_ref, grad_gate_ref, grad_up_ref, weight, gate_in, up_in, total, sem):
    n = weight.shape[0]
    loads = [pltpu.make_async_copy(weight_ref.at[:, 512 * q : 512 * (q + 1)], weight.at[q], sem.at[q]) for q in range(n)]
    loads.append(pltpu.make_async_copy(gate_ref, gate_in, sem.at[n]))
    loads.append(pltpu.make_async_copy(up_ref, up_in, sem.at[n + 1]))
    for load in loads:
        load.start()
    for q in range(n):
        loads[q].wait()
        part = lax.dot_general(weight[q], whole_ref[q], (((1,), (1,)), ((), ())), preferred_element_type=jnp.float32)
        total[...] = part if q == 0 else total[...] + part
    loads[n].wait()
    loads[n + 1].wait()
    grad_hidden = total[...]
    gate = gate_in[...].astype(jnp.float32)
    upper = up_in[...].astype(jnp.float32)
    sig = jax.nn.sigmoid(gate)
    grad_up_ref[...] = (grad_hidden * (gate * sig)).astype(jnp.bfloat16)
    grad_gate_ref[...] = (grad_hidden * upper * sig * (1.0 + gate * (1.0 - sig))).astype(jnp.bfloat16)


def input_grads(whole, weight, gate, up):
    h, t = gate.shape
    n = whole.shape[0]
    return pl.pallas_call(
        inputs_kernel,
        out_shape=(jax.ShapeDtypeStruct((h, t), jnp.bfloat16),) * 2,
        in_specs=[pl.BlockSpec(memory_space=pltpu.VMEM)] + [pl.BlockSpec(memory_space=pltpu.HBM)] * 3,
        out_specs=(pl.BlockSpec(memory_space=pltpu.VMEM),) * 2,
        scratch_shapes=[
            pltpu.VMEM((n, h, 512), jnp.bfloat16),
            pltpu.VMEM((h, t), jnp.bfloat16),
            pltpu.VMEM((h, t), jnp.bfloat16),
            pltpu.VMEM((h, t), jnp.float32),
            pltpu.SemaphoreType.DMA((n + 2,)),
        ],
        cost_estimate=pl.CostEstimate(flops=2 * h * t * 512 * n, bytes_accessed=6_000_000, transcendentals=h * t),
        compiler_params=pltpu.CompilerParams(vmem_limit_bytes=50 << 20),
        name="input_grads",
    )(whole, weight, gate, up)


def sections(grad_out, gate_pre, up_pre, down_weight):
    gate_t, up_t = gate_pre.T, up_pre.T
    _, t = gate_t.shape

    pieces = split_rows(grad_out)
    mine = lax.all_to_all(pieces, ("x", "zl"), 0, 0)
    turns = [grad_out]
    for s in (1, 2, 3):
        turns.append(turned(grad_out, "zl", s))
    copies = hidden_copies(gate_t, up_t)
    hiddens = lax.all_to_all(copies, "x", 0, 0)

    own, own_k = scaled(own_kernel, *turns)
    feats, feats_k = scaled(rows_kernel, mine)
    message = jnp.concatenate([own, feats, own_k[None], feats_k[None]], 0).astype(jnp.float16)
    got = lax.all_gather(message, "y", axis=1, tiled=True)

    scale = power(got[65].astype(jnp.float32), -1)
    feats = (got[32:64].astype(jnp.float32) * scale).astype(jnp.bfloat16).reshape(8 * t, 512)
    theirs, ours = weight_parts(hiddens, feats)
    swap = lax.all_gather(theirs.astype(jnp.bfloat16), "c", axis=0)
    part = ours + lax.dynamic_index_in_dim(swap, 1 - lax.axis_index("c"), 0, keepdims=False).astype(jnp.float32)
    away = turned(part[:, :128].astype(jnp.bfloat16), "zh", 1)
    here = part[:, 128:]

    scale = power(got[64].astype(jnp.float32), -1)
    whole = (got[:32].astype(jnp.float32) * scale).astype(jnp.bfloat16).reshape(8, t, 512)
    grad_gate, grad_up = input_grads(whole, down_weight.T, gate_t, up_t)
    return (here + away.astype(jnp.float32)).T, grad_gate.T, grad_up.T


def solution(mesh):
    dims = (2, 8, 2, 4, 8)
    fine = Mesh(mesh.devices.reshape(dims), AXES)
    dp, tensor = ("zh", "x", "c"), ("zl", "y")
    in_specs = (P(dp + tensor, None), P(dp, tensor), P(dp, tensor), P(None, tensor))
    out_specs = (P(dp, tensor), P(dp, tensor), P(dp, tensor))
    return jax.shard_map(sections, mesh=fine, in_specs=in_specs, out_specs=out_specs, check_vma=False)
```

```python
import jax
import jax.numpy as jnp
from jax import lax
from jax.experimental import pallas as pl
from jax.experimental.pallas import tpu as pltpu
from jax.sharding import Mesh, PartitionSpec as P


AXES = ("zh", "x", "c", "zl", "y")
STEPS = (64.0, 32.0, 16.0, 8.0, 4.0, 2.0)


def exponents(most):
    k = jnp.zeros_like(most)
    for bit in STEPS:
        fits = most * (2.0**bit) <= 32768.0
        most = jnp.where(fits, most * (2.0**bit), most)
        k = jnp.where(fits, k + bit, k)
    return k


def power(k, sign):
    scale = jnp.ones_like(k)
    for bit in STEPS:
        has = k >= bit
        scale = jnp.where(has, scale * (2.0 ** (sign * bit)), scale)
        k = jnp.where(has, k - bit, k)
    return scale


def scales_of(most):
    k = exponents(jnp.max(jnp.max(most, axis=1, keepdims=True), axis=0, keepdims=True))
    return power(k, 1), k


def own_kernel(a_ref, b_ref, c_ref, d_ref, out_ref, k_ref):
    zl = lax.axis_index("zl")
    turns = (a_ref, b_ref, c_ref, d_ref)
    for b in range(4):
        most = None
        for ref in turns:
            for q in range(8):
                value = jnp.abs(ref[:, 512 * q + 128 * b : 512 * q + 128 * (b + 1)].astype(jnp.float32))
                most = value if most is None else jnp.maximum(most, value)
        scale, k = scales_of(most)
        k_ref[:, 128 * b : 128 * (b + 1)] = jnp.broadcast_to(k, (8, 128)).astype(jnp.bfloat16)
        for s, ref in enumerate(turns):
            place = lax.bitwise_xor(zl, s)
            for q in range(8):
                value = ref[:, 512 * q + 128 * b : 512 * q + 128 * (b + 1)].astype(jnp.float32) * scale
                out_ref[4 * q + place, :, 128 * b : 128 * (b + 1)] = value.astype(jnp.bfloat16)


def rows_kernel(rows_ref, out_ref, k_ref):
    for b in range(4):
        cols = slice(128 * b, 128 * (b + 1))
        most = jnp.max(jnp.abs(rows_ref[:, :, cols].astype(jnp.float32)), axis=0)
        scale, k = scales_of(most)
        k_ref[:, cols] = jnp.broadcast_to(k, (8, 128)).astype(jnp.bfloat16)
        out_ref[:, :, cols] = (rows_ref[:, :, cols].astype(jnp.float32) * scale[None]).astype(jnp.bfloat16)


def scaled(kernel, *rows):
    return pl.pallas_call(
        kernel,
        out_shape=(jax.ShapeDtypeStruct((32, 8, 512), jnp.bfloat16), jax.ShapeDtypeStruct((8, 512), jnp.bfloat16)),
        in_specs=[pl.BlockSpec(memory_space=pltpu.VMEM)] * len(rows),
        out_specs=(pl.BlockSpec(memory_space=pltpu.VMEM),) * 2,
        cost_estimate=pl.CostEstimate(flops=1_000_000, bytes_accessed=600_000, transcendentals=0),
        compiler_params=pltpu.CompilerParams(vmem_limit_bytes=4 << 20),
    )(*rows)


def hidden_kernel(gate_ref, up_ref, out_ref, gate_in, up_in, done, in_sem, out_sem):
    h = gate_ref.shape[0]
    part = h // 4 // 16 * 16
    bands = [pl.ds(n * part, part if n < 3 else h - 3 * part) for n in range(4)]
    loads = []
    for n, band in enumerate(bands):
        for i, (ref, into) in enumerate(((gate_ref, gate_in), (up_ref, up_in))):
            loads.append(pltpu.make_async_copy(ref.at[band, :], into.at[band, :], in_sem.at[n, i]))
            loads[-1].start()
    copies = []
    for n, band in enumerate(bands):
        loads[2 * n].wait()
        loads[2 * n + 1].wait()
        gate = gate_in[band, :].astype(jnp.float32)
        sig = jax.nn.sigmoid(gate)
        done[band, :] = ((gate * sig) * up_in[band, :].astype(jnp.float32)).astype(jnp.bfloat16)
        for i in range(8):
            copies.append(pltpu.make_async_copy(done.at[band, :], out_ref.at[i, band, :], out_sem.at[n, i]))
            copies[-1].start()
    for copy in copies:
        copy.wait()


def hidden_copies(gate, up):
    h, t = gate.shape
    return pl.pallas_call(
        hidden_kernel,
        out_shape=jax.ShapeDtypeStruct((8, h, t), jnp.bfloat16),
        in_specs=[pl.BlockSpec(memory_space=pltpu.HBM)] * 2,
        out_specs=pl.BlockSpec(memory_space=pl.ANY),
        scratch_shapes=[pltpu.VMEM((h, t), jnp.bfloat16)] * 3 + [pltpu.SemaphoreType.DMA((4, 2)), pltpu.SemaphoreType.DMA((4, 8))],
        cost_estimate=pl.CostEstimate(flops=2_000_000, bytes_accessed=10 * h * t * 2, transcendentals=h * t),
        compiler_params=pltpu.CompilerParams(vmem_limit_bytes=60 * 1024 * 1024),
        name="hidden_copies",
    )(gate, up)


def split_kernel(g_ref, out_ref, held, sem):
    zh, c = lax.axis_index("zh"), lax.axis_index("c")
    for x in range(8):
        for i, core in enumerate((1 - c, c)):
            for j, z in enumerate((1 - zh, zh)):
                at = pl.multiple_of(2048 * z + 256 * x + 128 * core, 128)
                piece = g_ref[:, pl.ds(at, 128)]
                for zl in range(4):
                    held[4 * x + zl, :, 256 * i + 128 * j : 256 * i + 128 * (j + 1)] = piece
    copy = pltpu.make_async_copy(held, out_ref, sem)
    copy.start()
    copy.wait()


def split_rows(g):
    return pl.pallas_call(
        split_kernel,
        out_shape=jax.ShapeDtypeStruct((32, 8, 512), jnp.bfloat16),
        in_specs=[pl.BlockSpec(memory_space=pltpu.VMEM)],
        out_specs=pl.BlockSpec(memory_space=pl.ANY),
        scratch_shapes=[pltpu.VMEM((32, 8, 512), jnp.bfloat16), pltpu.SemaphoreType.DMA],
        compiler_params=pltpu.CompilerParams(vmem_limit_bytes=2 << 20),
        name="split_rows",
    )(g)


def weights_kernel(hidden_ref, feats_ref, theirs_ref, ours_ref, held, sem):
    t = hidden_ref.shape[2]
    loads = [pltpu.make_async_copy(hidden_ref.at[i], held.at[:, t * i : t * (i + 1)], sem.at[i]) for i in range(8)]
    for load in loads:
        load.start()
    for i in range(0, 8, 2):
        loads[i].wait()
        loads[i + 1].wait()
        cols = slice(t * i, t * (i + 2))
        for n, ref in enumerate((theirs_ref, ours_ref)):
            part = jnp.dot(held[:, cols], feats_ref[cols, 256 * n : 256 * (n + 1)], preferred_element_type=jnp.float32)
            ref[...] = part if i == 0 else ref[...] + part


def weight_parts(hiddens, feats):
    _, h, t = hiddens.shape
    return pl.pallas_call(
        weights_kernel,
        out_shape=(jax.ShapeDtypeStruct((h, 256), jnp.float32),) * 2,
        in_specs=[pl.BlockSpec(memory_space=pltpu.HBM), pl.BlockSpec(memory_space=pltpu.VMEM)],
        out_specs=(pl.BlockSpec(memory_space=pltpu.VMEM),) * 2,
        scratch_shapes=[pltpu.VMEM((h, 8 * t), jnp.bfloat16), pltpu.SemaphoreType.DMA((8,))],
        cost_estimate=pl.CostEstimate(flops=2 * 8 * t * h * 512, bytes_accessed=4_000_000, transcendentals=0),
        compiler_params=pltpu.CompilerParams(vmem_limit_bytes=12 << 20),
        name="weight_parts",
    )(hiddens, feats)


def turned(x, axis, by):
    return lax.ppermute(x, axis, [(i, i ^ by) for i in range(lax.axis_size(axis))])


def sections(grad_out, gate_pre, up_pre, down_weight):
    gate_t, up_t = gate_pre.T, up_pre.T
    h, t = gate_t.shape

    pieces = split_rows(grad_out)
    mine = lax.all_to_all(pieces, ("x", "zl"), 0, 0)
    turns = [grad_out]
    for s in (1, 2, 3):
        turns.append(turned(grad_out, "zl", s))
    copies = hidden_copies(gate_t, up_t)
    hiddens = lax.all_to_all(copies, "x", 0, 0)

    own, own_k = scaled(own_kernel, *turns)
    feats, feats_k = scaled(rows_kernel, mine)
    message = jnp.concatenate([own, feats, own_k[None], feats_k[None]], 0).astype(jnp.float16)
    got = lax.all_gather(message, "y", axis=1, tiled=True)

    scale = power(got[65].astype(jnp.float32), -1)
    feats = (got[32:64].astype(jnp.float32) * scale).astype(jnp.bfloat16).reshape(8 * t, 512)
    theirs, ours = weight_parts(hiddens, feats)
    swap = lax.all_gather(theirs.astype(jnp.bfloat16), "c", axis=0)
    part = ours + lax.dynamic_index_in_dim(swap, 1 - lax.axis_index("c"), 0, keepdims=False).astype(jnp.float32)
    away = turned(part[:, :128].astype(jnp.bfloat16), "zh", 1)
    here = part[:, 128:]

    scale = power(got[64].astype(jnp.float32), -1)
    whole = (got[:32].astype(jnp.float32) * scale).astype(jnp.bfloat16).reshape(8, t, 512)
    weight = down_weight.T.reshape(h, 8, 512)
    grad_hidden = lax.dot_general(weight, whole, (((1, 2), (0, 2)), ((), ())), preferred_element_type=jnp.float32)
    gate = gate_t.astype(jnp.float32)
    upper = up_t.astype(jnp.float32)
    sig = jax.nn.sigmoid(gate)
    act = gate * sig
    grad_up = (grad_hidden * act).astype(jnp.bfloat16)
    grad_gate = (grad_hidden * upper * sig * (1.0 + gate * (1.0 - sig))).astype(jnp.bfloat16)
    return (here + away.astype(jnp.float32)).T, grad_gate.T, grad_up.T


def solution(mesh):
    dims = (2, 8, 2, 4, 8)
    fine = Mesh(mesh.devices.reshape(dims), AXES)
    dp, tensor = ("zh", "x", "c"), ("zl", "y")
    in_specs = (P(dp + tensor, None), P(dp, tensor), P(dp, tensor), P(None, tensor))
    out_specs = (P(dp, tensor), P(dp, tensor), P(dp, tensor))
    return jax.shard_map(sections, mesh=fine, in_specs=in_specs, out_specs=out_specs, check_vma=False)
```

```python
import jax
import jax.numpy as jnp
from jax import lax
from jax.experimental import pallas as pl
from jax.experimental.pallas import tpu as pltpu
from jax.sharding import Mesh, PartitionSpec as P


AXES = ("zh", "xh", "xl", "c", "zl", "y")
NEAR = ("zh", "xl")
STEPS = (64.0, 32.0, 16.0, 8.0, 4.0, 2.0)


def exponents(most):
    k = jnp.zeros_like(most)
    for bit in STEPS:
        fits = most * (2.0**bit) <= 32768.0
        most = jnp.where(fits, most * (2.0**bit), most)
        k = jnp.where(fits, k + bit, k)
    return k


def power(k, sign):
    scale = jnp.ones_like(k)
    for bit in STEPS:
        has = k >= bit
        scale = jnp.where(has, scale * (2.0 ** (sign * bit)), scale)
        k = jnp.where(has, k - bit, k)
    return scale


def scales_of(most):
    k = exponents(jnp.max(jnp.max(most, axis=1, keepdims=True), axis=0, keepdims=True))
    return power(k, 1), k


def columns(zh, xh, xl, c, size):
    return pl.multiple_of(2048 * zh + 512 * xh + 256 * xl + 128 * c, size)


def own_kernel(a_ref, b_ref, c_ref, d_ref, out_ref, k_ref):
    zh, xl, zl = lax.axis_index("zh"), lax.axis_index("xl"), lax.axis_index("zl")
    turns = (a_ref, b_ref, c_ref, d_ref)
    most = None
    for ref in turns:
        for n in range(32):
            value = jnp.abs(ref[:, 128 * n : 128 * (n + 1)].astype(jnp.float32))
            most = value if most is None else jnp.maximum(most, value)
    scale, k = scales_of(most)
    k_ref[...] = jnp.broadcast_to(k[None], (1, 8, 512)).astype(jnp.bfloat16)
    for turn, ref in enumerate(turns):
        place = lax.bitwise_xor(zl, turn)
        for s in (1, 2, 3):
            for xh in range(4):
                at = columns(lax.bitwise_xor(zh, s // 2), xh, lax.bitwise_xor(xl, s % 2), 0, 256)
                value = (ref[:, pl.ds(at, 256)].astype(jnp.float32) * scale).astype(jnp.bfloat16)
                out_ref[4 * (2 * (s - 1) + xh // 2) + place, :, 256 * (xh % 2) : 256 * (xh % 2 + 1)] = value


def rows_kernel(rows_ref, out_ref, k_ref):
    for half in range(2):
        for b in range(4):
            into = slice(128 * b, 128 * (b + 1))
            cols = slice(512 * half + 128 * b, 512 * half + 128 * (b + 1))
            most = jnp.max(jnp.abs(rows_ref[:, :, cols].astype(jnp.float32)), axis=0)
            scale, k = scales_of(most)
            k_ref[half, :, into] = jnp.broadcast_to(k, (8, 128)).astype(jnp.bfloat16)
            value = rows_ref[:, :, cols].astype(jnp.float32) * scale[None]
            out_ref[16 * half : 16 * (half + 1), :, into] = value.astype(jnp.bfloat16)


def scaled(kernel, blocks, ks, *rows):
    return pl.pallas_call(
        kernel,
        out_shape=(jax.ShapeDtypeStruct((blocks, 8, 512), jnp.bfloat16), jax.ShapeDtypeStruct((ks, 8, 512), jnp.bfloat16)),
        in_specs=[pl.BlockSpec(memory_space=pltpu.VMEM)] * len(rows),
        out_specs=(pl.BlockSpec(memory_space=pltpu.VMEM),) * 2,
        cost_estimate=pl.CostEstimate(flops=1_000_000, bytes_accessed=600_000, transcendentals=0),
        compiler_params=pltpu.CompilerParams(vmem_limit_bytes=4 << 20),
    )(*rows)


def hidden_kernel(gate_ref, up_ref, out_ref, gate_in, up_in, done, in_sem, out_sem):
    h = gate_ref.shape[0]
    part = h // 4 // 16 * 16
    bands = [pl.ds(n * part, part if n < 3 else h - 3 * part) for n in range(4)]
    loads = []
    for n, band in enumerate(bands):
        for i, (ref, into) in enumerate(((gate_ref, gate_in), (up_ref, up_in))):
            loads.append(pltpu.make_async_copy(ref.at[band, :], into.at[band, :], in_sem.at[n, i]))
            loads[-1].start()
    copies = []
    for n, band in enumerate(bands):
        loads[2 * n].wait()
        loads[2 * n + 1].wait()
        gate = gate_in[band, :].astype(jnp.float32)
        sig = jax.nn.sigmoid(gate)
        done[band, :] = ((gate * sig) * up_in[band, :].astype(jnp.float32)).astype(jnp.bfloat16)
        for i in range(4):
            copies.append(pltpu.make_async_copy(done.at[band, :], out_ref.at[i, band, :], out_sem.at[n, i]))
            copies[-1].start()
    for copy in copies:
        copy.wait()


def hidden_copies(gate, up):
    h, t = gate.shape
    return pl.pallas_call(
        hidden_kernel,
        out_shape=jax.ShapeDtypeStruct((4, h, t), jnp.bfloat16),
        in_specs=[pl.BlockSpec(memory_space=pltpu.HBM)] * 2,
        out_specs=pl.BlockSpec(memory_space=pl.ANY),
        scratch_shapes=[pltpu.VMEM((h, t), jnp.bfloat16)] * 3 + [pltpu.SemaphoreType.DMA((4, 2)), pltpu.SemaphoreType.DMA((4, 4))],
        cost_estimate=pl.CostEstimate(flops=2_000_000, bytes_accessed=6 * h * t * 2, transcendentals=h * t),
        compiler_params=pltpu.CompilerParams(vmem_limit_bytes=60 * 1024 * 1024),
        name="hidden_copies",
    )(gate, up)


def split_kernel(g_ref, out_ref, held, sem):
    c = lax.axis_index("c")
    for n in range(4):
        for i, core in enumerate((1 - c, c)):
            for xh in range(4):
                piece = g_ref[:, pl.ds(columns(n // 2, xh, n % 2, core, 128), 128)]
                for zl in range(4):
                    held[4 * n + zl, :, 512 * i + 128 * xh : 512 * i + 128 * (xh + 1)] = piece
    copy = pltpu.make_async_copy(held, out_ref, sem)
    copy.start()
    copy.wait()


def split_rows(g):
    return pl.pallas_call(
        split_kernel,
        out_shape=jax.ShapeDtypeStruct((16, 8, 1024), jnp.bfloat16),
        in_specs=[pl.BlockSpec(memory_space=pltpu.VMEM)],
        out_specs=pl.BlockSpec(memory_space=pl.ANY),
        scratch_shapes=[pltpu.VMEM((16, 8, 1024), jnp.bfloat16), pltpu.SemaphoreType.DMA],
        compiler_params=pltpu.CompilerParams(vmem_limit_bytes=2 << 20),
        name="split_rows",
    )(g)


def weights_kernel(hidden_ref, first_ref, second_ref, theirs_ref, ours_ref, held, total, sem):
    n, _, t = hidden_ref.shape
    loads = [pltpu.make_async_copy(hidden_ref.at[i], held.at[:, t * i : t * (i + 1)], sem.at[i]) for i in range(n)]
    for load in loads:
        load.start()
    for i in range(0, n, 2):
        loads[i].wait()
        loads[i + 1].wait()
        cols = slice(t * i, t * (i + 2))
        for half, (rows, ref) in enumerate(((first_ref, total), (second_ref, ours_ref))):
            part = jnp.dot(held[:, cols], rows[cols, :], preferred_element_type=jnp.float32)
            if half == 0 and i == n - 2:
                theirs_ref[...] = (total[...] + part).astype(jnp.bfloat16)
            else:
                ref[...] = part if i == 0 else ref[...] + part


def weight_parts(hiddens, first, second):
    n, h, t = hiddens.shape
    return pl.pallas_call(
        weights_kernel,
        out_shape=(jax.ShapeDtypeStruct((h, 512), jnp.bfloat16), jax.ShapeDtypeStruct((h, 512), jnp.float32)),
        in_specs=[pl.BlockSpec(memory_space=pltpu.HBM)] + [pl.BlockSpec(memory_space=pltpu.VMEM)] * 2,
        out_specs=(pl.BlockSpec(memory_space=pltpu.VMEM),) * 2,
        scratch_shapes=[pltpu.VMEM((h, n * t), jnp.bfloat16), pltpu.VMEM((h, 512), jnp.float32), pltpu.SemaphoreType.DMA((n,))],
        cost_estimate=pl.CostEstimate(flops=2 * n * t * h * 1024, bytes_accessed=4_000_000, transcendentals=0),
        compiler_params=pltpu.CompilerParams(vmem_limit_bytes=12 << 20),
        name="weight_parts",
    )(hiddens, first, second)


def merge_kernel(ours_ref, swap_ref, out_ref):
    other = 1 - lax.axis_index("c")
    for xh in range(4):
        cols = slice(128 * xh, 128 * (xh + 1))
        out_ref[xh] = (ours_ref[:, cols] + swap_ref[other, :, cols].astype(jnp.float32)).astype(jnp.bfloat16)


def merged(ours, swap):
    h = ours.shape[0]
    return pl.pallas_call(
        merge_kernel,
        out_shape=jax.ShapeDtypeStruct((4, h, 128), jnp.bfloat16),
        in_specs=[pl.BlockSpec(memory_space=pltpu.VMEM)] * 2,
        out_specs=pl.BlockSpec(memory_space=pltpu.VMEM),
        cost_estimate=pl.CostEstimate(flops=h * 512, bytes_accessed=h * 512 * 10, transcendentals=0),
        compiler_params=pltpu.CompilerParams(vmem_limit_bytes=4 << 20),
        name="merged",
    )(ours, swap)


def inputs_kernel(front_ref, last_ref, first_ref, second_ref, weight_ref, gate_ref, up_ref, grad_gate_ref, grad_up_ref, weight, shared, gate_in, up_in, total, sem):
    zh, xl, c = lax.axis_index("zh"), lax.axis_index("xl"), lax.axis_index("c")
    t = gate_in.shape[1]
    loads = [[] for _ in range(8)]
    for s in (1, 2, 3):
        for xh in range(4):
            at = columns(lax.bitwise_xor(zh, s // 2), xh, lax.bitwise_xor(xl, s % 2), 0, 256)
            n = 2 * (s - 1) + xh // 2
            into = weight.at[n, :, 256 * (xh % 2) : 256 * (xh % 2 + 1)]
            loads[n].append(pltpu.make_async_copy(weight_ref.at[:, pl.ds(at, 256)], into, sem.at[4 * (s - 1) + xh]))
    for half, (core, rows) in enumerate(((1 - c, first_ref), (c, second_ref))):
        loads[6 + half].append(pltpu.make_async_copy(rows.at[pl.ds((2 * zh + xl) * t, t), :], shared.at[half], sem.at[12 + half]))
        for xh in range(4):
            into = weight.at[6 + half, :, 128 * xh : 128 * (xh + 1)]
            copy = pltpu.make_async_copy(weight_ref.at[:, pl.ds(columns(zh, xh, xl, core, 128), 128)], into, sem.at[14 + 4 * half + xh])
            loads[6 + half].append(copy)
    ends = [pltpu.make_async_copy(gate_ref, gate_in, sem.at[22]), pltpu.make_async_copy(up_ref, up_in, sem.at[23])]
    for copy in [copy for group in loads for copy in group] + ends:
        copy.start()
    for n in range(8):
        for copy in loads[n]:
            copy.wait()
        rows = front_ref[n] if n < 5 else last_ref[0] if n == 5 else shared[n - 6]
        part = lax.dot_general(weight[n], rows, (((1,), (1,)), ((), ())), preferred_element_type=jnp.float32)
        total[...] = part if n == 0 else total[...] + part
    for copy in ends:
        copy.wait()
    grad_hidden = total[...]
    gate = gate_in[...].astype(jnp.float32)
    upper = up_in[...].astype(jnp.float32)
    sig = jax.nn.sigmoid(gate)
    grad_up_ref[...] = (grad_hidden * (gate * sig)).astype(jnp.bfloat16)
    grad_gate_ref[...] = (grad_hidden * upper * sig * (1.0 + gate * (1.0 - sig))).astype(jnp.bfloat16)


def input_grads(front, last, first, second, weight, gate, up):
    h, t = gate.shape
    return pl.pallas_call(
        inputs_kernel,
        out_shape=(jax.ShapeDtypeStruct((h, t), jnp.bfloat16),) * 2,
        in_specs=[pl.BlockSpec(memory_space=pltpu.VMEM)] * 2 + [pl.BlockSpec(memory_space=pl.ANY)] * 2 + [pl.BlockSpec(memory_space=pltpu.HBM)] * 3,
        out_specs=(pl.BlockSpec(memory_space=pltpu.VMEM),) * 2,
        scratch_shapes=[
            pltpu.VMEM((8, h, 512), jnp.bfloat16),
            pltpu.VMEM((2, t, 512), jnp.bfloat16),
            pltpu.VMEM((h, t), jnp.bfloat16),
            pltpu.VMEM((h, t), jnp.bfloat16),
            pltpu.VMEM((h, t), jnp.float32),
            pltpu.SemaphoreType.DMA((24,)),
        ],
        cost_estimate=pl.CostEstimate(flops=2 * h * t * 4096, bytes_accessed=6_000_000, transcendentals=h * t),
        compiler_params=pltpu.CompilerParams(vmem_limit_bytes=50 << 20),
        name="input_grads",
    )(front, last, first, second, weight, gate, up)


def turned(x, axis, by):
    return lax.ppermute(x, axis, [(i, i ^ by) for i in range(lax.axis_size(axis))])


def sections(grad_out, gate_pre, up_pre, down_weight):
    gate_t, up_t = gate_pre.T, up_pre.T
    _, t = gate_t.shape

    pieces = split_rows(grad_out)
    mine = lax.all_to_all(pieces, NEAR + ("zl",), 0, 0)
    turns = [grad_out]
    for s in (1, 2, 3):
        turns.append(turned(grad_out, "zl", s))
    copies = hidden_copies(gate_t, up_t)
    hiddens = lax.all_to_all(copies, NEAR, 0, 0)

    own, own_k = scaled(own_kernel, 24, 1, *turns)
    rows, rows_k = scaled(rows_kernel, 32, 2, mine)
    message = jnp.concatenate([own, rows, own_k, rows_k], 0).astype(jnp.float16)
    got = lax.all_gather(message, "y", axis=1, tiled=True)

    scale = power(got[56:].astype(jnp.float32), -1)
    first = (got[24:40].astype(jnp.float32) * scale[1]).astype(jnp.bfloat16).reshape(4 * t, 512)
    second = (got[40:56].astype(jnp.float32) * scale[2]).astype(jnp.bfloat16).reshape(4 * t, 512)
    front = (got[:20].astype(jnp.float32) * scale[0]).astype(jnp.bfloat16).reshape(5, t, 512)
    last = (got[20:24].astype(jnp.float32) * scale[0]).astype(jnp.bfloat16).reshape(1, t, 512)

    theirs, ours = weight_parts(hiddens, first, second)
    swap = lax.all_gather(theirs, "c", axis=0)
    part = merged(ours, swap)
    terms = lax.all_to_all(part, "xh", 0, 0)
    grad_gate, grad_up = input_grads(front, last, first, second, down_weight.T, gate_t, up_t)
    return terms.astype(jnp.float32).sum(0).T, grad_gate.T, grad_up.T


def solution(mesh):
    dims = (2, 4, 2, 2, 4, 8)
    fine = Mesh(mesh.devices.reshape(dims), AXES)
    dp, tensor = ("zh", "xh", "xl", "c"), ("zl", "y")
    in_specs = (P(dp + tensor, None), P(dp, tensor), P(dp, tensor), P(None, tensor))
    out_specs = (P(dp, tensor), P(dp, tensor), P(dp, tensor))
    return jax.shard_map(sections, mesh=fine, in_specs=in_specs, out_specs=out_specs, check_vma=False)
```

```python
import jax
import jax.numpy as jnp
from jax import lax
from jax.experimental import pallas as pl
from jax.experimental.pallas import tpu as pltpu
from jax.sharding import Mesh, PartitionSpec as P


AXES = ("zh", "xh", "xl", "c", "zl", "y")
NEAR = ("zh", "xl")
STEPS = (64.0, 32.0, 16.0, 8.0, 4.0, 2.0)


def exponents(most):
    k = jnp.zeros_like(most)
    for bit in STEPS:
        fits = most * (2.0**bit) <= 32768.0
        most = jnp.where(fits, most * (2.0**bit), most)
        k = jnp.where(fits, k + bit, k)
    return k


def power(k, sign):
    scale = jnp.ones_like(k)
    for bit in STEPS:
        has = k >= bit
        scale = jnp.where(has, scale * (2.0 ** (sign * bit)), scale)
        k = jnp.where(has, k - bit, k)
    return scale


def scales_of(most):
    k = exponents(jnp.max(jnp.max(most, axis=1, keepdims=True), axis=0, keepdims=True))
    return power(k, 1), k


def columns(zh, xh, xl, c, size):
    return pl.multiple_of(2048 * zh + 512 * xh + 256 * xl + 128 * c, size)


def own_kernel(a_ref, b_ref, c_ref, d_ref, out_ref, k_ref):
    zh, xl, zl = lax.axis_index("zh"), lax.axis_index("xl"), lax.axis_index("zl")
    turns = (a_ref, b_ref, c_ref, d_ref)
    most = None
    for ref in turns:
        for n in range(32):
            value = jnp.abs(ref[:, 128 * n : 128 * (n + 1)].astype(jnp.float32))
            most = value if most is None else jnp.maximum(most, value)
    scale, k = scales_of(most)
    k_ref[...] = jnp.broadcast_to(k[None], (1, 8, 512)).astype(jnp.bfloat16)
    for turn, ref in enumerate(turns):
        place = lax.bitwise_xor(zl, turn)
        for s in (1, 2, 3):
            for xh in range(4):
                at = columns(lax.bitwise_xor(zh, s // 2), xh, lax.bitwise_xor(xl, s % 2), 0, 256)
                value = (ref[:, pl.ds(at, 256)].astype(jnp.float32) * scale).astype(jnp.bfloat16)
                out_ref[4 * (2 * (s - 1) + xh // 2) + place, :, 256 * (xh % 2) : 256 * (xh % 2 + 1)] = value


def rows_kernel(rows_ref, out_ref, k_ref):
    for half in range(2):
        for b in range(4):
            into = slice(128 * b, 128 * (b + 1))
            cols = slice(512 * half + 128 * b, 512 * half + 128 * (b + 1))
            most = jnp.max(jnp.abs(rows_ref[:, :, cols].astype(jnp.float32)), axis=0)
            scale, k = scales_of(most)
            k_ref[half, :, into] = jnp.broadcast_to(k, (8, 128)).astype(jnp.bfloat16)
            value = rows_ref[:, :, cols].astype(jnp.float32) * scale[None]
            out_ref[16 * half : 16 * (half + 1), :, into] = value.astype(jnp.bfloat16)


def scaled(kernel, blocks, ks, *rows):
    return pl.pallas_call(
        kernel,
        out_shape=(jax.ShapeDtypeStruct((blocks, 8, 512), jnp.bfloat16), jax.ShapeDtypeStruct((ks, 8, 512), jnp.bfloat16)),
        in_specs=[pl.BlockSpec(memory_space=pltpu.VMEM)] * len(rows),
        out_specs=(pl.BlockSpec(memory_space=pltpu.VMEM),) * 2,
        cost_estimate=pl.CostEstimate(flops=1_000_000, bytes_accessed=600_000, transcendentals=0),
        compiler_params=pltpu.CompilerParams(vmem_limit_bytes=4 << 20),
    )(*rows)


def hidden_kernel(gate_ref, up_ref, out_ref, gate_in, up_in, done, in_sem, out_sem):
    h = gate_ref.shape[0]
    part = h // 4 // 16 * 16
    bands = [pl.ds(n * part, part if n < 3 else h - 3 * part) for n in range(4)]
    loads = []
    for n, band in enumerate(bands):
        for i, (ref, into) in enumerate(((gate_ref, gate_in), (up_ref, up_in))):
            loads.append(pltpu.make_async_copy(ref.at[band, :], into.at[band, :], in_sem.at[n, i]))
            loads[-1].start()
    copies = []
    for n, band in enumerate(bands):
        loads[2 * n].wait()
        loads[2 * n + 1].wait()
        gate = gate_in[band, :].astype(jnp.float32)
        sig = jax.nn.sigmoid(gate)
        done[band, :] = ((gate * sig) * up_in[band, :].astype(jnp.float32)).astype(jnp.bfloat16)
        for i in range(4):
            copies.append(pltpu.make_async_copy(done.at[band, :], out_ref.at[i, band, :], out_sem.at[n, i]))
            copies[-1].start()
    for copy in copies:
        copy.wait()


def hidden_copies(gate, up):
    h, t = gate.shape
    return pl.pallas_call(
        hidden_kernel,
        out_shape=jax.ShapeDtypeStruct((4, h, t), jnp.bfloat16),
        in_specs=[pl.BlockSpec(memory_space=pltpu.HBM)] * 2,
        out_specs=pl.BlockSpec(memory_space=pl.ANY),
        scratch_shapes=[pltpu.VMEM((h, t), jnp.bfloat16)] * 3 + [pltpu.SemaphoreType.DMA((4, 2)), pltpu.SemaphoreType.DMA((4, 4))],
        cost_estimate=pl.CostEstimate(flops=2_000_000, bytes_accessed=6 * h * t * 2, transcendentals=h * t),
        compiler_params=pltpu.CompilerParams(vmem_limit_bytes=60 * 1024 * 1024),
        name="hidden_copies",
    )(gate, up)


def split_kernel(g_ref, out_ref, held, sem):
    c = lax.axis_index("c")
    for n in range(4):
        for i, core in enumerate((1 - c, c)):
            for xh in range(4):
                piece = g_ref[:, pl.ds(columns(n // 2, xh, n % 2, core, 128), 128)]
                for zl in range(4):
                    held[4 * n + zl, :, 512 * i + 128 * xh : 512 * i + 128 * (xh + 1)] = piece
    copy = pltpu.make_async_copy(held, out_ref, sem)
    copy.start()
    copy.wait()


def split_rows(g):
    return pl.pallas_call(
        split_kernel,
        out_shape=jax.ShapeDtypeStruct((16, 8, 1024), jnp.bfloat16),
        in_specs=[pl.BlockSpec(memory_space=pltpu.VMEM)],
        out_specs=pl.BlockSpec(memory_space=pl.ANY),
        scratch_shapes=[pltpu.VMEM((16, 8, 1024), jnp.bfloat16), pltpu.SemaphoreType.DMA],
        compiler_params=pltpu.CompilerParams(vmem_limit_bytes=2 << 20),
        name="split_rows",
    )(g)


def weights_kernel(hidden_ref, first_ref, second_ref, theirs_ref, ours_ref, held, total, sem):
    n, _, t = hidden_ref.shape
    loads = [pltpu.make_async_copy(hidden_ref.at[i], held.at[:, t * i : t * (i + 1)], sem.at[i]) for i in range(n)]
    for load in loads:
        load.start()
    for i in range(0, n, 2):
        loads[i].wait()
        loads[i + 1].wait()
        cols = slice(t * i, t * (i + 2))
        for half, (rows, ref) in enumerate(((first_ref, total), (second_ref, ours_ref))):
            part = jnp.dot(held[:, cols], rows[cols, :], preferred_element_type=jnp.float32)
            if half == 0 and i == n - 2:
                theirs_ref[...] = (total[...] + part).astype(jnp.bfloat16)
            else:
                ref[...] = part if i == 0 else ref[...] + part


def weight_parts(hiddens, first, second):
    n, h, t = hiddens.shape
    return pl.pallas_call(
        weights_kernel,
        out_shape=(jax.ShapeDtypeStruct((h, 512), jnp.bfloat16), jax.ShapeDtypeStruct((h, 512), jnp.float32)),
        in_specs=[pl.BlockSpec(memory_space=pltpu.HBM)] + [pl.BlockSpec(memory_space=pltpu.VMEM)] * 2,
        out_specs=(pl.BlockSpec(memory_space=pltpu.VMEM),) * 2,
        scratch_shapes=[pltpu.VMEM((h, n * t), jnp.bfloat16), pltpu.VMEM((h, 512), jnp.float32), pltpu.SemaphoreType.DMA((n,))],
        cost_estimate=pl.CostEstimate(flops=2 * n * t * h * 1024, bytes_accessed=4_000_000, transcendentals=0),
        compiler_params=pltpu.CompilerParams(vmem_limit_bytes=12 << 20),
        name="weight_parts",
    )(hiddens, first, second)


def merge_kernel(ours_ref, swap_ref, here_ref, *away_refs):
    other, xh = 1 - lax.axis_index("c"), lax.axis_index("xh")
    for s in range(4):
        cols = pl.ds(pl.multiple_of(128 * lax.bitwise_xor(xh, s), 128), 128)
        value = ours_ref[:, cols] + swap_ref[other, :, cols].astype(jnp.float32)
        if s == 0:
            here_ref[...] = value
        else:
            away_refs[s - 1][...] = value.astype(jnp.bfloat16)


def merged(ours, swap):
    h = ours.shape[0]
    return pl.pallas_call(
        merge_kernel,
        out_shape=(jax.ShapeDtypeStruct((h, 128), jnp.float32),) + (jax.ShapeDtypeStruct((h, 128), jnp.bfloat16),) * 3,
        in_specs=[pl.BlockSpec(memory_space=pltpu.VMEM)] * 2,
        out_specs=(pl.BlockSpec(memory_space=pltpu.VMEM),) * 4,
        cost_estimate=pl.CostEstimate(flops=h * 512, bytes_accessed=h * 512 * 10, transcendentals=0),
        compiler_params=pltpu.CompilerParams(vmem_limit_bytes=4 << 20),
        name="merged",
    )(ours, swap)


def inputs_kernel(front_ref, last_ref, first_ref, second_ref, weight_ref, gate_ref, up_ref, grad_gate_ref, grad_up_ref, weight, total):
    zh, xl, c = lax.axis_index("zh"), lax.axis_index("xl"), lax.axis_index("c")
    t = gate_ref.shape[1]
    shared = pl.ds(pl.multiple_of((2 * zh + xl) * t, t), t)
    for n in range(8):
        slot = n % 2
        if n < 6:
            for i in range(2):
                at = columns(lax.bitwise_xor(zh, (n // 2 + 1) // 2), 2 * (n % 2) + i, lax.bitwise_xor(xl, (n // 2 + 1) % 2), 0, 256)
                weight[slot, :, 256 * i : 256 * (i + 1)] = weight_ref[:, pl.ds(at, 256)]
            rows = front_ref[n] if n < 5 else last_ref[0]
        else:
            core = 1 - c if n == 6 else c
            for xh in range(4):
                weight[slot, :, 128 * xh : 128 * (xh + 1)] = weight_ref[:, pl.ds(columns(zh, xh, xl, core, 128), 128)]
            rows = first_ref[shared, :] if n == 6 else second_ref[shared, :]
        part = lax.dot_general(weight[slot], rows, (((1,), (1,)), ((), ())), preferred_element_type=jnp.float32)
        total[...] = part if n == 0 else total[...] + part
    grad_hidden = total[...]
    gate = gate_ref[...].astype(jnp.float32)
    upper = up_ref[...].astype(jnp.float32)
    sig = jax.nn.sigmoid(gate)
    grad_up_ref[...] = (grad_hidden * (gate * sig)).astype(jnp.bfloat16)
    grad_gate_ref[...] = (grad_hidden * upper * sig * (1.0 + gate * (1.0 - sig))).astype(jnp.bfloat16)


def input_grads(front, last, first, second, weight, gate, up):
    h, t = gate.shape
    return pl.pallas_call(
        inputs_kernel,
        out_shape=(jax.ShapeDtypeStruct((h, t), jnp.bfloat16),) * 2,
        in_specs=[pl.BlockSpec(memory_space=pltpu.VMEM)] * 7,
        out_specs=(pl.BlockSpec(memory_space=pltpu.VMEM),) * 2,
        scratch_shapes=[pltpu.VMEM((2, h, 512), jnp.bfloat16), pltpu.VMEM((h, t), jnp.float32)],
        cost_estimate=pl.CostEstimate(flops=2 * h * t * 4096, bytes_accessed=6_000_000, transcendentals=h * t),
        compiler_params=pltpu.CompilerParams(vmem_limit_bytes=16 << 20),
        name="input_grads",
    )(front, last, first, second, weight, gate, up)


def turned(x, axis, by):
    return lax.ppermute(x, axis, [(i, i ^ by) for i in range(lax.axis_size(axis))])


def sections(grad_out, gate_pre, up_pre, down_weight):
    gate_t, up_t = gate_pre.T, up_pre.T
    _, t = gate_t.shape

    pieces = split_rows(grad_out)
    mine = lax.all_to_all(pieces, NEAR + ("zl",), 0, 0)
    turns = [grad_out]
    for s in (1, 2, 3):
        turns.append(turned(grad_out, "zl", s))
    copies = hidden_copies(gate_t, up_t)
    hiddens = lax.all_to_all(copies, NEAR, 0, 0)

    own, own_k = scaled(own_kernel, 24, 1, *turns)
    rows, rows_k = scaled(rows_kernel, 32, 2, mine)
    message = jnp.concatenate([own, rows, own_k, rows_k], 0).astype(jnp.float16)
    got = lax.all_gather(message, "y", axis=1, tiled=True)

    scale = power(got[56:].astype(jnp.float32), -1)
    first = (got[24:40].astype(jnp.float32) * scale[1]).astype(jnp.bfloat16).reshape(4 * t, 512)
    second = (got[40:56].astype(jnp.float32) * scale[2]).astype(jnp.bfloat16).reshape(4 * t, 512)
    front = (got[:20].astype(jnp.float32) * scale[0]).astype(jnp.bfloat16).reshape(5, t, 512)
    last = (got[20:24].astype(jnp.float32) * scale[0]).astype(jnp.bfloat16).reshape(1, t, 512)

    theirs, ours = weight_parts(hiddens, first, second)
    swap = lax.all_gather(theirs, "c", axis=0)
    here, *away = merged(ours, swap)
    for s in (2, 1, 3):
        here = here + turned(away[s - 1], "xh", s).astype(jnp.float32)
    grad_gate, grad_up = input_grads(front, last, first, second, down_weight.T, gate_t, up_t)
    return here.T, grad_gate.T, grad_up.T


def solution(mesh):
    dims = (2, 4, 2, 2, 4, 8)
    fine = Mesh(mesh.devices.reshape(dims), AXES)
    dp, tensor = ("zh", "xh", "xl", "c"), ("zl", "y")
    in_specs = (P(dp + tensor, None), P(dp, tensor), P(dp, tensor), P(None, tensor))
    out_specs = (P(dp, tensor), P(dp, tensor), P(dp, tensor))
    return jax.shard_map(sections, mesh=fine, in_specs=in_specs, out_specs=out_specs, check_vma=False)
```

```python
import jax
import jax.numpy as jnp
from jax import lax
from jax.experimental import pallas as pl
from jax.experimental.pallas import tpu as pltpu
from jax.sharding import Mesh, PartitionSpec as P


AXES = ("zh", "x", "c", "zl", "y")
STEPS = (64.0, 32.0, 16.0, 8.0, 4.0, 2.0)


def exponents(most):
    k = jnp.zeros_like(most)
    for bit in STEPS:
        fits = most * (2.0**bit) <= 32768.0
        most = jnp.where(fits, most * (2.0**bit), most)
        k = jnp.where(fits, k + bit, k)
    return k


def power(k, sign):
    scale = jnp.ones_like(k)
    for bit in STEPS:
        has = k >= bit
        scale = jnp.where(has, scale * (2.0 ** (sign * bit)), scale)
        k = jnp.where(has, k - bit, k)
    return scale


def scales_of(most):
    k = exponents(jnp.max(jnp.max(most, axis=1, keepdims=True), axis=0, keepdims=True))
    return power(k, 1), k


def own_kernel(a_ref, b_ref, c_ref, d_ref, out_ref, k_ref):
    x, zl = lax.axis_index("x"), lax.axis_index("zl")
    turns = (a_ref, b_ref, c_ref, d_ref)
    most = None
    for ref in turns:
        for n in range(32):
            value = jnp.abs(ref[:, 128 * n : 128 * (n + 1)].astype(jnp.float32))
            most = value if most is None else jnp.maximum(most, value)
    scale, k = scales_of(most)
    k_ref[...] = jnp.broadcast_to(k[None], (1, 8, 512)).astype(jnp.bfloat16)
    for turn, ref in enumerate(turns):
        place = lax.bitwise_xor(zl, turn)
        for s in range(1, 8):
            for z in range(2):
                at = pl.multiple_of(2048 * z + 256 * lax.bitwise_xor(x, s), 256)
                value = (ref[:, pl.ds(at, 256)].astype(jnp.float32) * scale).astype(jnp.bfloat16)
                out_ref[4 * (s - 1) + place, :, 256 * z : 256 * (z + 1)] = value


def rows_kernel(rows_ref, out_ref, k_ref):
    for b in range(4):
        cols = slice(128 * b, 128 * (b + 1))
        most = jnp.max(jnp.abs(rows_ref[:, :, cols].astype(jnp.float32)), axis=0)
        scale, k = scales_of(most)
        k_ref[0, :, cols] = jnp.broadcast_to(k, (8, 128)).astype(jnp.bfloat16)
        out_ref[:, :, cols] = (rows_ref[:, :, cols].astype(jnp.float32) * scale[None]).astype(jnp.bfloat16)


def scaled(kernel, blocks, ks, *rows):
    return pl.pallas_call(
        kernel,
        out_shape=(jax.ShapeDtypeStruct((blocks, 8, 512), jnp.bfloat16), jax.ShapeDtypeStruct((ks, 8, 512), jnp.bfloat16)),
        in_specs=[pl.BlockSpec(memory_space=pltpu.VMEM)] * len(rows),
        out_specs=(pl.BlockSpec(memory_space=pltpu.VMEM),) * 2,
        cost_estimate=pl.CostEstimate(flops=1_000_000, bytes_accessed=600_000, transcendentals=0),
        compiler_params=pltpu.CompilerParams(vmem_limit_bytes=4 << 20),
    )(*rows)


def hidden_kernel(gate_ref, up_ref, out_ref, gate_in, up_in, done, in_sem, out_sem):
    h = gate_ref.shape[0]
    part = h // 4 // 16 * 16
    bands = [pl.ds(n * part, part if n < 3 else h - 3 * part) for n in range(4)]
    loads = []
    for n, band in enumerate(bands):
        for i, (ref, into) in enumerate(((gate_ref, gate_in), (up_ref, up_in))):
            loads.append(pltpu.make_async_copy(ref.at[band, :], into.at[band, :], in_sem.at[n, i]))
            loads[-1].start()
    copies = []
    for n, band in enumerate(bands):
        loads[2 * n].wait()
        loads[2 * n + 1].wait()
        gate = gate_in[band, :].astype(jnp.float32)
        sig = jax.nn.sigmoid(gate)
        done[band, :] = ((gate * sig) * up_in[band, :].astype(jnp.float32)).astype(jnp.bfloat16)
        for i in range(8):
            copies.append(pltpu.make_async_copy(done.at[band, :], out_ref.at[i, band, :], out_sem.at[n, i]))
            copies[-1].start()
    for copy in copies:
        copy.wait()


def hidden_copies(gate, up):
    h, t = gate.shape
    return pl.pallas_call(
        hidden_kernel,
        out_shape=jax.ShapeDtypeStruct((8, h, t), jnp.bfloat16),
        in_specs=[pl.BlockSpec(memory_space=pltpu.HBM)] * 2,
        out_specs=pl.BlockSpec(memory_space=pl.ANY),
        scratch_shapes=[pltpu.VMEM((h, t), jnp.bfloat16)] * 3 + [pltpu.SemaphoreType.DMA((4, 2)), pltpu.SemaphoreType.DMA((4, 8))],
        cost_estimate=pl.CostEstimate(flops=2_000_000, bytes_accessed=10 * h * t * 2, transcendentals=h * t),
        compiler_params=pltpu.CompilerParams(vmem_limit_bytes=60 * 1024 * 1024),
        name="hidden_copies",
    )(gate, up)


def split_kernel(g_ref, out_ref, held, sem):
    zh, c = lax.axis_index("zh"), lax.axis_index("c")
    for x in range(8):
        for i, core in enumerate((1 - c, c)):
            for j, z in enumerate((1 - zh, zh)):
                at = pl.multiple_of(2048 * z + 256 * x + 128 * core, 128)
                piece = g_ref[:, pl.ds(at, 128)]
                for zl in range(4):
                    held[4 * x + zl, :, 256 * i + 128 * j : 256 * i + 128 * (j + 1)] = piece
    copy = pltpu.make_async_copy(held, out_ref, sem)
    copy.start()
    copy.wait()


def split_rows(g):
    return pl.pallas_call(
        split_kernel,
        out_shape=jax.ShapeDtypeStruct((32, 8, 512), jnp.bfloat16),
        in_specs=[pl.BlockSpec(memory_space=pltpu.VMEM)],
        out_specs=pl.BlockSpec(memory_space=pl.ANY),
        scratch_shapes=[pltpu.VMEM((32, 8, 512), jnp.bfloat16), pltpu.SemaphoreType.DMA],
        compiler_params=pltpu.CompilerParams(vmem_limit_bytes=2 << 20),
        name="split_rows",
    )(g)


def weights_kernel(hidden_ref, feats_ref, theirs_ref, ours_ref, held, sem):
    t = hidden_ref.shape[2]
    loads = [pltpu.make_async_copy(hidden_ref.at[i], held.at[:, t * i : t * (i + 1)], sem.at[i]) for i in range(8)]
    for load in loads:
        load.start()
    for i in range(0, 8, 2):
        loads[i].wait()
        loads[i + 1].wait()
        cols = slice(t * i, t * (i + 2))
        for n, ref in enumerate((theirs_ref, ours_ref)):
            part = jnp.dot(held[:, cols], feats_ref[cols, 256 * n : 256 * (n + 1)], preferred_element_type=jnp.float32)
            ref[...] = part if i == 0 else ref[...] + part


def weight_parts(hiddens, feats):
    _, h, t = hiddens.shape
    return pl.pallas_call(
        weights_kernel,
        out_shape=(jax.ShapeDtypeStruct((h, 256), jnp.float32),) * 2,
        in_specs=[pl.BlockSpec(memory_space=pltpu.HBM), pl.BlockSpec(memory_space=pltpu.VMEM)],
        out_specs=(pl.BlockSpec(memory_space=pltpu.VMEM),) * 2,
        scratch_shapes=[pltpu.VMEM((h, 8 * t), jnp.bfloat16), pltpu.SemaphoreType.DMA((8,))],
        cost_estimate=pl.CostEstimate(flops=2 * 8 * t * h * 512, bytes_accessed=4_000_000, transcendentals=0),
        compiler_params=pltpu.CompilerParams(vmem_limit_bytes=12 << 20),
        name="weight_parts",
    )(hiddens, feats)


def inputs_kernel(front_ref, last_ref, feats_ref, weight_ref, gate_ref, up_ref, grad_gate_ref, grad_up_ref, weight, total):
    zh, x, c = lax.axis_index("zh"), lax.axis_index("x"), lax.axis_index("c")
    t = gate_ref.shape[1]
    for n in range(8):
        slot = n % 2
        if n < 7:
            for z in range(2):
                at = pl.multiple_of(2048 * z + 256 * lax.bitwise_xor(x, n + 1), 256)
                weight[slot, :, 256 * z : 256 * (z + 1)] = weight_ref[:, pl.ds(at, 256)]
            rows = front_ref[n] if n < 5 else last_ref[n - 5]
        else:
            for i, core in enumerate((1 - c, c)):
                for j, z in enumerate((1 - zh, zh)):
                    at = pl.multiple_of(2048 * z + 256 * x + 128 * core, 128)
                    weight[slot, :, 256 * i + 128 * j : 256 * i + 128 * (j + 1)] = weight_ref[:, pl.ds(at, 128)]
            rows = feats_ref[pl.ds(pl.multiple_of(x * t, t), t), :]
        part = lax.dot_general(weight[slot], rows, (((1,), (1,)), ((), ())), preferred_element_type=jnp.float32)
        total[...] = part if n == 0 else total[...] + part
    grad_hidden = total[...]
    gate = gate_ref[...].astype(jnp.float32)
    upper = up_ref[...].astype(jnp.float32)
    sig = jax.nn.sigmoid(gate)
    grad_up_ref[...] = (grad_hidden * (gate * sig)).astype(jnp.bfloat16)
    grad_gate_ref[...] = (grad_hidden * upper * sig * (1.0 + gate * (1.0 - sig))).astype(jnp.bfloat16)


def input_grads(front, last, feats, weight, gate, up):
    h, t = gate.shape
    return pl.pallas_call(
        inputs_kernel,
        out_shape=(jax.ShapeDtypeStruct((h, t), jnp.bfloat16),) * 2,
        in_specs=[pl.BlockSpec(memory_space=pltpu.VMEM)] * 6,
        out_specs=(pl.BlockSpec(memory_space=pltpu.VMEM),) * 2,
        scratch_shapes=[pltpu.VMEM((2, h, 512), jnp.bfloat16), pltpu.VMEM((h, t), jnp.float32)],
        cost_estimate=pl.CostEstimate(flops=2 * h * t * 4096, bytes_accessed=6_000_000, transcendentals=h * t),
        compiler_params=pltpu.CompilerParams(vmem_limit_bytes=16 << 20),
        name="input_grads",
    )(front, last, feats, weight, gate, up)


def turned(x, axis, by):
    return lax.ppermute(x, axis, [(i, i ^ by) for i in range(lax.axis_size(axis))])


def sections(grad_out, gate_pre, up_pre, down_weight):
    gate_t, up_t = gate_pre.T, up_pre.T
    _, t = gate_t.shape

    pieces = split_rows(grad_out)
    mine = lax.all_to_all(pieces, ("x", "zl"), 0, 0)
    turns = [grad_out]
    for s in (1, 2, 3):
        turns.append(turned(grad_out, "zl", s))
    copies = hidden_copies(gate_t, up_t)
    hiddens = lax.all_to_all(copies, "x", 0, 0)

    own, own_k = scaled(own_kernel, 28, 1, *turns)
    rows, rows_k = scaled(rows_kernel, 32, 1, mine)
    message = jnp.concatenate([own, rows, own_k, rows_k], 0).astype(jnp.float16)
    got = lax.all_gather(message, "y", axis=1, tiled=True)

    scale = power(got[60:].astype(jnp.float32), -1)
    feats = (got[28:60].astype(jnp.float32) * scale[1]).astype(jnp.bfloat16).reshape(8 * t, 512)
    front = (got[:20].astype(jnp.float32) * scale[0]).astype(jnp.bfloat16).reshape(5, t, 512)
    last = (got[20:28].astype(jnp.float32) * scale[0]).astype(jnp.bfloat16).reshape(2, t, 512)

    theirs, ours = weight_parts(hiddens, feats)
    swap = lax.all_gather(theirs.astype(jnp.bfloat16), "c", axis=0)
    part = ours + lax.dynamic_index_in_dim(swap, 1 - lax.axis_index("c"), 0, keepdims=False).astype(jnp.float32)
    away = turned(part[:, :128].astype(jnp.bfloat16), "zh", 1)
    here = part[:, 128:]

    grad_gate, grad_up = input_grads(front, last, feats, down_weight.T, gate_t, up_t)
    return (here + away.astype(jnp.float32)).T, grad_gate.T, grad_up.T


def solution(mesh):
    dims = (2, 8, 2, 4, 8)
    fine = Mesh(mesh.devices.reshape(dims), AXES)
    dp, tensor = ("zh", "x", "c"), ("zl", "y")
    in_specs = (P(dp + tensor, None), P(dp, tensor), P(dp, tensor), P(None, tensor))
    out_specs = (P(dp, tensor), P(dp, tensor), P(dp, tensor))
    return jax.shard_map(sections, mesh=fine, in_specs=in_specs, out_specs=out_specs, check_vma=False)
```

```python
import jax
import jax.numpy as jnp
from jax import lax
from jax.experimental import pallas as pl
from jax.experimental.pallas import tpu as pltpu
from jax.sharding import Mesh, PartitionSpec as P


AXES = ("zh", "x", "c", "zl", "y")
STEPS = (64.0, 32.0, 16.0, 8.0, 4.0, 2.0)


def exponents(most):
    k = jnp.zeros_like(most)
    for bit in STEPS:
        fits = most * (2.0**bit) <= 32768.0
        most = jnp.where(fits, most * (2.0**bit), most)
        k = jnp.where(fits, k + bit, k)
    return k


def power(k, sign):
    scale = jnp.ones_like(k)
    for bit in STEPS:
        has = k >= bit
        scale = jnp.where(has, scale * (2.0 ** (sign * bit)), scale)
        k = jnp.where(has, k - bit, k)
    return scale


def scales_of(most):
    k = exponents(jnp.max(jnp.max(most, axis=1, keepdims=True), axis=0, keepdims=True))
    return power(k, 1), k


def own_kernel(pair_ref, far_ref, out_ref, k_ref):
    x, zl = lax.axis_index("x"), lax.axis_index("zl")
    turns = (pair_ref.at[0], pair_ref.at[1], far_ref.at[0], far_ref.at[1])
    most = None
    for ref in turns:
        for n in range(32):
            value = jnp.abs(ref[:, 128 * n : 128 * (n + 1)].astype(jnp.float32))
            most = value if most is None else jnp.maximum(most, value)
    scale, k = scales_of(most)
    k_ref[...] = jnp.broadcast_to(k[None], (1, 8, 512)).astype(jnp.bfloat16)
    for turn, ref in enumerate(turns):
        place = lax.bitwise_xor(zl, turn)
        for s in range(1, 8):
            for z in range(2):
                at = pl.multiple_of(2048 * z + 256 * lax.bitwise_xor(x, s), 256)
                value = (ref[:, pl.ds(at, 256)].astype(jnp.float32) * scale).astype(jnp.bfloat16)
                out_ref[4 * (s - 1) + place, :, 256 * z : 256 * (z + 1)] = value


def rows_kernel(rows_ref, out_ref, k_ref):
    for b in range(4):
        cols = slice(128 * b, 128 * (b + 1))
        most = jnp.max(jnp.abs(rows_ref[:, :, cols].astype(jnp.float32)), axis=0)
        scale, k = scales_of(most)
        k_ref[0, :, cols] = jnp.broadcast_to(k, (8, 128)).astype(jnp.bfloat16)
        out_ref[:, :, cols] = (rows_ref[:, :, cols].astype(jnp.float32) * scale[None]).astype(jnp.bfloat16)


def scaled(kernel, blocks, ks, *rows):
    return pl.pallas_call(
        kernel,
        out_shape=(jax.ShapeDtypeStruct((blocks, 8, 512), jnp.bfloat16), jax.ShapeDtypeStruct((ks, 8, 512), jnp.bfloat16)),
        in_specs=[pl.BlockSpec(memory_space=pltpu.VMEM)] * len(rows),
        out_specs=(pl.BlockSpec(memory_space=pltpu.VMEM),) * 2,
        cost_estimate=pl.CostEstimate(flops=1_000_000, bytes_accessed=600_000, transcendentals=0),
        compiler_params=pltpu.CompilerParams(vmem_limit_bytes=4 << 20),
    )(*rows)


def hidden_kernel(gate_ref, up_ref, out_ref, gate_in, up_in, done, in_sem, out_sem):
    h = gate_ref.shape[0]
    part = h // 4 // 16 * 16
    bands = [pl.ds(n * part, part if n < 3 else h - 3 * part) for n in range(4)]
    loads = []
    for n, band in enumerate(bands):
        for i, (ref, into) in enumerate(((gate_ref, gate_in), (up_ref, up_in))):
            loads.append(pltpu.make_async_copy(ref.at[band, :], into.at[band, :], in_sem.at[n, i]))
            loads[-1].start()
    copies = []
    for n, band in enumerate(bands):
        loads[2 * n].wait()
        loads[2 * n + 1].wait()
        gate = gate_in[band, :].astype(jnp.float32)
        sig = jax.nn.sigmoid(gate)
        done[band, :] = ((gate * sig) * up_in[band, :].astype(jnp.float32)).astype(jnp.bfloat16)
        for i in range(8):
            copies.append(pltpu.make_async_copy(done.at[band, :], out_ref.at[i, band, :], out_sem.at[n, i]))
            copies[-1].start()
    for copy in copies:
        copy.wait()


def hidden_copies(gate, up):
    h, t = gate.shape
    return pl.pallas_call(
        hidden_kernel,
        out_shape=jax.ShapeDtypeStruct((8, h, t), jnp.bfloat16),
        in_specs=[pl.BlockSpec(memory_space=pltpu.HBM)] * 2,
        out_specs=pl.BlockSpec(memory_space=pl.ANY),
        scratch_shapes=[pltpu.VMEM((h, t), jnp.bfloat16)] * 3 + [pltpu.SemaphoreType.DMA((4, 2)), pltpu.SemaphoreType.DMA((4, 8))],
        cost_estimate=pl.CostEstimate(flops=2_000_000, bytes_accessed=10 * h * t * 2, transcendentals=h * t),
        compiler_params=pltpu.CompilerParams(vmem_limit_bytes=60 * 1024 * 1024),
        name="hidden_copies",
    )(gate, up)


def split_kernel(g_ref, out_ref, held, sem):
    zh, c = lax.axis_index("zh"), lax.axis_index("c")
    for x in range(8):
        for i, core in enumerate((1 - c, c)):
            for j, z in enumerate((1 - zh, zh)):
                at = pl.multiple_of(2048 * z + 256 * x + 128 * core, 128)
                piece = g_ref[:, pl.ds(at, 128)]
                for zl in range(4):
                    held[4 * x + zl, :, 256 * i + 128 * j : 256 * i + 128 * (j + 1)] = piece
    copy = pltpu.make_async_copy(held, out_ref, sem)
    copy.start()
    copy.wait()


def split_rows(g):
    return pl.pallas_call(
        split_kernel,
        out_shape=jax.ShapeDtypeStruct((32, 8, 512), jnp.bfloat16),
        in_specs=[pl.BlockSpec(memory_space=pltpu.VMEM)],
        out_specs=pl.BlockSpec(memory_space=pl.ANY),
        scratch_shapes=[pltpu.VMEM((32, 8, 512), jnp.bfloat16), pltpu.SemaphoreType.DMA],
        compiler_params=pltpu.CompilerParams(vmem_limit_bytes=2 << 20),
        name="split_rows",
    )(g)


def weights_kernel(hidden_ref, feats_ref, theirs_ref, ours_ref, held, sem):
    t = hidden_ref.shape[2]
    loads = [pltpu.make_async_copy(hidden_ref.at[i], held.at[:, t * i : t * (i + 1)], sem.at[i]) for i in range(8)]
    for load in loads:
        load.start()
    for i in range(0, 8, 2):
        loads[i].wait()
        loads[i + 1].wait()
        cols = slice(t * i, t * (i + 2))
        for n, ref in enumerate((theirs_ref, ours_ref)):
            part = jnp.dot(held[:, cols], feats_ref[cols, 256 * n : 256 * (n + 1)], preferred_element_type=jnp.float32)
            ref[...] = part if i == 0 else ref[...] + part


def weight_parts(hiddens, feats):
    _, h, t = hiddens.shape
    return pl.pallas_call(
        weights_kernel,
        out_shape=(jax.ShapeDtypeStruct((h, 256), jnp.float32),) * 2,
        in_specs=[pl.BlockSpec(memory_space=pltpu.HBM), pl.BlockSpec(memory_space=pltpu.VMEM)],
        out_specs=(pl.BlockSpec(memory_space=pltpu.VMEM),) * 2,
        scratch_shapes=[pltpu.VMEM((h, 8 * t), jnp.bfloat16), pltpu.SemaphoreType.DMA((8,))],
        cost_estimate=pl.CostEstimate(flops=2 * 8 * t * h * 512, bytes_accessed=4_000_000, transcendentals=0),
        compiler_params=pltpu.CompilerParams(vmem_limit_bytes=12 << 20),
        name="weight_parts",
    )(hiddens, feats)


def inputs_kernel(front_ref, last_ref, feats_ref, weight_ref, gate_ref, up_ref, grad_gate_ref, grad_up_ref, weight, total):
    zh, x, c = lax.axis_index("zh"), lax.axis_index("x"), lax.axis_index("c")
    t = gate_ref.shape[1]
    for n in range(8):
        slot = n % 2
        if n < 7:
            for z in range(2):
                at = pl.multiple_of(2048 * z + 256 * lax.bitwise_xor(x, n + 1), 256)
                weight[slot, :, 256 * z : 256 * (z + 1)] = weight_ref[:, pl.ds(at, 256)]
            rows = front_ref[n] if n < 5 else last_ref[n - 5]
        else:
            for i, core in enumerate((1 - c, c)):
                for j, z in enumerate((1 - zh, zh)):
                    at = pl.multiple_of(2048 * z + 256 * x + 128 * core, 128)
                    weight[slot, :, 256 * i + 128 * j : 256 * i + 128 * (j + 1)] = weight_ref[:, pl.ds(at, 128)]
            rows = feats_ref[pl.ds(pl.multiple_of(x * t, t), t), :]
        part = lax.dot_general(weight[slot], rows, (((1,), (1,)), ((), ())), preferred_element_type=jnp.float32)
        total[...] = part if n == 0 else total[...] + part
    grad_hidden = total[...]
    gate = gate_ref[...].astype(jnp.float32)
    upper = up_ref[...].astype(jnp.float32)
    sig = jax.nn.sigmoid(gate)
    grad_up_ref[...] = (grad_hidden * (gate * sig)).astype(jnp.bfloat16)
    grad_gate_ref[...] = (grad_hidden * upper * sig * (1.0 + gate * (1.0 - sig))).astype(jnp.bfloat16)


def input_grads(front, last, feats, weight, gate, up):
    h, t = gate.shape
    return pl.pallas_call(
        inputs_kernel,
        out_shape=(jax.ShapeDtypeStruct((h, t), jnp.bfloat16),) * 2,
        in_specs=[pl.BlockSpec(memory_space=pltpu.VMEM)] * 6,
        out_specs=(pl.BlockSpec(memory_space=pltpu.VMEM),) * 2,
        scratch_shapes=[pltpu.VMEM((2, h, 512), jnp.bfloat16), pltpu.VMEM((h, t), jnp.float32)],
        cost_estimate=pl.CostEstimate(flops=2 * h * t * 4096, bytes_accessed=6_000_000, transcendentals=h * t),
        compiler_params=pltpu.CompilerParams(vmem_limit_bytes=16 << 20),
        name="input_grads",
    )(front, last, feats, weight, gate, up)


def turned(x, axis, by):
    return lax.ppermute(x, axis, [(i, i ^ by) for i in range(lax.axis_size(axis))])


def sections(grad_out, gate_pre, up_pre, down_weight):
    gate_t, up_t = gate_pre.T, up_pre.T
    _, t = gate_t.shape

    pieces = split_rows(grad_out)
    mine = lax.all_to_all(pieces, ("x", "zl"), 0, 0)
    near = turned(grad_out, "zl", 1)
    pair = jnp.stack([grad_out, near])
    far = turned(pair, "zl", 2)
    copies = hidden_copies(gate_t, up_t)
    hiddens = lax.all_to_all(copies, "x", 0, 0)

    own, own_k = scaled(own_kernel, 28, 1, pair, far)
    rows, rows_k = scaled(rows_kernel, 32, 1, mine)
    message = jnp.concatenate([own, rows, own_k, rows_k], 0).astype(jnp.float16)
    got = lax.all_gather(message, "y", axis=1, tiled=True)

    scale = power(got[60:].astype(jnp.float32), -1)
    feats = (got[28:60].astype(jnp.float32) * scale[1]).astype(jnp.bfloat16).reshape(8 * t, 512)
    front = (got[:20].astype(jnp.float32) * scale[0]).astype(jnp.bfloat16).reshape(5, t, 512)
    last = (got[20:28].astype(jnp.float32) * scale[0]).astype(jnp.bfloat16).reshape(2, t, 512)

    theirs, ours = weight_parts(hiddens, feats)
    swap = lax.all_gather(theirs.astype(jnp.bfloat16), "c", axis=0)
    part = ours + lax.dynamic_index_in_dim(swap, 1 - lax.axis_index("c"), 0, keepdims=False).astype(jnp.float32)
    away = turned(part[:, :128].astype(jnp.bfloat16), "zh", 1)
    here = part[:, 128:]

    grad_gate, grad_up = input_grads(front, last, feats, down_weight.T, gate_t, up_t)
    return (here + away.astype(jnp.float32)).T, grad_gate.T, grad_up.T


def solution(mesh):
    dims = (2, 8, 2, 4, 8)
    fine = Mesh(mesh.devices.reshape(dims), AXES)
    dp, tensor = ("zh", "x", "c"), ("zl", "y")
    in_specs = (P(dp + tensor, None), P(dp, tensor), P(dp, tensor), P(None, tensor))
    out_specs = (P(dp, tensor), P(dp, tensor), P(dp, tensor))
    return jax.shard_map(sections, mesh=fine, in_specs=in_specs, out_specs=out_specs, check_vma=False)
```

```python
import jax
import jax.numpy as jnp
from jax import lax
from jax.experimental import pallas as pl
from jax.experimental.pallas import tpu as pltpu
from jax.sharding import Mesh, PartitionSpec as P


AXES = ("zh", "x", "c", "zl2", "zl1", "y")
STEPS = (64.0, 32.0, 16.0, 8.0, 4.0, 2.0)


def exponents(most):
    k = jnp.zeros_like(most)
    for bit in STEPS:
        fits = most * (2.0**bit) <= 32768.0
        most = jnp.where(fits, most * (2.0**bit), most)
        k = jnp.where(fits, k + bit, k)
    return k


def power(k, sign):
    scale = jnp.ones_like(k)
    for bit in STEPS:
        has = k >= bit
        scale = jnp.where(has, scale * (2.0 ** (sign * bit)), scale)
        k = jnp.where(has, k - bit, k)
    return scale


def scales_of(most):
    k = exponents(jnp.max(jnp.max(most, axis=1, keepdims=True), axis=0, keepdims=True))
    return power(k, 1), k


def pack_kernel(own_ref, near_ref, rows_ref, out_ref):
    x = lax.axis_index("x")
    for turn, ref in enumerate((own_ref, near_ref)):
        for s in range(1, 8):
            for z in range(2):
                at = pl.multiple_of(2048 * z + 256 * lax.bitwise_xor(x, s), 256)
                out_ref[7 * turn + s - 1, :, 256 * z : 256 * (z + 1)] = ref[:, pl.ds(at, 256)]
    out_ref[14:] = rows_ref[...]


def code_kernel(here_ref, far_ref, out_ref):
    zl2, zl1 = lax.axis_index("zl2"), lax.axis_index("zl1")
    sides = ((here_ref, 2 * zl2), (far_ref, 2 * (1 - zl2)))
    most = None
    for ref, _ in sides:
        for b in range(4):
            value = jnp.max(jnp.abs(ref[:14, :, 128 * b : 128 * (b + 1)].astype(jnp.float32)), axis=0)
            most = value if most is None else jnp.maximum(most, value)
    scale, k = scales_of(most)
    out_ref[60] = jnp.broadcast_to(k, (8, 512)).astype(jnp.bfloat16)
    for ref, first in sides:
        for turn in range(2):
            place = first + lax.bitwise_xor(zl1, turn)
            for s in range(7):
                out_ref[4 * s + place] = (ref[7 * turn + s].astype(jnp.float32) * scale).astype(jnp.bfloat16)
    for b in range(4):
        cols = slice(128 * b, 128 * (b + 1))
        values = [ref[14:, :, cols].astype(jnp.float32) for ref, _ in sides]
        scale, k = scales_of(jnp.max(jnp.maximum(jnp.abs(values[0]), jnp.abs(values[1])), axis=0))
        out_ref[61, :, cols] = jnp.broadcast_to(k, (8, 128)).astype(jnp.bfloat16)
        for value, (_, first) in zip(values, sides):
            for x in range(8):
                for i in range(2):
                    out_ref[28 + 4 * x + first + i, :, cols] = (value[2 * x + i] * scale).astype(jnp.bfloat16)


def in_vmem(kernel, blocks, *args):
    return pl.pallas_call(
        kernel,
        out_shape=jax.ShapeDtypeStruct((blocks, 8, 512), jnp.bfloat16),
        in_specs=[pl.BlockSpec(memory_space=pltpu.VMEM)] * len(args),
        out_specs=pl.BlockSpec(memory_space=pltpu.VMEM),
        cost_estimate=pl.CostEstimate(flops=1_000_000, bytes_accessed=600_000, transcendentals=0),
        compiler_params=pltpu.CompilerParams(vmem_limit_bytes=4 << 20),
    )(*args)


def hidden_kernel(gate_ref, up_ref, out_ref, gate_in, up_in, done, in_sem, out_sem):
    h = gate_ref.shape[0]
    part = h // 4 // 16 * 16
    bands = [pl.ds(n * part, part if n < 3 else h - 3 * part) for n in range(4)]
    loads = []
    for n, band in enumerate(bands):
        for i, (ref, into) in enumerate(((gate_ref, gate_in), (up_ref, up_in))):
            loads.append(pltpu.make_async_copy(ref.at[band, :], into.at[band, :], in_sem.at[n, i]))
            loads[-1].start()
    copies = []
    for n, band in enumerate(bands):
        loads[2 * n].wait()
        loads[2 * n + 1].wait()
        gate = gate_in[band, :].astype(jnp.float32)
        sig = jax.nn.sigmoid(gate)
        done[band, :] = ((gate * sig) * up_in[band, :].astype(jnp.float32)).astype(jnp.bfloat16)
        for i in range(8):
            copies.append(pltpu.make_async_copy(done.at[band, :], out_ref.at[i, band, :], out_sem.at[n, i]))
            copies[-1].start()
    for copy in copies:
        copy.wait()


def hidden_copies(gate, up):
    h, t = gate.shape
    return pl.pallas_call(
        hidden_kernel,
        out_shape=jax.ShapeDtypeStruct((8, h, t), jnp.bfloat16),
        in_specs=[pl.BlockSpec(memory_space=pltpu.HBM)] * 2,
        out_specs=pl.BlockSpec(memory_space=pl.ANY),
        scratch_shapes=[pltpu.VMEM((h, t), jnp.bfloat16)] * 3 + [pltpu.SemaphoreType.DMA((4, 2)), pltpu.SemaphoreType.DMA((4, 8))],
        cost_estimate=pl.CostEstimate(flops=2_000_000, bytes_accessed=10 * h * t * 2, transcendentals=h * t),
        compiler_params=pltpu.CompilerParams(vmem_limit_bytes=60 * 1024 * 1024),
        name="hidden_copies",
    )(gate, up)


def split_kernel(g_ref, out_ref, held, sem):
    zh, c = lax.axis_index("zh"), lax.axis_index("c")
    for x in range(8):
        for i, core in enumerate((1 - c, c)):
            for j, z in enumerate((1 - zh, zh)):
                at = pl.multiple_of(2048 * z + 256 * x + 128 * core, 128)
                piece = g_ref[:, pl.ds(at, 128)]
                for zl in range(2):
                    held[2 * x + zl, :, 256 * i + 128 * j : 256 * i + 128 * (j + 1)] = piece
    copy = pltpu.make_async_copy(held, out_ref, sem)
    copy.start()
    copy.wait()


def split_rows(g):
    return pl.pallas_call(
        split_kernel,
        out_shape=jax.ShapeDtypeStruct((16, 8, 512), jnp.bfloat16),
        in_specs=[pl.BlockSpec(memory_space=pltpu.VMEM)],
        out_specs=pl.BlockSpec(memory_space=pl.ANY),
        scratch_shapes=[pltpu.VMEM((16, 8, 512), jnp.bfloat16), pltpu.SemaphoreType.DMA],
        compiler_params=pltpu.CompilerParams(vmem_limit_bytes=2 << 20),
        name="split_rows",
    )(g)


def weights_kernel(hidden_ref, feats_ref, theirs_ref, ours_ref, held, sem):
    t = hidden_ref.shape[2]
    loads = [pltpu.make_async_copy(hidden_ref.at[i], held.at[:, t * i : t * (i + 1)], sem.at[i]) for i in range(8)]
    for load in loads:
        load.start()
    for i in range(0, 8, 2):
        loads[i].wait()
        loads[i + 1].wait()
        cols = slice(t * i, t * (i + 2))
        for n, ref in enumerate((theirs_ref, ours_ref)):
            part = jnp.dot(held[:, cols], feats_ref[cols, 256 * n : 256 * (n + 1)], preferred_element_type=jnp.float32)
            ref[...] = part if i == 0 else ref[...] + part


def weight_parts(hiddens, feats):
    _, h, t = hiddens.shape
    return pl.pallas_call(
        weights_kernel,
        out_shape=(jax.ShapeDtypeStruct((h, 256), jnp.float32),) * 2,
        in_specs=[pl.BlockSpec(memory_space=pltpu.HBM), pl.BlockSpec(memory_space=pltpu.VMEM)],
        out_specs=(pl.BlockSpec(memory_space=pltpu.VMEM),) * 2,
        scratch_shapes=[pltpu.VMEM((h, 8 * t), jnp.bfloat16), pltpu.SemaphoreType.DMA((8,))],
        cost_estimate=pl.CostEstimate(flops=2 * 8 * t * h * 512, bytes_accessed=4_000_000, transcendentals=0),
        compiler_params=pltpu.CompilerParams(vmem_limit_bytes=12 << 20),
        name="weight_parts",
    )(hiddens, feats)


def inputs_kernel(front_ref, last_ref, feats_ref, weight_ref, gate_ref, up_ref, grad_gate_ref, grad_up_ref, weight, total):
    zh, x, c = lax.axis_index("zh"), lax.axis_index("x"), lax.axis_index("c")
    t = gate_ref.shape[1]
    for n in range(8):
        slot = n % 2
        if n < 7:
            for z in range(2):
                at = pl.multiple_of(2048 * z + 256 * lax.bitwise_xor(x, n + 1), 256)
                weight[slot, :, 256 * z : 256 * (z + 1)] = weight_ref[:, pl.ds(at, 256)]
            rows = front_ref[n] if n < 5 else last_ref[n - 5]
        else:
            for i, core in enumerate((1 - c, c)):
                for j, z in enumerate((1 - zh, zh)):
                    at = pl.multiple_of(2048 * z + 256 * x + 128 * core, 128)
                    weight[slot, :, 256 * i + 128 * j : 256 * i + 128 * (j + 1)] = weight_ref[:, pl.ds(at, 128)]
            rows = feats_ref[pl.ds(pl.multiple_of(x * t, t), t), :]
        part = lax.dot_general(weight[slot], rows, (((1,), (1,)), ((), ())), preferred_element_type=jnp.float32)
        total[...] = part if n == 0 else total[...] + part
    grad_hidden = total[...]
    gate = gate_ref[...].astype(jnp.float32)
    upper = up_ref[...].astype(jnp.float32)
    sig = jax.nn.sigmoid(gate)
    grad_up_ref[...] = (grad_hidden * (gate * sig)).astype(jnp.bfloat16)
    grad_gate_ref[...] = (grad_hidden * upper * sig * (1.0 + gate * (1.0 - sig))).astype(jnp.bfloat16)


def input_grads(front, last, feats, weight, gate, up):
    h, t = gate.shape
    return pl.pallas_call(
        inputs_kernel,
        out_shape=(jax.ShapeDtypeStruct((h, t), jnp.bfloat16),) * 2,
        in_specs=[pl.BlockSpec(memory_space=pltpu.VMEM)] * 6,
        out_specs=(pl.BlockSpec(memory_space=pltpu.VMEM),) * 2,
        scratch_shapes=[pltpu.VMEM((2, h, 512), jnp.bfloat16), pltpu.VMEM((h, t), jnp.float32)],
        cost_estimate=pl.CostEstimate(flops=2 * h * t * 4096, bytes_accessed=6_000_000, transcendentals=h * t),
        compiler_params=pltpu.CompilerParams(vmem_limit_bytes=16 << 20),
        name="input_grads",
    )(front, last, feats, weight, gate, up)


def turned(x, axis, by):
    return lax.ppermute(x, axis, [(i, i ^ by) for i in range(lax.axis_size(axis))])


def sections(grad_out, gate_pre, up_pre, down_weight):
    gate_t, up_t = gate_pre.T, up_pre.T
    _, t = gate_t.shape

    pieces = split_rows(grad_out)
    mine = lax.all_to_all(pieces, ("x", "zl1"), 0, 0)
    near = turned(grad_out, "zl1", 1)
    copies = hidden_copies(gate_t, up_t)
    packed = in_vmem(pack_kernel, 30, grad_out, near, mine)
    far = turned(packed, "zl2", 1)
    hiddens = lax.all_to_all(copies, "x", 0, 0)

    message = in_vmem(code_kernel, 62, packed, far).astype(jnp.float16)
    got = lax.all_gather(message, "y", axis=1, tiled=True)

    scale = power(got[60:].astype(jnp.float32), -1)
    feats = (got[28:60].astype(jnp.float32) * scale[1]).astype(jnp.bfloat16).reshape(8 * t, 512)
    front = (got[:20].astype(jnp.float32) * scale[0]).astype(jnp.bfloat16).reshape(5, t, 512)
    last = (got[20:28].astype(jnp.float32) * scale[0]).astype(jnp.bfloat16).reshape(2, t, 512)

    theirs, ours = weight_parts(hiddens, feats)
    swap = lax.all_gather(theirs.astype(jnp.bfloat16), "c", axis=0)
    part = ours + lax.dynamic_index_in_dim(swap, 1 - lax.axis_index("c"), 0, keepdims=False).astype(jnp.float32)
    away = turned(part[:, :128].astype(jnp.bfloat16), "zh", 1)
    here = part[:, 128:]

    grad_gate, grad_up = input_grads(front, last, feats, down_weight.T, gate_t, up_t)
    return (here + away.astype(jnp.float32)).T, grad_gate.T, grad_up.T


def solution(mesh):
    dims = (2, 8, 2, 2, 2, 8)
    fine = Mesh(mesh.devices.reshape(dims), AXES)
    dp, tensor = ("zh", "x", "c"), ("zl2", "zl1", "y")
    in_specs = (P(dp + tensor, None), P(dp, tensor), P(dp, tensor), P(None, tensor))
    out_specs = (P(dp, tensor), P(dp, tensor), P(dp, tensor))
    return jax.shard_map(sections, mesh=fine, in_specs=in_specs, out_specs=out_specs, check_vma=False)
```

```python
import jax
import jax.numpy as jnp
from jax import lax
from jax.experimental import pallas as pl
from jax.experimental.pallas import tpu as pltpu
from jax.sharding import Mesh, PartitionSpec as P


AXES = ("zh", "x", "c", "zl2", "zl1", "y")
STEPS = (64.0, 32.0, 16.0, 8.0, 4.0, 2.0)


def exponents(most):
    k = jnp.zeros_like(most)
    for bit in STEPS:
        fits = most * (2.0**bit) <= 32768.0
        most = jnp.where(fits, most * (2.0**bit), most)
        k = jnp.where(fits, k + bit, k)
    return k


def power(k, sign):
    scale = jnp.ones_like(k)
    for bit in STEPS:
        has = k >= bit
        scale = jnp.where(has, scale * (2.0 ** (sign * bit)), scale)
        k = jnp.where(has, k - bit, k)
    return scale


def scales_of(most):
    k = exponents(jnp.max(jnp.max(most, axis=1, keepdims=True), axis=0, keepdims=True))
    return power(k, 1), k


def pack_kernel(own_ref, near_ref, rows_ref, out_ref):
    x = lax.axis_index("x")
    for turn, ref in enumerate((own_ref, near_ref)):
        for s in range(1, 8):
            for z in range(2):
                at = pl.multiple_of(2048 * z + 256 * lax.bitwise_xor(x, s), 256)
                out_ref[7 * turn + s - 1, :, 256 * z : 256 * (z + 1)] = ref[:, pl.ds(at, 256)]
    out_ref[14:] = rows_ref[...]


def code_kernel(here_ref, far_ref, out_ref):
    zl2, zl1 = lax.axis_index("zl2"), lax.axis_index("zl1")
    sides = ((here_ref, zl1), (far_ref, 1 - zl1))
    most = None
    for ref, _ in sides:
        for b in range(4):
            value = jnp.max(jnp.abs(ref[:14, :, 128 * b : 128 * (b + 1)].astype(jnp.float32)), axis=0)
            most = value if most is None else jnp.maximum(most, value)
    scale, k = scales_of(most)
    out_ref[60] = jnp.broadcast_to(k, (8, 512)).astype(jnp.bfloat16)
    for ref, first in sides:
        for turn in range(2):
            place = first + 2 * lax.bitwise_xor(zl2, turn)
            for s in range(7):
                out_ref[4 * s + place] = (ref[7 * turn + s].astype(jnp.float32) * scale).astype(jnp.bfloat16)
    for b in range(4):
        cols = slice(128 * b, 128 * (b + 1))
        values = [ref[14:, :, cols].astype(jnp.float32) for ref, _ in sides]
        scale, k = scales_of(jnp.max(jnp.maximum(jnp.abs(values[0]), jnp.abs(values[1])), axis=0))
        out_ref[61, :, cols] = jnp.broadcast_to(k, (8, 128)).astype(jnp.bfloat16)
        for value, (_, first) in zip(values, sides):
            for x in range(8):
                for i in range(2):
                    out_ref[28 + 4 * x + first + 2 * i, :, cols] = (value[2 * x + i] * scale).astype(jnp.bfloat16)


def in_vmem(kernel, blocks, *args):
    return pl.pallas_call(
        kernel,
        out_shape=jax.ShapeDtypeStruct((blocks, 8, 512), jnp.bfloat16),
        in_specs=[pl.BlockSpec(memory_space=pltpu.VMEM)] * len(args),
        out_specs=pl.BlockSpec(memory_space=pltpu.VMEM),
        cost_estimate=pl.CostEstimate(flops=1_000_000, bytes_accessed=600_000, transcendentals=0),
        compiler_params=pltpu.CompilerParams(vmem_limit_bytes=4 << 20),
    )(*args)


def hidden_kernel(gate_ref, up_ref, out_ref, gate_in, up_in, done, in_sem, out_sem):
    h = gate_ref.shape[0]
    part = h // 4 // 16 * 16
    bands = [pl.ds(n * part, part if n < 3 else h - 3 * part) for n in range(4)]
    loads = []
    for n, band in enumerate(bands):
        for i, (ref, into) in enumerate(((gate_ref, gate_in), (up_ref, up_in))):
            loads.append(pltpu.make_async_copy(ref.at[band, :], into.at[band, :], in_sem.at[n, i]))
            loads[-1].start()
    copies = []
    for n, band in enumerate(bands):
        loads[2 * n].wait()
        loads[2 * n + 1].wait()
        gate = gate_in[band, :].astype(jnp.float32)
        sig = jax.nn.sigmoid(gate)
        done[band, :] = ((gate * sig) * up_in[band, :].astype(jnp.float32)).astype(jnp.bfloat16)
        for i in range(8):
            copies.append(pltpu.make_async_copy(done.at[band, :], out_ref.at[i, band, :], out_sem.at[n, i]))
            copies[-1].start()
    for copy in copies:
        copy.wait()


def hidden_copies(gate, up):
    h, t = gate.shape
    return pl.pallas_call(
        hidden_kernel,
        out_shape=jax.ShapeDtypeStruct((8, h, t), jnp.bfloat16),
        in_specs=[pl.BlockSpec(memory_space=pltpu.HBM)] * 2,
        out_specs=pl.BlockSpec(memory_space=pl.ANY),
        scratch_shapes=[pltpu.VMEM((h, t), jnp.bfloat16)] * 3 + [pltpu.SemaphoreType.DMA((4, 2)), pltpu.SemaphoreType.DMA((4, 8))],
        cost_estimate=pl.CostEstimate(flops=2_000_000, bytes_accessed=10 * h * t * 2, transcendentals=h * t),
        compiler_params=pltpu.CompilerParams(vmem_limit_bytes=60 * 1024 * 1024),
        name="hidden_copies",
    )(gate, up)


def split_kernel(g_ref, out_ref, held, sem):
    zh, c = lax.axis_index("zh"), lax.axis_index("c")
    for x in range(8):
        for i, core in enumerate((1 - c, c)):
            for j, z in enumerate((1 - zh, zh)):
                at = pl.multiple_of(2048 * z + 256 * x + 128 * core, 128)
                piece = g_ref[:, pl.ds(at, 128)]
                for zl in range(2):
                    held[2 * x + zl, :, 256 * i + 128 * j : 256 * i + 128 * (j + 1)] = piece
    copy = pltpu.make_async_copy(held, out_ref, sem)
    copy.start()
    copy.wait()


def split_rows(g):
    return pl.pallas_call(
        split_kernel,
        out_shape=jax.ShapeDtypeStruct((16, 8, 512), jnp.bfloat16),
        in_specs=[pl.BlockSpec(memory_space=pltpu.VMEM)],
        out_specs=pl.BlockSpec(memory_space=pl.ANY),
        scratch_shapes=[pltpu.VMEM((16, 8, 512), jnp.bfloat16), pltpu.SemaphoreType.DMA],
        compiler_params=pltpu.CompilerParams(vmem_limit_bytes=2 << 20),
        name="split_rows",
    )(g)


def weights_kernel(hidden_ref, feats_ref, theirs_ref, ours_ref, held, sem):
    t = hidden_ref.shape[2]
    loads = [pltpu.make_async_copy(hidden_ref.at[i], held.at[:, t * i : t * (i + 1)], sem.at[i]) for i in range(8)]
    for load in loads:
        load.start()
    for i in range(0, 8, 2):
        loads[i].wait()
        loads[i + 1].wait()
        cols = slice(t * i, t * (i + 2))
        for n, ref in enumerate((theirs_ref, ours_ref)):
            part = jnp.dot(held[:, cols], feats_ref[cols, 256 * n : 256 * (n + 1)], preferred_element_type=jnp.float32)
            ref[...] = part if i == 0 else ref[...] + part


def weight_parts(hiddens, feats):
    _, h, t = hiddens.shape
    return pl.pallas_call(
        weights_kernel,
        out_shape=(jax.ShapeDtypeStruct((h, 256), jnp.float32),) * 2,
        in_specs=[pl.BlockSpec(memory_space=pltpu.HBM), pl.BlockSpec(memory_space=pltpu.VMEM)],
        out_specs=(pl.BlockSpec(memory_space=pltpu.VMEM),) * 2,
        scratch_shapes=[pltpu.VMEM((h, 8 * t), jnp.bfloat16), pltpu.SemaphoreType.DMA((8,))],
        cost_estimate=pl.CostEstimate(flops=2 * 8 * t * h * 512, bytes_accessed=4_000_000, transcendentals=0),
        compiler_params=pltpu.CompilerParams(vmem_limit_bytes=12 << 20),
        name="weight_parts",
    )(hiddens, feats)


def inputs_kernel(front_ref, last_ref, feats_ref, weight_ref, gate_ref, up_ref, grad_gate_ref, grad_up_ref, weight, total):
    zh, x, c = lax.axis_index("zh"), lax.axis_index("x"), lax.axis_index("c")
    t = gate_ref.shape[1]
    for n in range(8):
        slot = n % 2
        if n < 7:
            for z in range(2):
                at = pl.multiple_of(2048 * z + 256 * lax.bitwise_xor(x, n + 1), 256)
                weight[slot, :, 256 * z : 256 * (z + 1)] = weight_ref[:, pl.ds(at, 256)]
            rows = front_ref[n] if n < 5 else last_ref[n - 5]
        else:
            for i, core in enumerate((1 - c, c)):
                for j, z in enumerate((1 - zh, zh)):
                    at = pl.multiple_of(2048 * z + 256 * x + 128 * core, 128)
                    weight[slot, :, 256 * i + 128 * j : 256 * i + 128 * (j + 1)] = weight_ref[:, pl.ds(at, 128)]
            rows = feats_ref[pl.ds(pl.multiple_of(x * t, t), t), :]
        part = lax.dot_general(weight[slot], rows, (((1,), (1,)), ((), ())), preferred_element_type=jnp.float32)
        total[...] = part if n == 0 else total[...] + part
    grad_hidden = total[...]
    gate = gate_ref[...].astype(jnp.float32)
    upper = up_ref[...].astype(jnp.float32)
    sig = jax.nn.sigmoid(gate)
    grad_up_ref[...] = (grad_hidden * (gate * sig)).astype(jnp.bfloat16)
    grad_gate_ref[...] = (grad_hidden * upper * sig * (1.0 + gate * (1.0 - sig))).astype(jnp.bfloat16)


def input_grads(front, last, feats, weight, gate, up):
    h, t = gate.shape
    return pl.pallas_call(
        inputs_kernel,
        out_shape=(jax.ShapeDtypeStruct((h, t), jnp.bfloat16),) * 2,
        in_specs=[pl.BlockSpec(memory_space=pltpu.VMEM)] * 6,
        out_specs=(pl.BlockSpec(memory_space=pltpu.VMEM),) * 2,
        scratch_shapes=[pltpu.VMEM((2, h, 512), jnp.bfloat16), pltpu.VMEM((h, t), jnp.float32)],
        cost_estimate=pl.CostEstimate(flops=2 * h * t * 4096, bytes_accessed=6_000_000, transcendentals=h * t),
        compiler_params=pltpu.CompilerParams(vmem_limit_bytes=16 << 20),
        name="input_grads",
    )(front, last, feats, weight, gate, up)


def turned(x, axis, by):
    return lax.ppermute(x, axis, [(i, i ^ by) for i in range(lax.axis_size(axis))])


def sections(grad_out, gate_pre, up_pre, down_weight):
    gate_t, up_t = gate_pre.T, up_pre.T
    _, t = gate_t.shape

    pieces = split_rows(grad_out)
    mine = lax.all_to_all(pieces, ("x", "zl2"), 0, 0)
    near = turned(grad_out, "zl2", 1)
    copies = hidden_copies(gate_t, up_t)
    packed = in_vmem(pack_kernel, 30, grad_out, near, mine)
    far = turned(packed, "zl1", 1)
    hiddens = lax.all_to_all(copies, "x", 0, 0)

    message = in_vmem(code_kernel, 62, packed, far).astype(jnp.float16)
    got = lax.all_gather(message, "y", axis=1, tiled=True)

    scale = power(got[60:].astype(jnp.float32), -1)
    feats = (got[28:60].astype(jnp.float32) * scale[1]).astype(jnp.bfloat16).reshape(8 * t, 512)
    front = (got[:20].astype(jnp.float32) * scale[0]).astype(jnp.bfloat16).reshape(5, t, 512)
    last = (got[20:28].astype(jnp.float32) * scale[0]).astype(jnp.bfloat16).reshape(2, t, 512)

    theirs, ours = weight_parts(hiddens, feats)
    swap = lax.all_gather(theirs.astype(jnp.bfloat16), "c", axis=0)
    part = ours + lax.dynamic_index_in_dim(swap, 1 - lax.axis_index("c"), 0, keepdims=False).astype(jnp.float32)
    away = turned(part[:, :128].astype(jnp.bfloat16), "zh", 1)
    here = part[:, 128:]

    grad_gate, grad_up = input_grads(front, last, feats, down_weight.T, gate_t, up_t)
    return (here + away.astype(jnp.float32)).T, grad_gate.T, grad_up.T


def solution(mesh):
    dims = (2, 8, 2, 2, 2, 8)
    fine = Mesh(mesh.devices.reshape(dims), AXES)
    dp, tensor = ("zh", "x", "c"), ("zl2", "zl1", "y")
    in_specs = (P(dp + tensor, None), P(dp, tensor), P(dp, tensor), P(None, tensor))
    out_specs = (P(dp, tensor), P(dp, tensor), P(dp, tensor))
    return jax.shard_map(sections, mesh=fine, in_specs=in_specs, out_specs=out_specs, check_vma=False)
```

```python
import jax
import jax.numpy as jnp
from jax import lax
from jax.experimental import pallas as pl
from jax.experimental.pallas import tpu as pltpu
from jax.sharding import Mesh, PartitionSpec as P


AXES = ("zh", "x", "c", "zl2", "zl1", "y")
STEPS = (64.0, 32.0, 16.0, 8.0, 4.0, 2.0)


def exponents(most):
    k = jnp.zeros_like(most)
    for bit in STEPS:
        fits = most * (2.0**bit) <= 32768.0
        most = jnp.where(fits, most * (2.0**bit), most)
        k = jnp.where(fits, k + bit, k)
    return k


def power(k, sign):
    scale = jnp.ones_like(k)
    for bit in STEPS:
        has = k >= bit
        scale = jnp.where(has, scale * (2.0 ** (sign * bit)), scale)
        k = jnp.where(has, k - bit, k)
    return scale


def scales_of(most):
    k = exponents(jnp.max(jnp.max(most, axis=1, keepdims=True), axis=0, keepdims=True))
    return power(k, 1), k


def pack_kernel(own_ref, near_ref, rows_ref, out_ref):
    x = lax.axis_index("x")
    for turn, ref in enumerate((own_ref, near_ref)):
        for s in range(1, 8):
            for z in range(2):
                at = pl.multiple_of(2048 * z + 256 * lax.bitwise_xor(x, s), 256)
                out_ref[7 * turn + s - 1, :, 256 * z : 256 * (z + 1)] = ref[:, pl.ds(at, 256)]
    out_ref[14:] = rows_ref[...]


def code_kernel(here_ref, far_ref, out_ref):
    zl2, zl1 = lax.axis_index("zl2"), lax.axis_index("zl1")
    sides = ((here_ref, zl1), (far_ref, 1 - zl1))
    most = None
    for ref, _ in sides:
        for b in range(4):
            value = jnp.max(jnp.abs(ref[:14, :, 128 * b : 128 * (b + 1)].astype(jnp.float32)), axis=0)
            most = value if most is None else jnp.maximum(most, value)
    scale, k = scales_of(most)
    out_ref[60] = jnp.broadcast_to(k, (8, 512)).astype(jnp.bfloat16)
    for ref, first in sides:
        for turn in range(2):
            place = first + 2 * lax.bitwise_xor(zl2, turn)
            for s in range(7):
                out_ref[4 * s + place] = (ref[7 * turn + s].astype(jnp.float32) * scale).astype(jnp.bfloat16)
    for b in range(4):
        cols = slice(128 * b, 128 * (b + 1))
        values = [ref[14:, :, cols].astype(jnp.float32) for ref, _ in sides]
        scale, k = scales_of(jnp.max(jnp.maximum(jnp.abs(values[0]), jnp.abs(values[1])), axis=0))
        out_ref[61, :, cols] = jnp.broadcast_to(k, (8, 128)).astype(jnp.bfloat16)
        for value, (_, first) in zip(values, sides):
            for x in range(8):
                for i in range(2):
                    out_ref[28 + 4 * x + first + 2 * i, :, cols] = (value[2 * x + i] * scale).astype(jnp.bfloat16)


def in_vmem(kernel, blocks, *args):
    return pl.pallas_call(
        kernel,
        out_shape=jax.ShapeDtypeStruct((blocks, 8, 512), jnp.bfloat16),
        in_specs=[pl.BlockSpec(memory_space=pltpu.VMEM)] * len(args),
        out_specs=pl.BlockSpec(memory_space=pltpu.VMEM),
        cost_estimate=pl.CostEstimate(flops=1_000_000, bytes_accessed=600_000, transcendentals=0),
        compiler_params=pltpu.CompilerParams(vmem_limit_bytes=4 << 20),
    )(*args)


def hidden_kernel(gate_ref, up_ref, out_ref, gate_in, up_in, done, in_sem, out_sem):
    h = gate_ref.shape[0]
    part = h // 4 // 16 * 16
    bands = [pl.ds(n * part, part if n < 3 else h - 3 * part) for n in range(4)]
    loads = []
    for n, band in enumerate(bands):
        for i, (ref, into) in enumerate(((gate_ref, gate_in), (up_ref, up_in))):
            loads.append(pltpu.make_async_copy(ref.at[band, :], into.at[band, :], in_sem.at[n, i]))
            loads[-1].start()
    copies = []
    for n, band in enumerate(bands):
        loads[2 * n].wait()
        loads[2 * n + 1].wait()
        gate = gate_in[band, :].astype(jnp.float32)
        sig = jax.nn.sigmoid(gate)
        done[band, :] = ((gate * sig) * up_in[band, :].astype(jnp.float32)).astype(jnp.bfloat16)
        for i in range(8):
            copies.append(pltpu.make_async_copy(done.at[band, :], out_ref.at[i, band, :], out_sem.at[n, i]))
            copies[-1].start()
    for copy in copies:
        copy.wait()


def hidden_copies(gate, up):
    h, t = gate.shape
    return pl.pallas_call(
        hidden_kernel,
        out_shape=jax.ShapeDtypeStruct((8, h, t), jnp.bfloat16),
        in_specs=[pl.BlockSpec(memory_space=pltpu.HBM)] * 2,
        out_specs=pl.BlockSpec(memory_space=pl.ANY),
        scratch_shapes=[pltpu.VMEM((h, t), jnp.bfloat16)] * 3 + [pltpu.SemaphoreType.DMA((4, 2)), pltpu.SemaphoreType.DMA((4, 8))],
        cost_estimate=pl.CostEstimate(flops=2_000_000, bytes_accessed=10 * h * t * 2, transcendentals=h * t),
        compiler_params=pltpu.CompilerParams(vmem_limit_bytes=60 * 1024 * 1024),
        name="hidden_copies",
    )(gate, up)


def split_kernel(g_ref, out_ref, held, sem):
    zh, c = lax.axis_index("zh"), lax.axis_index("c")
    for x in range(8):
        for i, core in enumerate((1 - c, c)):
            for j, z in enumerate((1 - zh, zh)):
                at = pl.multiple_of(2048 * z + 256 * x + 128 * core, 128)
                piece = g_ref[:, pl.ds(at, 128)]
                for zl in range(2):
                    held[2 * x + zl, :, 256 * i + 128 * j : 256 * i + 128 * (j + 1)] = piece
    copy = pltpu.make_async_copy(held, out_ref, sem)
    copy.start()
    copy.wait()


def split_rows(g):
    return pl.pallas_call(
        split_kernel,
        out_shape=jax.ShapeDtypeStruct((16, 8, 512), jnp.bfloat16),
        in_specs=[pl.BlockSpec(memory_space=pltpu.VMEM)],
        out_specs=pl.BlockSpec(memory_space=pl.ANY),
        scratch_shapes=[pltpu.VMEM((16, 8, 512), jnp.bfloat16), pltpu.SemaphoreType.DMA],
        compiler_params=pltpu.CompilerParams(vmem_limit_bytes=2 << 20),
        name="split_rows",
    )(g)


def weights_kernel(hidden_ref, feats_ref, theirs_ref, ours_ref, held, sem):
    t = hidden_ref.shape[2]
    loads = [pltpu.make_async_copy(hidden_ref.at[i], held.at[:, t * i : t * (i + 1)], sem.at[i]) for i in range(8)]
    for load in loads:
        load.start()
    for i in range(0, 8, 2):
        loads[i].wait()
        loads[i + 1].wait()
        cols = slice(t * i, t * (i + 2))
        for n, ref in enumerate((theirs_ref, ours_ref)):
            part = jnp.dot(held[:, cols], feats_ref[cols, 256 * n : 256 * (n + 1)], preferred_element_type=jnp.float32)
            ref[...] = part if i == 0 else ref[...] + part


def weight_parts(hiddens, feats):
    _, h, t = hiddens.shape
    return pl.pallas_call(
        weights_kernel,
        out_shape=(jax.ShapeDtypeStruct((h, 256), jnp.float32),) * 2,
        in_specs=[pl.BlockSpec(memory_space=pltpu.HBM), pl.BlockSpec(memory_space=pltpu.VMEM)],
        out_specs=(pl.BlockSpec(memory_space=pltpu.VMEM),) * 2,
        scratch_shapes=[pltpu.VMEM((h, 8 * t), jnp.bfloat16), pltpu.SemaphoreType.DMA((8,))],
        cost_estimate=pl.CostEstimate(flops=2 * 8 * t * h * 512, bytes_accessed=4_000_000, transcendentals=0),
        compiler_params=pltpu.CompilerParams(vmem_limit_bytes=12 << 20),
        name="weight_parts",
    )(hiddens, feats)


def input_grads(front_ref, last_ref, feats_ref, weight_ref, gate_ref, up_ref, grads, weight, total, done, sem):
    zh, x, c = lax.axis_index("zh"), lax.axis_index("x"), lax.axis_index("c")
    t = gate_ref.shape[1]
    for n in range(8):
        slot = n % 2
        if n < 7:
            for z in range(2):
                at = pl.multiple_of(2048 * z + 256 * lax.bitwise_xor(x, n + 1), 256)
                weight[slot, :, 256 * z : 256 * (z + 1)] = weight_ref[:, pl.ds(at, 256)]
            rows = front_ref[n] if n < 5 else last_ref[n - 5]
        else:
            for i, core in enumerate((1 - c, c)):
                for j, z in enumerate((1 - zh, zh)):
                    at = pl.multiple_of(2048 * z + 256 * x + 128 * core, 128)
                    weight[slot, :, 256 * i + 128 * j : 256 * i + 128 * (j + 1)] = weight_ref[:, pl.ds(at, 128)]
            rows = feats_ref[pl.ds(pl.multiple_of(x * t, t), t), :]
        part = lax.dot_general(weight[slot], rows, (((1,), (1,)), ((), ())), preferred_element_type=jnp.float32)
        total[...] = part if n == 0 else total[...] + part
    grad_hidden = total[...]
    gate = gate_ref[...].astype(jnp.float32)
    upper = up_ref[...].astype(jnp.float32)
    sig = jax.nn.sigmoid(gate)
    done[0] = (grad_hidden * upper * sig * (1.0 + gate * (1.0 - sig))).astype(jnp.bfloat16)
    done[1] = (grad_hidden * (gate * sig)).astype(jnp.bfloat16)
    copies = [pltpu.make_async_copy(done.at[i], grads[i], sem.at[i]) for i in range(2)]
    for copy in copies:
        copy.start()
    for copy in copies:
        copy.wait()


def before_kernel(ours_ref, swap_ref, *refs):
    inputs, (send_ref, here_ref), grads, scratch = refs[:6], refs[6:8], refs[8:10], refs[10:]
    other = 1 - lax.axis_index("c")
    send_ref[...] = (ours_ref[:, :128] + swap_ref[other, :, :128].astype(jnp.float32)).astype(jnp.bfloat16)
    here_ref[...] = ours_ref[:, 128:] + swap_ref[other, :, 128:].astype(jnp.float32)
    pl.when(lax.axis_index("zh") == 0)(lambda: input_grads(*inputs, grads, *scratch))


def after_kernel(here_ref, both_ref, *refs):
    inputs, sum_ref, grads, scratch = refs[:6], refs[8], refs[9:11], refs[11:]
    zh = lax.axis_index("zh")
    sum_ref[...] = here_ref[...] + both_ref[1 - zh].astype(jnp.float32)
    pl.when(zh == 1)(lambda: input_grads(*inputs, grads, *scratch))


def with_grads(kernel, terms, inputs, grads, outs):
    h, t = inputs[-1].shape
    vmem, anywhere = pl.BlockSpec(memory_space=pltpu.VMEM), pl.BlockSpec(memory_space=pl.ANY)
    args = terms + inputs + grads
    return pl.pallas_call(
        kernel,
        out_shape=tuple(jax.ShapeDtypeStruct((h, 128), dtype) for dtype in outs) + (jax.ShapeDtypeStruct((h, t), jnp.bfloat16),) * 2,
        in_specs=[vmem] * len(terms + inputs) + [anywhere] * len(grads),
        out_specs=(vmem,) * len(outs) + (anywhere,) * 2,
        input_output_aliases={len(terms + inputs) + i: len(outs) + i for i in range(len(grads))},
        scratch_shapes=[
            pltpu.VMEM((2, h, 512), jnp.bfloat16),
            pltpu.VMEM((h, t), jnp.float32),
            pltpu.VMEM((2, h, t), jnp.bfloat16),
            pltpu.SemaphoreType.DMA((2,)),
        ],
        cost_estimate=pl.CostEstimate(flops=2 * h * t * 4096, bytes_accessed=6_000_000, transcendentals=h * t),
        compiler_params=pltpu.CompilerParams(vmem_limit_bytes=16 << 20),
    )(*args)


def turned(x, axis, by):
    return lax.ppermute(x, axis, [(i, i ^ by) for i in range(lax.axis_size(axis))])


def sections(grad_out, gate_pre, up_pre, down_weight):
    gate_t, up_t = gate_pre.T, up_pre.T
    _, t = gate_t.shape

    pieces = split_rows(grad_out)
    mine = lax.all_to_all(pieces, ("x", "zl2"), 0, 0)
    near = turned(grad_out, "zl2", 1)
    copies = hidden_copies(gate_t, up_t)
    packed = in_vmem(pack_kernel, 30, grad_out, near, mine)
    far = turned(packed, "zl1", 1)
    hiddens = lax.all_to_all(copies, "x", 0, 0)

    message = in_vmem(code_kernel, 62, packed, far).astype(jnp.float16)
    got = lax.all_gather(message, "y", axis=1, tiled=True)

    scale = power(got[60:].astype(jnp.float32), -1)
    feats = (got[28:60].astype(jnp.float32) * scale[1]).astype(jnp.bfloat16).reshape(8 * t, 512)
    front = (got[:20].astype(jnp.float32) * scale[0]).astype(jnp.bfloat16).reshape(5, t, 512)
    last = (got[20:28].astype(jnp.float32) * scale[0]).astype(jnp.bfloat16).reshape(2, t, 512)

    theirs, ours = weight_parts(hiddens, feats)
    swap = lax.all_gather(theirs.astype(jnp.bfloat16), "c", axis=0)
    inputs = (front, last, feats, down_weight.T, gate_t, up_t)
    send, here, *grads = with_grads(before_kernel, (ours, swap), inputs, (), (jnp.bfloat16, jnp.float32))
    both = lax.all_gather(send, "zh", axis=0)
    total, grad_gate, grad_up = with_grads(after_kernel, (here, both), inputs, tuple(grads), (jnp.float32,))
    return total.T, grad_gate.T, grad_up.T


def solution(mesh):
    dims = (2, 8, 2, 2, 2, 8)
    fine = Mesh(mesh.devices.reshape(dims), AXES)
    dp, tensor = ("zh", "x", "c"), ("zl2", "zl1", "y")
    in_specs = (P(dp + tensor, None), P(dp, tensor), P(dp, tensor), P(None, tensor))
    out_specs = (P(dp, tensor), P(dp, tensor), P(dp, tensor))
    return jax.shard_map(sections, mesh=fine, in_specs=in_specs, out_specs=out_specs, check_vma=False)
```

```python
import jax
import jax.numpy as jnp
from jax import lax
from jax.experimental import pallas as pl
from jax.experimental.pallas import tpu as pltpu
from jax.sharding import Mesh, PartitionSpec as P


AXES = ("zh", "x", "c", "zl2", "zl1", "y")
STEPS = (64.0, 32.0, 16.0, 8.0, 4.0, 2.0)


def exponents(most):
    k = jnp.zeros_like(most)
    for bit in STEPS:
        fits = most * (2.0**bit) <= 32768.0
        most = jnp.where(fits, most * (2.0**bit), most)
        k = jnp.where(fits, k + bit, k)
    return k


def power(k, sign):
    scale = jnp.ones_like(k)
    for bit in STEPS:
        has = k >= bit
        scale = jnp.where(has, scale * (2.0 ** (sign * bit)), scale)
        k = jnp.where(has, k - bit, k)
    return scale


def scales_of(most):
    k = exponents(jnp.max(jnp.max(most, axis=1, keepdims=True), axis=0, keepdims=True))
    return power(k, 1), k


def pack_kernel(own_ref, near_ref, rows_ref, out_ref):
    out_ref[:7] = own_ref[...]
    out_ref[7:14] = near_ref[...]
    out_ref[14:] = rows_ref[...]


def code_kernel(here_ref, far_ref, out_ref):
    zl2, zl1 = lax.axis_index("zl2"), lax.axis_index("zl1")
    sides = ((here_ref, zl1), (far_ref, 1 - zl1))
    most = None
    for ref, _ in sides:
        for b in range(4):
            value = jnp.max(jnp.abs(ref[:14, :, 128 * b : 128 * (b + 1)].astype(jnp.float32)), axis=0)
            most = value if most is None else jnp.maximum(most, value)
    scale, k = scales_of(most)
    out_ref[60] = jnp.broadcast_to(k, (8, 512)).astype(jnp.bfloat16)
    for ref, first in sides:
        for turn in range(2):
            place = first + 2 * lax.bitwise_xor(zl2, turn)
            for s in range(7):
                out_ref[4 * s + place] = (ref[7 * turn + s].astype(jnp.float32) * scale).astype(jnp.bfloat16)
    for b in range(4):
        cols = slice(128 * b, 128 * (b + 1))
        values = [ref[14:, :, cols].astype(jnp.float32) for ref, _ in sides]
        scale, k = scales_of(jnp.max(jnp.maximum(jnp.abs(values[0]), jnp.abs(values[1])), axis=0))
        out_ref[61, :, cols] = jnp.broadcast_to(k, (8, 128)).astype(jnp.bfloat16)
        for value, (_, first) in zip(values, sides):
            for x in range(8):
                for i in range(2):
                    out_ref[28 + 4 * x + first + 2 * i, :, cols] = (value[2 * x + i] * scale).astype(jnp.bfloat16)


def in_vmem(kernel, blocks, *args):
    return pl.pallas_call(
        kernel,
        out_shape=jax.ShapeDtypeStruct((blocks, 8, 512), jnp.bfloat16),
        in_specs=[pl.BlockSpec(memory_space=pltpu.VMEM)] * len(args),
        out_specs=pl.BlockSpec(memory_space=pltpu.VMEM),
        cost_estimate=pl.CostEstimate(flops=1_000_000, bytes_accessed=600_000, transcendentals=0),
        compiler_params=pltpu.CompilerParams(vmem_limit_bytes=4 << 20),
    )(*args)


def hidden_kernel(gate_ref, up_ref, out_ref, gate_in, up_in, done, in_sem, out_sem):
    h = gate_ref.shape[0]
    part = h // 4 // 16 * 16
    bands = [pl.ds(n * part, part if n < 3 else h - 3 * part) for n in range(4)]
    loads = []
    for n, band in enumerate(bands):
        for i, (ref, into) in enumerate(((gate_ref, gate_in), (up_ref, up_in))):
            loads.append(pltpu.make_async_copy(ref.at[band, :], into.at[band, :], in_sem.at[n, i]))
            loads[-1].start()
    copies = []
    for n, band in enumerate(bands):
        loads[2 * n].wait()
        loads[2 * n + 1].wait()
        gate = gate_in[band, :].astype(jnp.float32)
        sig = jax.nn.sigmoid(gate)
        done[band, :] = ((gate * sig) * up_in[band, :].astype(jnp.float32)).astype(jnp.bfloat16)
        for i in range(8):
            copies.append(pltpu.make_async_copy(done.at[band, :], out_ref.at[i, band, :], out_sem.at[n, i]))
            copies[-1].start()
    for copy in copies:
        copy.wait()


def hidden_copies(gate, up):
    h, t = gate.shape
    return pl.pallas_call(
        hidden_kernel,
        out_shape=jax.ShapeDtypeStruct((8, h, t), jnp.bfloat16),
        in_specs=[pl.BlockSpec(memory_space=pltpu.HBM)] * 2,
        out_specs=pl.BlockSpec(memory_space=pl.ANY),
        scratch_shapes=[pltpu.VMEM((h, t), jnp.bfloat16)] * 3 + [pltpu.SemaphoreType.DMA((4, 2)), pltpu.SemaphoreType.DMA((4, 8))],
        cost_estimate=pl.CostEstimate(flops=2_000_000, bytes_accessed=10 * h * t * 2, transcendentals=h * t),
        compiler_params=pltpu.CompilerParams(vmem_limit_bytes=60 * 1024 * 1024),
        name="hidden_copies",
    )(gate, up)


def split_kernel(g_ref, out_ref, own_ref, held, sem):
    zh, x, c = lax.axis_index("zh"), lax.axis_index("x"), lax.axis_index("c")
    for n in range(8):
        for i, core in enumerate((1 - c, c)):
            for j, z in enumerate((1 - zh, zh)):
                at = pl.multiple_of(2048 * z + 256 * n + 128 * core, 128)
                piece = g_ref[:, pl.ds(at, 128)]
                for zl in range(2):
                    held[2 * n + zl, :, 256 * i + 128 * j : 256 * i + 128 * (j + 1)] = piece
    copy = pltpu.make_async_copy(held, out_ref, sem)
    copy.start()
    for s in range(1, 8):
        for z in range(2):
            at = pl.multiple_of(2048 * z + 256 * lax.bitwise_xor(x, s), 256)
            own_ref[s - 1, :, 256 * z : 256 * (z + 1)] = g_ref[:, pl.ds(at, 256)]
    copy.wait()


def split_rows(g):
    return pl.pallas_call(
        split_kernel,
        out_shape=(jax.ShapeDtypeStruct((16, 8, 512), jnp.bfloat16), jax.ShapeDtypeStruct((7, 8, 512), jnp.bfloat16)),
        in_specs=[pl.BlockSpec(memory_space=pltpu.VMEM)],
        out_specs=(pl.BlockSpec(memory_space=pl.ANY), pl.BlockSpec(memory_space=pltpu.VMEM)),
        scratch_shapes=[pltpu.VMEM((16, 8, 512), jnp.bfloat16), pltpu.SemaphoreType.DMA],
        compiler_params=pltpu.CompilerParams(vmem_limit_bytes=2 << 20),
        name="split_rows",
    )(g)


def weights_kernel(hidden_ref, feats_ref, theirs_ref, ours_ref, held, sem):
    t = hidden_ref.shape[2]
    loads = [pltpu.make_async_copy(hidden_ref.at[i], held.at[:, t * i : t * (i + 1)], sem.at[i]) for i in range(8)]
    for load in loads:
        load.start()
    for i in range(0, 8, 2):
        loads[i].wait()
        loads[i + 1].wait()
        cols = slice(t * i, t * (i + 2))
        for n, ref in enumerate((theirs_ref, ours_ref)):
            part = jnp.dot(held[:, cols], feats_ref[cols, 256 * n : 256 * (n + 1)], preferred_element_type=jnp.float32)
            ref[...] = part if i == 0 else ref[...] + part


def weight_parts(hiddens, feats):
    _, h, t = hiddens.shape
    return pl.pallas_call(
        weights_kernel,
        out_shape=(jax.ShapeDtypeStruct((h, 256), jnp.float32),) * 2,
        in_specs=[pl.BlockSpec(memory_space=pltpu.HBM), pl.BlockSpec(memory_space=pltpu.VMEM)],
        out_specs=(pl.BlockSpec(memory_space=pltpu.VMEM),) * 2,
        scratch_shapes=[pltpu.VMEM((h, 8 * t), jnp.bfloat16), pltpu.SemaphoreType.DMA((8,))],
        cost_estimate=pl.CostEstimate(flops=2 * 8 * t * h * 512, bytes_accessed=4_000_000, transcendentals=0),
        compiler_params=pltpu.CompilerParams(vmem_limit_bytes=12 << 20),
        name="weight_parts",
    )(hiddens, feats)


def input_grads(front_ref, last_ref, feats_ref, weight_ref, gate_ref, up_ref, grads, weight, total, done, sem):
    zh, x, c = lax.axis_index("zh"), lax.axis_index("x"), lax.axis_index("c")
    t = gate_ref.shape[1]
    for n in range(8):
        slot = n % 2
        if n < 7:
            for z in range(2):
                at = pl.multiple_of(2048 * z + 256 * lax.bitwise_xor(x, n + 1), 256)
                weight[slot, :, 256 * z : 256 * (z + 1)] = weight_ref[:, pl.ds(at, 256)]
            if n < 5:
                rows = front_ref[t * n : t * (n + 1), :]
            elif n == 5:
                rows = jnp.concatenate([front_ref[t * n :, :], last_ref[: last_ref.shape[0] - t, :]], 0)
            else:
                rows = last_ref[last_ref.shape[0] - t :, :]
        else:
            for i, core in enumerate((1 - c, c)):
                for j, z in enumerate((1 - zh, zh)):
                    at = pl.multiple_of(2048 * z + 256 * x + 128 * core, 128)
                    weight[slot, :, 256 * i + 128 * j : 256 * i + 128 * (j + 1)] = weight_ref[:, pl.ds(at, 128)]
            rows = feats_ref[pl.ds(pl.multiple_of(x * t, t), t), :]
        part = lax.dot_general(weight[slot], rows, (((1,), (1,)), ((), ())), preferred_element_type=jnp.float32)
        total[...] = part if n == 0 else total[...] + part
    grad_hidden = total[...]
    gate = gate_ref[...].astype(jnp.float32)
    upper = up_ref[...].astype(jnp.float32)
    sig = jax.nn.sigmoid(gate)
    done[0] = (grad_hidden * upper * sig * (1.0 + gate * (1.0 - sig))).astype(jnp.bfloat16)
    done[1] = (grad_hidden * (gate * sig)).astype(jnp.bfloat16)
    copies = [pltpu.make_async_copy(done.at[i], grads[i], sem.at[i]) for i in range(2)]
    for copy in copies:
        copy.start()
    for copy in copies:
        copy.wait()


def before_kernel(ours_ref, swap_ref, *refs):
    inputs, (send_ref, here_ref), grads, scratch = refs[:6], refs[6:8], refs[8:10], refs[10:]
    other = 1 - lax.axis_index("c")
    send_ref[...] = (ours_ref[:, :128] + swap_ref[other, :, :128].astype(jnp.float32)).astype(jnp.bfloat16)
    here_ref[...] = ours_ref[:, 128:] + swap_ref[other, :, 128:].astype(jnp.float32)
    pl.when(lax.axis_index("zh") == 0)(lambda: input_grads(*inputs, grads, *scratch))


def after_kernel(here_ref, both_ref, *refs):
    inputs, sum_ref, grads, scratch = refs[:6], refs[8], refs[9:11], refs[11:]
    zh = lax.axis_index("zh")
    sum_ref[...] = here_ref[...] + both_ref[1 - zh].astype(jnp.float32)
    pl.when(zh == 1)(lambda: input_grads(*inputs, grads, *scratch))


def with_grads(kernel, terms, inputs, grads, outs):
    h, t = inputs[-1].shape
    vmem, anywhere = pl.BlockSpec(memory_space=pltpu.VMEM), pl.BlockSpec(memory_space=pl.ANY)
    args = terms + inputs + grads
    return pl.pallas_call(
        kernel,
        out_shape=tuple(jax.ShapeDtypeStruct((h, 128), dtype) for dtype in outs) + (jax.ShapeDtypeStruct((h, t), jnp.bfloat16),) * 2,
        in_specs=[vmem] * len(terms + inputs) + [anywhere] * len(grads),
        out_specs=(vmem,) * len(outs) + (anywhere,) * 2,
        input_output_aliases={len(terms + inputs) + i: len(outs) + i for i in range(len(grads))},
        scratch_shapes=[
            pltpu.VMEM((2, h, 512), jnp.bfloat16),
            pltpu.VMEM((h, t), jnp.float32),
            pltpu.VMEM((2, h, t), jnp.bfloat16),
            pltpu.SemaphoreType.DMA((2,)),
        ],
        cost_estimate=pl.CostEstimate(flops=2 * h * t * 4096, bytes_accessed=6_000_000, transcendentals=h * t),
        compiler_params=pltpu.CompilerParams(vmem_limit_bytes=16 << 20),
    )(*args)


def turned(x, axis, by):
    return lax.ppermute(x, axis, [(i, i ^ by) for i in range(lax.axis_size(axis))])


def sections(grad_out, gate_pre, up_pre, down_weight):
    gate_t, up_t = gate_pre.T, up_pre.T
    _, t = gate_t.shape

    pieces, own = split_rows(grad_out)
    mine = lax.all_to_all(pieces, ("x", "zl2"), 0, 0)
    near = turned(own, "zl2", 1)
    copies = hidden_copies(gate_t, up_t)
    packed = in_vmem(pack_kernel, 30, own, near, mine)
    far = turned(packed, "zl1", 1)
    hiddens = lax.all_to_all(copies, "x", 0, 0)

    message = in_vmem(code_kernel, 62, packed, far).astype(jnp.float16)
    got = lax.all_gather(message, "y", axis=1, tiled=True)

    scale = power(got[60:].astype(jnp.float32), -1)
    feats = (got[28:60].astype(jnp.float32) * scale[1]).astype(jnp.bfloat16).reshape(8 * t, 512)
    front = (got[:22].astype(jnp.float32) * scale[0]).astype(jnp.bfloat16).reshape(22 * 64, 512)
    last = (got[22:28].astype(jnp.float32) * scale[0]).astype(jnp.bfloat16).reshape(6 * 64, 512)

    theirs, ours = weight_parts(hiddens, feats)
    swap = lax.all_gather(theirs.astype(jnp.bfloat16), "c", axis=0)
    inputs = (front, last, feats, down_weight.T, gate_t, up_t)
    send, here, *grads = with_grads(before_kernel, (ours, swap), inputs, (), (jnp.bfloat16, jnp.float32))
    both = lax.all_gather(send, "zh", axis=0)
    total, grad_gate, grad_up = with_grads(after_kernel, (here, both), inputs, tuple(grads), (jnp.float32,))
    return total.T, grad_gate.T, grad_up.T


def solution(mesh):
    dims = (2, 8, 2, 2, 2, 8)
    fine = Mesh(mesh.devices.reshape(dims), AXES)
    dp, tensor = ("zh", "x", "c"), ("zl2", "zl1", "y")
    in_specs = (P(dp + tensor, None), P(dp, tensor), P(dp, tensor), P(None, tensor))
    out_specs = (P(dp, tensor), P(dp, tensor), P(dp, tensor))
    return jax.shard_map(sections, mesh=fine, in_specs=in_specs, out_specs=out_specs, check_vma=False)
```

```python
import jax
import jax.numpy as jnp
from jax import lax
from jax.experimental import pallas as pl
from jax.experimental.pallas import tpu as pltpu
from jax.sharding import Mesh, PartitionSpec as P


AXES = ("zh", "x", "c", "zl2", "zl1", "y")
STEPS = (64.0, 32.0, 16.0, 8.0, 4.0, 2.0)


def exponents(most):
    k = jnp.zeros_like(most)
    for bit in STEPS:
        fits = most * (2.0**bit) <= 32768.0
        most = jnp.where(fits, most * (2.0**bit), most)
        k = jnp.where(fits, k + bit, k)
    return k


def power(k, sign):
    scale = jnp.ones_like(k)
    for bit in STEPS:
        has = k >= bit
        scale = jnp.where(has, scale * (2.0 ** (sign * bit)), scale)
        k = jnp.where(has, k - bit, k)
    return scale


def scales_of(most):
    k = exponents(jnp.max(jnp.max(most, axis=1, keepdims=True), axis=0, keepdims=True))
    return power(k, 1), k


def pack_kernel(own_ref, near_ref, rows_ref, out_ref):
    out_ref[:7] = own_ref[...]
    out_ref[7:14] = near_ref[...]
    out_ref[14:] = rows_ref[...]


def code_kernel(here_ref, far_ref, out_ref):
    zl2, zl1 = lax.axis_index("zl2"), lax.axis_index("zl1")
    sides = ((here_ref, zl1), (far_ref, 1 - zl1))
    most = None
    for ref, _ in sides:
        for b in range(4):
            value = jnp.max(jnp.abs(ref[:14, :, 128 * b : 128 * (b + 1)].astype(jnp.float32)), axis=0)
            most = value if most is None else jnp.maximum(most, value)
    scale, k = scales_of(most)
    line = lax.broadcasted_iota(jnp.int32, (8, 128), 0)
    own_k = k
    for ref, first in sides:
        for turn in range(2):
            place = first + 2 * lax.bitwise_xor(zl2, turn)
            for s in range(7):
                out_ref[4 * s + place] = (ref[7 * turn + s].astype(jnp.float32) * scale).astype(jnp.bfloat16)
    for b in range(4):
        cols = slice(128 * b, 128 * (b + 1))
        values = [ref[14:, :, cols].astype(jnp.float32) for ref, _ in sides]
        scale, k = scales_of(jnp.max(jnp.maximum(jnp.abs(values[0]), jnp.abs(values[1])), axis=0))
        out_ref[60, :, cols] = jnp.where(line < 4, own_k, k).astype(jnp.bfloat16)
        for value, (_, first) in zip(values, sides):
            for x in range(8):
                for i in range(2):
                    out_ref[28 + 4 * x + first + 2 * i, :, cols] = (value[2 * x + i] * scale).astype(jnp.bfloat16)


def in_vmem(kernel, blocks, *args):
    return pl.pallas_call(
        kernel,
        out_shape=jax.ShapeDtypeStruct((blocks, 8, 512), jnp.bfloat16),
        in_specs=[pl.BlockSpec(memory_space=pltpu.VMEM)] * len(args),
        out_specs=pl.BlockSpec(memory_space=pltpu.VMEM),
        cost_estimate=pl.CostEstimate(flops=1_000_000, bytes_accessed=600_000, transcendentals=0),
        compiler_params=pltpu.CompilerParams(vmem_limit_bytes=4 << 20),
    )(*args)


def scales_kernel(k_ref, own_ref, rows_ref):
    for y in range(8):
        k = k_ref[8 * y : 8 * y + 8, :].astype(jnp.float32)
        scale = power(k, -1)
        own_ref[8 * y : 8 * y + 8, :] = jnp.broadcast_to(scale[:1], (8, 512))
        rows_ref[8 * y : 8 * y + 8, :] = jnp.broadcast_to(scale[4:5], (8, 512))


def scales(k):
    return pl.pallas_call(
        scales_kernel,
        out_shape=(jax.ShapeDtypeStruct((64, 512), jnp.float32),) * 2,
        in_specs=[pl.BlockSpec(memory_space=pltpu.VMEM)],
        out_specs=(pl.BlockSpec(memory_space=pltpu.VMEM),) * 2,
        cost_estimate=pl.CostEstimate(flops=1_000_000, bytes_accessed=400_000, transcendentals=0),
        compiler_params=pltpu.CompilerParams(vmem_limit_bytes=2 << 20),
        name="scales",
    )(k)


def hidden_kernel(gate_ref, up_ref, out_ref, gate_in, up_in, done, in_sem, out_sem):
    h = gate_ref.shape[0]
    part = h // 4 // 16 * 16
    bands = [pl.ds(n * part, part if n < 3 else h - 3 * part) for n in range(4)]
    loads = []
    for n, band in enumerate(bands):
        for i, (ref, into) in enumerate(((gate_ref, gate_in), (up_ref, up_in))):
            loads.append(pltpu.make_async_copy(ref.at[band, :], into.at[band, :], in_sem.at[n, i]))
            loads[-1].start()
    copies = []
    for n, band in enumerate(bands):
        loads[2 * n].wait()
        loads[2 * n + 1].wait()
        gate = gate_in[band, :].astype(jnp.float32)
        sig = jax.nn.sigmoid(gate)
        done[band, :] = ((gate * sig) * up_in[band, :].astype(jnp.float32)).astype(jnp.bfloat16)
        for i in range(8):
            copies.append(pltpu.make_async_copy(done.at[band, :], out_ref.at[i, band, :], out_sem.at[n, i]))
            copies[-1].start()
    for copy in copies:
        copy.wait()


def hidden_copies(gate, up):
    h, t = gate.shape
    return pl.pallas_call(
        hidden_kernel,
        out_shape=jax.ShapeDtypeStruct((8, h, t), jnp.bfloat16),
        in_specs=[pl.BlockSpec(memory_space=pltpu.HBM)] * 2,
        out_specs=pl.BlockSpec(memory_space=pl.ANY),
        scratch_shapes=[pltpu.VMEM((h, t), jnp.bfloat16)] * 3 + [pltpu.SemaphoreType.DMA((4, 2)), pltpu.SemaphoreType.DMA((4, 8))],
        cost_estimate=pl.CostEstimate(flops=2_000_000, bytes_accessed=10 * h * t * 2, transcendentals=h * t),
        compiler_params=pltpu.CompilerParams(vmem_limit_bytes=60 * 1024 * 1024),
        name="hidden_copies",
    )(gate, up)


def split_kernel(g_ref, out_ref, own_ref, held, sem):
    zh, x, c = lax.axis_index("zh"), lax.axis_index("x"), lax.axis_index("c")
    for n in range(8):
        for i, core in enumerate((1 - c, c)):
            for j, z in enumerate((1 - zh, zh)):
                at = pl.multiple_of(2048 * z + 256 * n + 128 * core, 128)
                piece = g_ref[:, pl.ds(at, 128)]
                for zl in range(2):
                    held[2 * n + zl, :, 256 * i + 128 * j : 256 * i + 128 * (j + 1)] = piece
    copy = pltpu.make_async_copy(held, out_ref, sem)
    copy.start()
    for s in range(1, 8):
        for z in range(2):
            at = pl.multiple_of(2048 * z + 256 * lax.bitwise_xor(x, s), 256)
            own_ref[s - 1, :, 256 * z : 256 * (z + 1)] = g_ref[:, pl.ds(at, 256)]
    copy.wait()


def split_rows(g):
    return pl.pallas_call(
        split_kernel,
        out_shape=(jax.ShapeDtypeStruct((16, 8, 512), jnp.bfloat16), jax.ShapeDtypeStruct((7, 8, 512), jnp.bfloat16)),
        in_specs=[pl.BlockSpec(memory_space=pltpu.VMEM)],
        out_specs=(pl.BlockSpec(memory_space=pl.ANY), pl.BlockSpec(memory_space=pltpu.VMEM)),
        scratch_shapes=[pltpu.VMEM((16, 8, 512), jnp.bfloat16), pltpu.SemaphoreType.DMA],
        compiler_params=pltpu.CompilerParams(vmem_limit_bytes=2 << 20),
        name="split_rows",
    )(g)


def weights_kernel(hidden_ref, feats_ref, theirs_ref, ours_ref, held, sem):
    t = hidden_ref.shape[2]
    loads = [pltpu.make_async_copy(hidden_ref.at[i], held.at[:, t * i : t * (i + 1)], sem.at[i]) for i in range(8)]
    for load in loads:
        load.start()
    for i in range(0, 8, 2):
        loads[i].wait()
        loads[i + 1].wait()
        cols = slice(t * i, t * (i + 2))
        for n, ref in enumerate((theirs_ref, ours_ref)):
            part = jnp.dot(held[:, cols], feats_ref[cols, 256 * n : 256 * (n + 1)], preferred_element_type=jnp.float32)
            ref[...] = part if i == 0 else ref[...] + part


def weight_parts(hiddens, feats):
    _, h, t = hiddens.shape
    return pl.pallas_call(
        weights_kernel,
        out_shape=(jax.ShapeDtypeStruct((h, 256), jnp.float32),) * 2,
        in_specs=[pl.BlockSpec(memory_space=pltpu.HBM), pl.BlockSpec(memory_space=pltpu.VMEM)],
        out_specs=(pl.BlockSpec(memory_space=pltpu.VMEM),) * 2,
        scratch_shapes=[pltpu.VMEM((h, 8 * t), jnp.bfloat16), pltpu.SemaphoreType.DMA((8,))],
        cost_estimate=pl.CostEstimate(flops=2 * 8 * t * h * 512, bytes_accessed=4_000_000, transcendentals=0),
        compiler_params=pltpu.CompilerParams(vmem_limit_bytes=12 << 20),
        name="weight_parts",
    )(hiddens, feats)


def input_grads(front_ref, last_ref, feats_ref, weight_ref, gate_ref, up_ref, grads, weight, total, done, sem):
    zh, x, c = lax.axis_index("zh"), lax.axis_index("x"), lax.axis_index("c")
    t = gate_ref.shape[1]
    for n in range(8):
        slot = n % 2
        if n < 7:
            for z in range(2):
                at = pl.multiple_of(2048 * z + 256 * lax.bitwise_xor(x, n + 1), 256)
                weight[slot, :, 256 * z : 256 * (z + 1)] = weight_ref[:, pl.ds(at, 256)]
            if n < 5:
                rows = front_ref[t * n : t * (n + 1), :]
            elif n == 5:
                rows = jnp.concatenate([front_ref[t * n :, :], last_ref[: last_ref.shape[0] - t, :]], 0)
            else:
                rows = last_ref[last_ref.shape[0] - t :, :]
        else:
            for i, core in enumerate((1 - c, c)):
                for j, z in enumerate((1 - zh, zh)):
                    at = pl.multiple_of(2048 * z + 256 * x + 128 * core, 128)
                    weight[slot, :, 256 * i + 128 * j : 256 * i + 128 * (j + 1)] = weight_ref[:, pl.ds(at, 128)]
            rows = feats_ref[pl.ds(pl.multiple_of(x * t, t), t), :]
        part = lax.dot_general(weight[slot], rows, (((1,), (1,)), ((), ())), preferred_element_type=jnp.float32)
        total[...] = part if n == 0 else total[...] + part
    grad_hidden = total[...]
    gate = gate_ref[...].astype(jnp.float32)
    upper = up_ref[...].astype(jnp.float32)
    sig = jax.nn.sigmoid(gate)
    done[0] = (grad_hidden * upper * sig * (1.0 + gate * (1.0 - sig))).astype(jnp.bfloat16)
    done[1] = (grad_hidden * (gate * sig)).astype(jnp.bfloat16)
    copies = [pltpu.make_async_copy(done.at[i], grads[i], sem.at[i]) for i in range(2)]
    for copy in copies:
        copy.start()
    for copy in copies:
        copy.wait()


def before_kernel(ours_ref, swap_ref, *refs):
    inputs, (send_ref, here_ref), grads, scratch = refs[:6], refs[6:8], refs[8:10], refs[10:]
    other = 1 - lax.axis_index("c")
    send_ref[...] = (ours_ref[:, :128] + swap_ref[other, :, :128].astype(jnp.float32)).astype(jnp.bfloat16)
    here_ref[...] = ours_ref[:, 128:] + swap_ref[other, :, 128:].astype(jnp.float32)
    pl.when(lax.axis_index("zh") == 0)(lambda: input_grads(*inputs, grads, *scratch))


def after_kernel(here_ref, both_ref, *refs):
    inputs, sum_ref, grads, scratch = refs[:6], refs[8], refs[9:11], refs[11:]
    zh = lax.axis_index("zh")
    sum_ref[...] = here_ref[...] + both_ref[1 - zh].astype(jnp.float32)
    pl.when(zh == 1)(lambda: input_grads(*inputs, grads, *scratch))


def with_grads(kernel, terms, inputs, grads, outs):
    h, t = inputs[-1].shape
    vmem, anywhere = pl.BlockSpec(memory_space=pltpu.VMEM), pl.BlockSpec(memory_space=pl.ANY)
    args = terms + inputs + grads
    return pl.pallas_call(
        kernel,
        out_shape=tuple(jax.ShapeDtypeStruct((h, 128), dtype) for dtype in outs) + (jax.ShapeDtypeStruct((h, t), jnp.bfloat16),) * 2,
        in_specs=[vmem] * len(terms + inputs) + [anywhere] * len(grads),
        out_specs=(vmem,) * len(outs) + (anywhere,) * 2,
        input_output_aliases={len(terms + inputs) + i: len(outs) + i for i in range(len(grads))},
        scratch_shapes=[
            pltpu.VMEM((2, h, 512), jnp.bfloat16),
            pltpu.VMEM((h, t), jnp.float32),
            pltpu.VMEM((2, h, t), jnp.bfloat16),
            pltpu.SemaphoreType.DMA((2,)),
        ],
        cost_estimate=pl.CostEstimate(flops=2 * h * t * 4096, bytes_accessed=6_000_000, transcendentals=h * t),
        compiler_params=pltpu.CompilerParams(vmem_limit_bytes=16 << 20),
    )(*args)


def turned(x, axis, by):
    return lax.ppermute(x, axis, [(i, i ^ by) for i in range(lax.axis_size(axis))])


def sections(grad_out, gate_pre, up_pre, down_weight):
    gate_t, up_t = gate_pre.T, up_pre.T
    _, t = gate_t.shape

    pieces, own = split_rows(grad_out)
    mine = lax.all_to_all(pieces, ("x", "zl2"), 0, 0)
    near = turned(own, "zl2", 1)
    copies = hidden_copies(gate_t, up_t)
    packed = in_vmem(pack_kernel, 30, own, near, mine)
    far = turned(packed, "zl1", 1)
    hiddens = lax.all_to_all(copies, "x", 0, 0)

    message = in_vmem(code_kernel, 61, packed, far).astype(jnp.float16)
    got = lax.all_gather(message, "y", axis=1, tiled=True)

    scale = scales(got[60].astype(jnp.bfloat16))
    feats = (got[28:60].astype(jnp.float32) * scale[1]).astype(jnp.bfloat16).reshape(8 * t, 512)
    front = (got[:22].astype(jnp.float32) * scale[0]).astype(jnp.bfloat16).reshape(22 * 64, 512)
    last = (got[22:28].astype(jnp.float32) * scale[0]).astype(jnp.bfloat16).reshape(6 * 64, 512)

    theirs, ours = weight_parts(hiddens, feats)
    swap = lax.all_gather(theirs.astype(jnp.bfloat16), "c", axis=0)
    inputs = (front, last, feats, down_weight.T, gate_t, up_t)
    send, here, *grads = with_grads(before_kernel, (ours, swap), inputs, (), (jnp.bfloat16, jnp.float32))
    both = lax.all_gather(send, "zh", axis=0)
    total, grad_gate, grad_up = with_grads(after_kernel, (here, both), inputs, tuple(grads), (jnp.float32,))
    return total.T, grad_gate.T, grad_up.T


def solution(mesh):
    dims = (2, 8, 2, 2, 2, 8)
    fine = Mesh(mesh.devices.reshape(dims), AXES)
    dp, tensor = ("zh", "x", "c"), ("zl2", "zl1", "y")
    in_specs = (P(dp + tensor, None), P(dp, tensor), P(dp, tensor), P(None, tensor))
    out_specs = (P(dp, tensor), P(dp, tensor), P(dp, tensor))
    return jax.shard_map(sections, mesh=fine, in_specs=in_specs, out_specs=out_specs, check_vma=False)
```

```python
import jax
import jax.numpy as jnp
from jax import lax
from jax.experimental import pallas as pl
from jax.experimental.pallas import tpu as pltpu
from jax.sharding import Mesh, PartitionSpec as P


AXES = ("zh", "x", "c", "zl2", "zl1", "y")
STEPS = (64.0, 32.0, 16.0, 8.0, 4.0, 2.0)


def exponents(most):
    k = jnp.zeros_like(most)
    for bit in STEPS:
        fits = most * (2.0**bit) <= 32768.0
        most = jnp.where(fits, most * (2.0**bit), most)
        k = jnp.where(fits, k + bit, k)
    return k


def power(k, sign):
    scale = jnp.ones_like(k)
    for bit in STEPS:
        has = k >= bit
        scale = jnp.where(has, scale * (2.0 ** (sign * bit)), scale)
        k = jnp.where(has, k - bit, k)
    return scale


def scales_of(most):
    k = exponents(jnp.max(jnp.max(most, axis=1, keepdims=True), axis=0, keepdims=True))
    return power(k, 1), k


def pack_kernel(own_ref, near_ref, rows_ref, out_ref):
    out_ref[:7] = own_ref[...]
    out_ref[7:14] = near_ref[...]
    out_ref[14:] = rows_ref[...]


def code_kernel(here_ref, far_ref, out_ref):
    zl2, zl1 = lax.axis_index("zl2"), lax.axis_index("zl1")
    sides = ((here_ref, zl1), (far_ref, 1 - zl1))
    most = None
    for ref, _ in sides:
        for b in range(4):
            value = jnp.max(jnp.abs(ref[:14, :, 128 * b : 128 * (b + 1)].astype(jnp.float32)), axis=0)
            most = value if most is None else jnp.maximum(most, value)
    scale, k = scales_of(most)
    line = lax.broadcasted_iota(jnp.int32, (8, 128), 0)
    own_k = k
    for ref, first in sides:
        for turn in range(2):
            place = first + 2 * lax.bitwise_xor(zl2, turn)
            for s in range(7):
                out_ref[4 * s + place] = (ref[7 * turn + s].astype(jnp.float32) * scale).astype(jnp.bfloat16)
    for b in range(4):
        cols = slice(128 * b, 128 * (b + 1))
        values = [ref[14:, :, cols].astype(jnp.float32) for ref, _ in sides]
        scale, k = scales_of(jnp.max(jnp.maximum(jnp.abs(values[0]), jnp.abs(values[1])), axis=0))
        out_ref[60, :, cols] = jnp.where(line < 4, own_k, k).astype(jnp.bfloat16)
        for value, (_, first) in zip(values, sides):
            for x in range(8):
                for i in range(2):
                    out_ref[28 + 4 * x + first + 2 * i, :, cols] = (value[8 * i + x] * scale).astype(jnp.bfloat16)


def in_vmem(kernel, blocks, *args):
    return pl.pallas_call(
        kernel,
        out_shape=jax.ShapeDtypeStruct((blocks, 8, 512), jnp.bfloat16),
        in_specs=[pl.BlockSpec(memory_space=pltpu.VMEM)] * len(args),
        out_specs=pl.BlockSpec(memory_space=pltpu.VMEM),
        cost_estimate=pl.CostEstimate(flops=1_000_000, bytes_accessed=600_000, transcendentals=0),
        compiler_params=pltpu.CompilerParams(vmem_limit_bytes=4 << 20),
    )(*args)


def scales_kernel(k_ref, own_ref, rows_ref):
    for y in range(8):
        k = k_ref[8 * y : 8 * y + 8, :].astype(jnp.float32)
        scale = power(k, -1)
        own_ref[8 * y : 8 * y + 8, :] = jnp.broadcast_to(scale[:1], (8, 512))
        rows_ref[8 * y : 8 * y + 8, :] = jnp.broadcast_to(scale[4:5], (8, 512))


def scales(k):
    return pl.pallas_call(
        scales_kernel,
        out_shape=(jax.ShapeDtypeStruct((64, 512), jnp.float32),) * 2,
        in_specs=[pl.BlockSpec(memory_space=pltpu.VMEM)],
        out_specs=(pl.BlockSpec(memory_space=pltpu.VMEM),) * 2,
        cost_estimate=pl.CostEstimate(flops=1_000_000, bytes_accessed=400_000, transcendentals=0),
        compiler_params=pltpu.CompilerParams(vmem_limit_bytes=2 << 20),
        name="scales",
    )(k)


def hidden_kernel(gate_ref, up_ref, out_ref, gate_in, up_in, done, in_sem, out_sem):
    h = gate_ref.shape[0]
    part = h // 4 // 16 * 16
    bands = [pl.ds(n * part, part if n < 3 else h - 3 * part) for n in range(4)]
    loads = []
    for n, band in enumerate(bands):
        for i, (ref, into) in enumerate(((gate_ref, gate_in), (up_ref, up_in))):
            loads.append(pltpu.make_async_copy(ref.at[band, :], into.at[band, :], in_sem.at[n, i]))
            loads[-1].start()
    copies = []
    for n, band in enumerate(bands):
        loads[2 * n].wait()
        loads[2 * n + 1].wait()
        gate = gate_in[band, :].astype(jnp.float32)
        sig = jax.nn.sigmoid(gate)
        done[band, :] = ((gate * sig) * up_in[band, :].astype(jnp.float32)).astype(jnp.bfloat16)
        for i in range(8):
            copies.append(pltpu.make_async_copy(done.at[band, :], out_ref.at[i, band, :], out_sem.at[n, i]))
            copies[-1].start()
    for copy in copies:
        copy.wait()


def hidden_copies(gate, up):
    h, t = gate.shape
    return pl.pallas_call(
        hidden_kernel,
        out_shape=jax.ShapeDtypeStruct((8, h, t), jnp.bfloat16),
        in_specs=[pl.BlockSpec(memory_space=pltpu.HBM)] * 2,
        out_specs=pl.BlockSpec(memory_space=pl.ANY),
        scratch_shapes=[pltpu.VMEM((h, t), jnp.bfloat16)] * 3 + [pltpu.SemaphoreType.DMA((4, 2)), pltpu.SemaphoreType.DMA((4, 8))],
        cost_estimate=pl.CostEstimate(flops=2_000_000, bytes_accessed=10 * h * t * 2, transcendentals=h * t),
        compiler_params=pltpu.CompilerParams(vmem_limit_bytes=60 * 1024 * 1024),
        name="hidden_copies",
    )(gate, up)


def split_kernel(g_ref, out_ref, own_ref, held, sem):
    zh, x, c = lax.axis_index("zh"), lax.axis_index("x"), lax.axis_index("c")
    for n in range(8):
        for i, core in enumerate((1 - c, c)):
            for j, z in enumerate((1 - zh, zh)):
                at = pl.multiple_of(2048 * z + 256 * n + 128 * core, 128)
                piece = g_ref[:, pl.ds(at, 128)]
                for zl in range(2):
                    held[8 * zl + n, :, 256 * i + 128 * j : 256 * i + 128 * (j + 1)] = piece
    copy = pltpu.make_async_copy(held, out_ref, sem)
    copy.start()
    for s in range(1, 8):
        for z in range(2):
            at = pl.multiple_of(2048 * z + 256 * lax.bitwise_xor(x, s), 256)
            own_ref[s - 1, :, 256 * z : 256 * (z + 1)] = g_ref[:, pl.ds(at, 256)]
    copy.wait()


def split_rows(g):
    return pl.pallas_call(
        split_kernel,
        out_shape=(jax.ShapeDtypeStruct((16, 8, 512), jnp.bfloat16), jax.ShapeDtypeStruct((7, 8, 512), jnp.bfloat16)),
        in_specs=[pl.BlockSpec(memory_space=pltpu.VMEM)],
        out_specs=(pl.BlockSpec(memory_space=pl.ANY), pl.BlockSpec(memory_space=pltpu.VMEM)),
        scratch_shapes=[pltpu.VMEM((16, 8, 512), jnp.bfloat16), pltpu.SemaphoreType.DMA],
        compiler_params=pltpu.CompilerParams(vmem_limit_bytes=2 << 20),
        name="split_rows",
    )(g)


def weights_kernel(hidden_ref, feats_ref, theirs_ref, ours_ref, held, sem):
    t = hidden_ref.shape[2]
    loads = [pltpu.make_async_copy(hidden_ref.at[i], held.at[:, t * i : t * (i + 1)], sem.at[i]) for i in range(8)]
    for load in loads:
        load.start()
    for i in range(0, 8, 2):
        loads[i].wait()
        loads[i + 1].wait()
        cols = slice(t * i, t * (i + 2))
        for n, ref in enumerate((theirs_ref, ours_ref)):
            part = jnp.dot(held[:, cols], feats_ref[cols, 256 * n : 256 * (n + 1)], preferred_element_type=jnp.float32)
            ref[...] = part if i == 0 else ref[...] + part


def weight_parts(hiddens, feats):
    _, h, t = hiddens.shape
    return pl.pallas_call(
        weights_kernel,
        out_shape=(jax.ShapeDtypeStruct((h, 256), jnp.float32),) * 2,
        in_specs=[pl.BlockSpec(memory_space=pltpu.HBM), pl.BlockSpec(memory_space=pltpu.VMEM)],
        out_specs=(pl.BlockSpec(memory_space=pltpu.VMEM),) * 2,
        scratch_shapes=[pltpu.VMEM((h, 8 * t), jnp.bfloat16), pltpu.SemaphoreType.DMA((8,))],
        cost_estimate=pl.CostEstimate(flops=2 * 8 * t * h * 512, bytes_accessed=4_000_000, transcendentals=0),
        compiler_params=pltpu.CompilerParams(vmem_limit_bytes=12 << 20),
        name="weight_parts",
    )(hiddens, feats)


def input_grads(front_ref, last_ref, feats_ref, weight_ref, gate_ref, up_ref, grads, weight, total, done, sem):
    zh, x, c = lax.axis_index("zh"), lax.axis_index("x"), lax.axis_index("c")
    t = gate_ref.shape[1]
    for n in range(8):
        slot = n % 2
        if n < 7:
            for z in range(2):
                at = pl.multiple_of(2048 * z + 256 * lax.bitwise_xor(x, n + 1), 256)
                weight[slot, :, 256 * z : 256 * (z + 1)] = weight_ref[:, pl.ds(at, 256)]
            if n < 5:
                rows = front_ref[t * n : t * (n + 1), :]
            elif n == 5:
                rows = jnp.concatenate([front_ref[t * n :, :], last_ref[: last_ref.shape[0] - t, :]], 0)
            else:
                rows = last_ref[last_ref.shape[0] - t :, :]
        else:
            for i, core in enumerate((1 - c, c)):
                for j, z in enumerate((1 - zh, zh)):
                    at = pl.multiple_of(2048 * z + 256 * x + 128 * core, 128)
                    weight[slot, :, 256 * i + 128 * j : 256 * i + 128 * (j + 1)] = weight_ref[:, pl.ds(at, 128)]
            rows = feats_ref[pl.ds(pl.multiple_of(x * t, t), t), :]
        part = lax.dot_general(weight[slot], rows, (((1,), (1,)), ((), ())), preferred_element_type=jnp.float32)
        total[...] = part if n == 0 else total[...] + part
    grad_hidden = total[...]
    gate = gate_ref[...].astype(jnp.float32)
    upper = up_ref[...].astype(jnp.float32)
    sig = jax.nn.sigmoid(gate)
    done[0] = (grad_hidden * upper * sig * (1.0 + gate * (1.0 - sig))).astype(jnp.bfloat16)
    done[1] = (grad_hidden * (gate * sig)).astype(jnp.bfloat16)
    copies = [pltpu.make_async_copy(done.at[i], grads[i], sem.at[i]) for i in range(2)]
    for copy in copies:
        copy.start()
    for copy in copies:
        copy.wait()


def before_kernel(ours_ref, swap_ref, *refs):
    inputs, (send_ref, here_ref), grads, scratch = refs[:6], refs[6:8], refs[8:10], refs[10:]
    other = 1 - lax.axis_index("c")
    send_ref[...] = (ours_ref[:, :128] + swap_ref[other, :, :128].astype(jnp.float32)).astype(jnp.bfloat16)
    here_ref[...] = ours_ref[:, 128:] + swap_ref[other, :, 128:].astype(jnp.float32)
    pl.when(lax.axis_index("zh") == 0)(lambda: input_grads(*inputs, grads, *scratch))


def after_kernel(here_ref, both_ref, *refs):
    inputs, sum_ref, grads, scratch = refs[:6], refs[8], refs[9:11], refs[11:]
    zh = lax.axis_index("zh")
    sum_ref[...] = here_ref[...] + both_ref[1 - zh].astype(jnp.float32)
    pl.when(zh == 1)(lambda: input_grads(*inputs, grads, *scratch))


def with_grads(kernel, terms, inputs, grads, outs):
    h, t = inputs[-1].shape
    vmem, anywhere = pl.BlockSpec(memory_space=pltpu.VMEM), pl.BlockSpec(memory_space=pl.ANY)
    args = terms + inputs + grads
    return pl.pallas_call(
        kernel,
        out_shape=tuple(jax.ShapeDtypeStruct((h, 128), dtype) for dtype in outs) + (jax.ShapeDtypeStruct((h, t), jnp.bfloat16),) * 2,
        in_specs=[vmem] * len(terms + inputs) + [anywhere] * len(grads),
        out_specs=(vmem,) * len(outs) + (anywhere,) * 2,
        input_output_aliases={len(terms + inputs) + i: len(outs) + i for i in range(len(grads))},
        scratch_shapes=[
            pltpu.VMEM((2, h, 512), jnp.bfloat16),
            pltpu.VMEM((h, t), jnp.float32),
            pltpu.VMEM((2, h, t), jnp.bfloat16),
            pltpu.SemaphoreType.DMA((2,)),
        ],
        cost_estimate=pl.CostEstimate(flops=2 * h * t * 4096, bytes_accessed=6_000_000, transcendentals=h * t),
        compiler_params=pltpu.CompilerParams(vmem_limit_bytes=16 << 20),
    )(*args)


def turned(x, axis, by):
    return lax.ppermute(x, axis, [(i, i ^ by) for i in range(lax.axis_size(axis))])


def sections(grad_out, gate_pre, up_pre, down_weight):
    gate_t, up_t = gate_pre.T, up_pre.T
    _, t = gate_t.shape

    pieces, own = split_rows(grad_out)
    mine = lax.all_to_all(pieces, ("zl2", "x"), 0, 0)
    near = turned(own, "zl2", 1)
    copies = hidden_copies(gate_t, up_t)
    packed = in_vmem(pack_kernel, 30, own, near, mine)
    far = turned(packed, "zl1", 1)
    hiddens = lax.all_to_all(copies, "x", 0, 0)

    message = in_vmem(code_kernel, 61, packed, far).astype(jnp.float16)
    got = lax.all_gather(message, "y", axis=1, tiled=True)

    scale = scales(got[60].astype(jnp.bfloat16))
    feats = (got[28:60].astype(jnp.float32) * scale[1]).astype(jnp.bfloat16).reshape(8 * t, 512)
    front = (got[:22].astype(jnp.float32) * scale[0]).astype(jnp.bfloat16).reshape(22 * 64, 512)
    last = (got[22:28].astype(jnp.float32) * scale[0]).astype(jnp.bfloat16).reshape(6 * 64, 512)

    theirs, ours = weight_parts(hiddens, feats)
    swap = lax.all_gather(theirs.astype(jnp.bfloat16), "c", axis=0)
    inputs = (front, last, feats, down_weight.T, gate_t, up_t)
    send, here, *grads = with_grads(before_kernel, (ours, swap), inputs, (), (jnp.bfloat16, jnp.float32))
    both = lax.all_gather(send, "zh", axis=0)
    total, grad_gate, grad_up = with_grads(after_kernel, (here, both), inputs, tuple(grads), (jnp.float32,))
    return total.T, grad_gate.T, grad_up.T


def solution(mesh):
    dims = (2, 8, 2, 2, 2, 8)
    fine = Mesh(mesh.devices.reshape(dims), AXES)
    dp, tensor = ("zh", "x", "c"), ("zl2", "zl1", "y")
    in_specs = (P(dp + tensor, None), P(dp, tensor), P(dp, tensor), P(None, tensor))
    out_specs = (P(dp, tensor), P(dp, tensor), P(dp, tensor))
    return jax.shard_map(sections, mesh=fine, in_specs=in_specs, out_specs=out_specs, check_vma=False)
```
